16 devices in a mesh: rep: 2 (over y, z), dp: 8 (over x, core).
Axes of the slice: x: 4, y: 2, z: 1, core: 2. Of those that a mesh axis runs over, the one named last changes fastest.
The devices are a block of a 4x4x8 slice.
Arguments:
- hidden: bfloat16 [1024, 2048], P(('rep', 'dp')), parts along dimension 0
- ckv_cache: bfloat16 [1024, 256, 512], P(('rep', 'dp')), parts along dimension 0
- kr_cache: bfloat16 [1024, 256, 64], P(('rep', 'dp')), parts along dimension 0
- seq_lens: int32 [1024], P(('rep', 'dp')), parts along dimension 0
- expert_ids: int32 [1024, 6], P(('rep', 'dp')), parts along dimension 0
- attn_gain: bfloat16 [2048], replicated
- kv_gain: bfloat16 [512], replicated
- moe_gain: bfloat16 [2048], replicated
- w_q: bfloat16 [2048, 3072], replicated
- w_dkv: bfloat16 [2048, 576], replicated
- w_uk: bfloat16 [16, 128, 512], replicated
- w_uv: bfloat16 [16, 512, 128], replicated
- w_o: bfloat16 [2048, 2048], replicated
- w_router: bfloat16 [2048, 64], replicated
- shared_gate: bfloat16 [2048, 2816], replicated
- shared_up: bfloat16 [2048, 2816], replicated
- shared_down: bfloat16 [2816, 2048], replicated
- expert_gate: bfloat16 [64, 2048, 1408], P('dp')
- expert_up: bfloat16 [64, 2048, 1408], P('dp')
- expert_down: bfloat16 [64, 1408, 2048], P('dp')
Outputs:
- output 1: bfloat16 [1024, 2048], P(('rep', 'dp')), parts along dimension 0
- output 2: bfloat16 [1024, 512], P(('rep', 'dp')), parts along dimension 0
- output 3: bfloat16 [1024, 64], P(('rep', 'dp')), parts along dimension 0
There are 2 independent parts. The reference program is written for one: setup_inputs(seed, part) draws one part's arguments, and reference() takes and returns one part's arrays. A program takes and returns all parts, laid end to end along the dimension named above; an argument that names none is the same for every part.
All inputs are finite; a program needn't handle non-finite values.
Results may differ from the reference program's by a relative error of at most 0.0127322.
Values are sent between devices in bfloat16 or wider.
A program may use at most 768 MiB of HBM per device.

```python
import jax
import jax.numpy as jnp
from jax import lax

DP_SIZE = 8
SEQS_DEV = 64
CACHE_LEN = 256
D_MODEL = 2048
HEADS = 16
NOPE_DIM = 128
ROPE_DIM = 64
V_DIM = 128
KV_LORA = 512
EXPERTS = 64
TOP_K = 6
FF_DIM = 1408
N_SHARED = 2

GROUP_ROWS = DP_SIZE * SEQS_DEV
SLOT_CAP = max(2, (2 * SEQS_DEV * TOP_K) // EXPERTS)
NORM_EPS = 1e-6
ROPE_THETA = 10000.0
SCORE_SCALE = (NOPE_DIM + ROPE_DIM) ** -0.5


def normal_bf16(draw_key, arr_shape, std_scale):
    return (jax.random.normal(draw_key, arr_shape, jnp.float32) * std_scale).astype(jnp.bfloat16)


def draw_gain(draw_key, gain_len):
    return jax.random.uniform(draw_key, (gain_len,), jnp.float32, minval=0.5, maxval=1.5).astype(jnp.bfloat16)


def draw_lengths(len_key):
    base_key, order_key = jax.random.split(len_key)
    base_lens = jax.random.randint(base_key, (GROUP_ROWS,), CACHE_LEN // 8, CACHE_LEN)
    seq_order = jax.random.permutation(order_key, GROUP_ROWS)
    return base_lens.at[seq_order[0]].set(CACHE_LEN - 1).at[seq_order[1]].set(CACHE_LEN // 8).astype(jnp.int32)


def draw_routes(route_key):
    hot_key, dev_key = jax.random.split(route_key)
    hot_expert = jax.random.randint(hot_key, (), 0, EXPERTS)
    choice_col = jnp.arange(TOP_K)

    def one_device(device_key):
        perm_key, rank_key = jax.random.split(device_key)
        other_ids = jax.random.permutation(perm_key, EXPERTS - 1)
        other_ids = other_ids + (other_ids >= hot_expert).astype(other_ids.dtype)
        tok_rank = jax.random.permutation(rank_key, SEQS_DEV)
        cycle_pos = (tok_rank[:, None] * TOP_K + choice_col[None, :]) % (EXPERTS - 1)
        is_hot = (tok_rank[:, None] < SLOT_CAP) & (choice_col[None, :] == 0)
        return jnp.where(is_hot, hot_expert, other_ids[cycle_pos])

    routes = jax.vmap(one_device)(jax.random.split(dev_key, DP_SIZE))
    return routes.reshape(GROUP_ROWS, TOP_K).astype(jnp.int32)


def setup_inputs(seed: int = 0, part: int = 0) -> dict:
    root_key = jax.random.key(seed)
    part_keys = jax.random.split(jax.random.fold_in(root_key, part), 5)
    weight_keys = jax.random.split(root_key, 15)
    return {
        'hidden': normal_bf16(part_keys[0], (GROUP_ROWS, D_MODEL), 1.0),
        'ckv_cache': normal_bf16(part_keys[1], (GROUP_ROWS, CACHE_LEN, KV_LORA), 1.0),
        'kr_cache': normal_bf16(part_keys[2], (GROUP_ROWS, CACHE_LEN, ROPE_DIM), 1.0),
        'seq_lens': draw_lengths(part_keys[3]),
        'expert_ids': draw_routes(part_keys[4]),
        'attn_gain': draw_gain(weight_keys[0], D_MODEL),
        'kv_gain': draw_gain(weight_keys[1], KV_LORA),
        'moe_gain': draw_gain(weight_keys[2], D_MODEL),
        'w_q': normal_bf16(weight_keys[3], (D_MODEL, HEADS * (NOPE_DIM + ROPE_DIM)), D_MODEL ** -0.5),
        'w_dkv': normal_bf16(weight_keys[4], (D_MODEL, KV_LORA + ROPE_DIM), D_MODEL ** -0.5),
        'w_uk': normal_bf16(weight_keys[5], (HEADS, NOPE_DIM, KV_LORA), NOPE_DIM ** -0.5),
        'w_uv': normal_bf16(weight_keys[6], (HEADS, KV_LORA, V_DIM), 2.0 * KV_LORA ** -0.5),
        'w_o': normal_bf16(weight_keys[7], (HEADS * V_DIM, D_MODEL), 2.0 * (HEADS * V_DIM) ** -0.5),
        'w_router': normal_bf16(weight_keys[8], (D_MODEL, EXPERTS), D_MODEL ** -0.5),
        'shared_gate': normal_bf16(weight_keys[9], (D_MODEL, N_SHARED * FF_DIM), D_MODEL ** -0.5),
        'shared_up': normal_bf16(weight_keys[10], (D_MODEL, N_SHARED * FF_DIM), D_MODEL ** -0.5),
        'shared_down': normal_bf16(weight_keys[11], (N_SHARED * FF_DIM, D_MODEL), (N_SHARED * FF_DIM) ** -0.5),
        'expert_gate': normal_bf16(weight_keys[12], (EXPERTS, D_MODEL, FF_DIM), D_MODEL ** -0.5),
        'expert_up': normal_bf16(weight_keys[13], (EXPERTS, D_MODEL, FF_DIM), D_MODEL ** -0.5),
        'expert_down': normal_bf16(weight_keys[14], (EXPERTS, FF_DIM, D_MODEL), 2.0 * EXPERTS / TOP_K * FF_DIM ** -0.5),
    }


def rms_norm(values, gain_vec):
    vals_f32 = values.astype(jnp.float32)
    inv_rms = lax.rsqrt(jnp.mean(vals_f32 * vals_f32, axis=-1, keepdims=True) + NORM_EPS)
    return (vals_f32 * inv_rms * gain_vec.astype(jnp.float32)).astype(jnp.bfloat16)


def rope_tables(positions):
    inv_freq = ROPE_THETA ** (-2.0 * jnp.arange(ROPE_DIM // 2, dtype=jnp.float32) / ROPE_DIM)
    angles = positions.astype(jnp.float32)[:, None] * inv_freq[None, :]
    return jnp.cos(angles), jnp.sin(angles)


def apply_rope(values, rope_cos, rope_sin):
    half_dim = values.shape[-1] // 2
    first_half = values[..., :half_dim]
    second_half = values[..., half_dim:]
    return jnp.concatenate([first_half * rope_cos - second_half * rope_sin, second_half * rope_cos + first_half * rope_sin], axis=-1)


def attend_one(row_args):
    q_lat_row, q_rot_row, ckv_row, kr_row, seq_len, ckv_new_row, kr_new_row = row_args
    q_lat_f32 = q_lat_row.astype(jnp.float32)
    q_rot_f32 = q_rot_row.astype(jnp.float32)
    ckv_f32 = ckv_row.astype(jnp.float32)
    kr_f32 = kr_row.astype(jnp.float32)
    ckv_new_f32 = ckv_new_row.astype(jnp.float32)
    kr_new_f32 = kr_new_row.astype(jnp.float32)
    scores = (jnp.dot(q_lat_f32, ckv_f32.T) + jnp.dot(q_rot_f32, kr_f32.T)) * SCORE_SCALE
    valid_mask = jnp.arange(CACHE_LEN) < seq_len
    scores = jnp.where(valid_mask[None, :], scores, -jnp.inf)
    new_score = (jnp.dot(q_lat_f32, ckv_new_f32) + jnp.dot(q_rot_f32, kr_new_f32)) * SCORE_SCALE
    top_score = jnp.maximum(jnp.max(scores, axis=-1), new_score)
    exp_cache = jnp.exp(scores - top_score[:, None])
    exp_new = jnp.exp(new_score - top_score)
    denominator = jnp.sum(exp_cache, axis=-1) + exp_new
    prob_cache = (exp_cache / denominator[:, None]).astype(jnp.bfloat16).astype(jnp.float32)
    prob_new = (exp_new / denominator).astype(jnp.bfloat16).astype(jnp.float32)
    o_lat = jnp.dot(prob_cache, ckv_f32) + prob_new[:, None] * ckv_new_f32[None, :]
    return o_lat.astype(jnp.bfloat16)


def routed_experts(moe_in, gate_vals, expert_ids, expert_gate, expert_up, expert_down):
    rows_max = DP_SIZE * SLOT_CAP
    pad_in = jnp.concatenate([moe_in, jnp.zeros((1, D_MODEL), moe_in.dtype)], axis=0)

    def per_expert(acc_out, expert_no):
        picked = expert_ids == expert_no
        gate_tok = jnp.concatenate([jnp.sum(jnp.where(picked, gate_vals, 0.0), axis=-1), jnp.zeros((1,), gate_vals.dtype)])
        row_ids = jnp.nonzero(jnp.any(picked, axis=-1), size=rows_max, fill_value=GROUP_ROWS)[0]
        tok_rows = pad_in[row_ids]
        gate_act = jnp.dot(tok_rows, expert_gate[expert_no], preferred_element_type=jnp.float32)
        up_act = jnp.dot(tok_rows, expert_up[expert_no], preferred_element_type=jnp.float32)
        mid_act = (jax.nn.silu(gate_act) * up_act).astype(jnp.bfloat16)
        expert_out = jnp.dot(mid_act, expert_down[expert_no], preferred_element_type=jnp.float32).astype(jnp.bfloat16)
        acc_out = acc_out.at[row_ids].add(gate_tok[row_ids][:, None] * expert_out.astype(jnp.float32), mode='drop')
        return acc_out, None

    scanned = lax.scan(per_expert, jnp.zeros((GROUP_ROWS, D_MODEL), jnp.float32), jnp.arange(EXPERTS))
    return scanned[0]


def reference(hidden, ckv_cache, kr_cache, seq_lens, expert_ids, attn_gain, kv_gain, moe_gain, w_q, w_dkv, w_uk, w_uv, w_o, w_router, shared_gate, shared_up, shared_down, expert_gate, expert_up, expert_down):
    normed_x = rms_norm(hidden, attn_gain)
    q_all = jnp.dot(normed_x, w_q, preferred_element_type=jnp.float32).astype(jnp.bfloat16).reshape(GROUP_ROWS, HEADS, NOPE_DIM + ROPE_DIM)
    latent_kv = jnp.dot(normed_x, w_dkv, preferred_element_type=jnp.float32)
    ckv_new = rms_norm(latent_kv[:, :KV_LORA], kv_gain)
    rope_cos, rope_sin = rope_tables(seq_lens)
    kr_new = apply_rope(latent_kv[:, KV_LORA:], rope_cos, rope_sin).astype(jnp.bfloat16)
    q_rot = apply_rope(q_all[:, :, NOPE_DIM:].astype(jnp.float32), rope_cos[:, None, :], rope_sin[:, None, :]).astype(jnp.bfloat16)
    q_lat = jnp.einsum('bhn,hnc->bhc', q_all[:, :, :NOPE_DIM].astype(jnp.float32), w_uk.astype(jnp.float32)).astype(jnp.bfloat16)
    o_lat = lax.map(attend_one, (q_lat, q_rot, ckv_cache, kr_cache, seq_lens, ckv_new, kr_new))
    head_out = jnp.einsum('bhc,hcv->bhv', o_lat.astype(jnp.float32), w_uv.astype(jnp.float32)).astype(jnp.bfloat16).reshape(GROUP_ROWS, HEADS * V_DIM)
    resid_out = (hidden.astype(jnp.float32) + jnp.dot(head_out, w_o, preferred_element_type=jnp.float32)).astype(jnp.bfloat16)
    moe_in = rms_norm(resid_out, moe_gain)
    router_prob = jax.nn.softmax(jnp.dot(moe_in, w_router, preferred_element_type=jnp.float32), axis=-1)
    gate_vals = jnp.take_along_axis(router_prob, expert_ids, axis=-1)
    shared_act = (jax.nn.silu(jnp.dot(moe_in, shared_gate, preferred_element_type=jnp.float32)) * jnp.dot(moe_in, shared_up, preferred_element_type=jnp.float32)).astype(jnp.bfloat16)
    shared_out = jnp.dot(shared_act, shared_down, preferred_element_type=jnp.float32)
    routed_out = routed_experts(moe_in, gate_vals, expert_ids, expert_gate, expert_up, expert_down)
    layer_out = (resid_out.astype(jnp.float32) + shared_out + routed_out).astype(jnp.bfloat16)
    return layer_out, ckv_new, kr_new
```

```python
import functools

import jax
import jax.numpy as jnp
from jax import lax
from jax.experimental import pallas as pl
from jax.experimental.pallas import tpu as pltpu
from jax.sharding import PartitionSpec as P

NORM_EPS = 1e-6
ROPE_THETA = 10000.0


def rms_norm(values, gain_vec):
    vals_f32 = values.astype(jnp.float32)
    inv_rms = lax.rsqrt(jnp.mean(vals_f32 * vals_f32, axis=-1, keepdims=True) + NORM_EPS)
    return (vals_f32 * inv_rms * gain_vec.astype(jnp.float32)).astype(jnp.bfloat16)


def rope_tables(positions, rope_dim):
    inv_freq = ROPE_THETA ** (-2.0 * jnp.arange(rope_dim // 2, dtype=jnp.float32) / rope_dim)
    angles = positions.astype(jnp.float32)[:, None] * inv_freq[None, :]
    return jnp.cos(angles), jnp.sin(angles)


def apply_rope(values, rope_cos, rope_sin):
    half_dim = values.shape[-1] // 2
    first_half = values[..., :half_dim]
    second_half = values[..., half_dim:]
    return jnp.concatenate([first_half * rope_cos - second_half * rope_sin, second_half * rope_cos + first_half * rope_sin], axis=-1)


def attention_block(hidden, ckv_cache, kr_cache, seq_lens, attn_gain, kv_gain, w_q, w_dkv, w_uk, w_uv, w_o):
    batch_rows = hidden.shape[0]
    num_heads, nope_dim, value_a8 = w_uk.shape
    rope_dim = kr_cache.shape[-1]
    cache_len = ckv_cache.shape[1]
    score_scale = (nope_dim + rope_dim) ** -0.5
    normed_x = rms_norm(hidden, attn_gain)
    q_all = jnp.dot(normed_x, w_q, preferred_element_type=jnp.float32).astype(jnp.bfloat16).reshape(batch_rows, num_heads, nope_dim + rope_dim)
    latent_kv = jnp.dot(normed_x, w_dkv, preferred_element_type=jnp.float32)
    ckv_new = rms_norm(latent_kv[:, :value_a8], kv_gain)
    rope_cos, rope_sin = rope_tables(seq_lens, rope_dim)
    kr_new = apply_rope(latent_kv[:, value_a8:], rope_cos, rope_sin).astype(jnp.bfloat16)
    q_rot = apply_rope(q_all[:, :, nope_dim:].astype(jnp.float32), rope_cos[:, None, :], rope_sin[:, None, :]).astype(jnp.bfloat16)
    q_lat = jnp.einsum('bhn,hnc->bhc', q_all[:, :, :nope_dim], w_uk, preferred_element_type=jnp.float32).astype(jnp.bfloat16)
    scores = (jnp.einsum('bhc,blc->bhl', q_lat, ckv_cache, preferred_element_type=jnp.float32) + jnp.einsum('bhr,blr->bhl', q_rot, kr_cache, preferred_element_type=jnp.float32)) * score_scale
    valid_mask = jnp.arange(cache_len)[None, None, :] < seq_lens[:, None, None]
    scores = jnp.where(valid_mask, scores, -jnp.inf)
    new_score = (jnp.einsum('bhc,bc->bh', q_lat, ckv_new, preferred_element_type=jnp.float32) + jnp.einsum('bhr,br->bh', q_rot, kr_new, preferred_element_type=jnp.float32)) * score_scale
    top_score = jnp.maximum(jnp.max(scores, axis=-1), new_score)
    exp_cache = jnp.exp(scores - top_score[:, :, None])
    exp_new = jnp.exp(new_score - top_score)
    denominator = jnp.sum(exp_cache, axis=-1) + exp_new
    prob_cache = (exp_cache / denominator[:, :, None]).astype(jnp.bfloat16)
    prob_new = (exp_new / denominator).astype(jnp.bfloat16)
    o_lat = (jnp.einsum('bhl,blc->bhc', prob_cache, ckv_cache, preferred_element_type=jnp.float32) + jnp.einsum('bh,bc->bhc', prob_new, ckv_new, preferred_element_type=jnp.float32)).astype(jnp.bfloat16)
    head_out = jnp.einsum('bhc,hcv->bhv', o_lat, w_uv, preferred_element_type=jnp.float32).astype(jnp.bfloat16).reshape(batch_rows, -1)
    resid_out = (hidden.astype(jnp.float32) + jnp.dot(head_out, w_o, preferred_element_type=jnp.float32)).astype(jnp.bfloat16)
    return resid_out, ckv_new, kr_new


MESH_ID = pl.DeviceIdType.MESH


def silu(value):
    return value * (1.0 / (1.0 + jnp.exp(-value)))


def moe_kernel(dims, resid_ref, ids_ref, gain_ref, router_ref, sgate_hbm, sup_hbm, sdown_hbm, egate_hbm, eup_hbm, edown_hbm, out_ref,
               ublk, tokx, midx, send, recv, acc, table, tail, gu_buf, dn_buf,
               gu_sem, dn_sem, us_sem, ur_sem, ys_sem, yr_sem):
    group, experts_dev, experts, cap, depth, rep_axis, dp_axis = dims
    rows, width = resid_ref.shape
    half = rows // 2
    ff = gu_buf.shape[-1]
    n_shared = sgate_hbm.shape[-1] // ff
    steps = experts_dev + n_shared
    slot16 = 16
    slots = group * slot16
    main = send.shape[-1]
    blk = main // 3
    top_k = ids_ref.shape[-1]
    lanes = 128
    me = lax.axis_index(dp_axis)
    chips = group // 2
    core = lax.rem(me, 2)
    chip = me // 2
    partner = chip * 2 + (1 - core)
    left = lax.rem(chip + chips - 1, chips) * 2 + core
    right = lax.rem(chip + 1, chips) * 2 + core
    far = lax.rem(chip + 2, chips) * 2 + core

    def weights_gu(step, which, hbm, shared_hbm, action):
        slot = lax.rem(step, depth)

        @pl.when(step < experts_dev)
        def _():
            getattr(pltpu.make_async_copy(hbm.at[step], gu_buf.at[slot, which], gu_sem.at[slot, which]), action)()

        @pl.when(step >= experts_dev)
        def _():
            cols = pl.ds(pl.multiple_of((step - experts_dev) * ff, 128), ff)
            getattr(pltpu.make_async_copy(shared_hbm.at[:, cols], gu_buf.at[slot, which], gu_sem.at[slot, which]), action)()

    def weights_dn(step, action):
        slot = lax.rem(step, depth)

        @pl.when(step < experts_dev)
        def _():
            getattr(pltpu.make_async_copy(edown_hbm.at[step], dn_buf.at[slot], dn_sem.at[slot]), action)()

        @pl.when(step >= experts_dev)
        def _():
            cols = pl.ds(pl.multiple_of((step - experts_dev) * ff, 128), ff)
            getattr(pltpu.make_async_copy(sdown_hbm.at[cols], dn_buf.at[slot], dn_sem.at[slot]), action)()

    def fetch(step):
        weights_gu(step, 0, egate_hbm, sgate_hbm, "start")
        weights_gu(step, 1, eup_hbm, sup_hbm, "start")

    for first in range(depth):
        fetch(jnp.int32(first))
        weights_dn(jnp.int32(first), "start")

    barrier = pltpu.get_barrier_semaphore()
    for k in range(1, group):
        pl.semaphore_signal(barrier, inc=1, device_id={dp_axis: lax.rem(me + k, group)}, device_id_type=MESH_ID)

    resid = resid_ref[...].astype(jnp.float32)
    inv = lax.rsqrt(jnp.mean(resid * resid, axis=-1, keepdims=True) + NORM_EPS)
    u = (resid * inv * gain_ref[...].astype(jnp.float32)).astype(jnp.bfloat16)
    lane = lax.broadcasted_iota(jnp.int32, (rows, lanes), 1)
    picked = jnp.zeros((rows, lanes), jnp.bool_)
    for k in range(top_k):
        picked = picked | (ids_ref[:, k:k + 1] == lane)
    lower = (lax.broadcasted_iota(jnp.int32, (rows, rows), 1) < lax.broadcasted_iota(jnp.int32, (rows, rows), 0)).astype(jnp.float32).astype(jnp.bfloat16)
    rank = jnp.dot(lower, jnp.where(picked, 1.0, 0.0).astype(jnp.bfloat16), preferred_element_type=jnp.float32)
    codes = jnp.where(picked, rank, -1.0).astype(jnp.bfloat16)
    for h in range(2):
        ublk[me, h, :, :width] = u[h * half:(h + 1) * half]
        ublk[me, h, :, width:] = codes[h * half:(h + 1) * half]
    logits = jnp.dot(u, router_ref[...], preferred_element_type=jnp.float32)
    logits = logits - jnp.max(logits, axis=-1, keepdims=True)
    expl = jnp.exp(logits)
    prob = expl / jnp.sum(expl, axis=-1, keepdims=True)
    prob = jnp.concatenate([prob, jnp.zeros((rows, lanes - experts), jnp.float32)], axis=-1)
    p0 = prob.astype(jnp.bfloat16)
    rest = prob - p0.astype(jnp.float32)
    p1 = rest.astype(jnp.bfloat16)
    p2 = (rest - p1.astype(jnp.float32)).astype(jnp.bfloat16)
    table[0] = codes
    table[1] = p0
    table[2] = p1
    table[3] = p2
    acc[...] = resid

    pl.semaphore_wait(barrier, group - 1)

    def block_copy(block, h, dest, sem_no):
        return pltpu.make_async_remote_copy(src_ref=ublk.at[block, h], dst_ref=ublk.at[block, h], send_sem=us_sem.at[sem_no], recv_sem=ur_sem.at[block, h], device_id={dp_axis: dest}, device_id_type=MESH_ID)

    copies = []

    def send_block(block, h, dest):
        copy = block_copy(block, h, dest, len(copies))
        copy.start()
        copies.append(copy)

    def arrived(block, h):
        block_copy(block, h, partner, 0).wait_recv()

    send_block(me, 0, right)
    send_block(me, 1, left)
    send_block(me, 1, right)
    send_block(me, 0, left)
    send_block(me, 0, partner)
    send_block(me, 1, partner)
    arrived(left, 0)
    send_block(left, 0, right)
    send_block(left, 0, partner)
    arrived(right, 1)
    send_block(right, 1, left)
    send_block(right, 1, partner)
    arrived(left, 1)
    send_block(left, 1, partner)
    arrived(right, 0)
    send_block(right, 0, partner)
    arrived(far, 0)
    send_block(far, 0, partner)
    arrived(far, 1)
    send_block(far, 1, partner)
    for block in (partner, lax.rem(left + 1 - 2 * core + group, group), lax.rem(right + 1 - 2 * core + group, group), lax.rem(far + 1 - 2 * core + group, group)):
        for h in range(2):
            arrived(block, h)

    row_i = lax.broadcasted_iota(jnp.int32, (lanes, slots), 0)
    col_i = lax.broadcasted_iota(jnp.int32, (lanes, slots), 1)

    def return_copy(step, dest):
        return pltpu.make_async_remote_copy(src_ref=send.at[step, dest], dst_ref=recv.at[step, me], send_sem=ys_sem.at[step, dest], recv_sem=yr_sem.at[step, me], device_id={dp_axis: dest}, device_id_type=MESH_ID)

    def arrival(step, source):
        return pltpu.make_async_remote_copy(src_ref=send.at[step, source], dst_ref=recv.at[step, source], send_sem=ys_sem.at[step, source], recv_sem=yr_sem.at[step, source], device_id={dp_axis: source}, device_id_type=MESH_ID)

    def gather_rows(step):
        pick = (row_i == me * experts_dev + step).astype(jnp.float32).astype(jnp.bfloat16)
        code_all = ublk[:, :, :, width:].reshape(group * rows, lanes)
        code_b = jnp.dot(code_all, pick, preferred_element_type=jnp.float32)
        tok = lax.broadcasted_iota(jnp.int32, (group * rows, slots), 0)
        col = lax.broadcasted_iota(jnp.int32, (group * rows, slots), 1)
        hit = (code_b == lax.rem(col, slot16).astype(jnp.float32)) & (tok // rows == col // slot16)
        place = jnp.where(hit, 1.0, 0.0).astype(jnp.bfloat16)
        for c0 in range(0, width, 512):
            rows_u = ublk[:, :, :, c0:c0 + 512].reshape(group * rows, 512)
            picked_rows = lax.dot_general(place, rows_u, (((0,), (0,)), ((), ())), preferred_element_type=jnp.float32)
            tokx[:, c0:c0 + 512] = picked_rows.astype(jnp.bfloat16)

    def pack_block(y_main, q):
        y_main = y_main.reshape(group, 2, 8, blk)
        y_tail = tail[...].reshape(group, 2, 8, blk)
        sub = lax.broadcasted_iota(jnp.int32, (group, 8, blk), 1)
        part = y_tail[:, 1 if q == 2 else 0]
        if q != 1:
            part = pltpu.roll(part.reshape(group * 8, blk).reshape(group, 8, blk), 4, 1)
        low = jnp.where(sub >= 4, part, y_main[:, 1])
        return jnp.concatenate([y_main[:, 0], low], axis=1).astype(jnp.bfloat16)

    def combine(step):
        for k in range(1, group):
            arrival(step, lax.rem(me + k, group)).wait_recv()
        spread = (row_i == (col_i // slot16) * experts_dev + step).astype(jnp.float32).astype(jnp.bfloat16)
        wide = jnp.dot(table[...].reshape(4 * rows, lanes), spread, preferred_element_type=jnp.float32)
        code_b = wide[:rows]
        slot_i = lax.rem(lax.broadcasted_iota(jnp.int32, (rows, slots), 1), slot16)
        slot_f = slot_i.astype(jnp.float32)
        for q in range(3):
            hits = [code_b == slot_f, (slot_i >= cap) & (code_b == slot_f - cap + 4 * q)]
            lhs = jnp.concatenate([jnp.where(hit, wide[p * rows:(p + 1) * rows], 0.0) for hit in hits for p in (1, 2, 3)], axis=0).astype(jnp.bfloat16)
            y_blk = recv[step, :, :, q * blk:(q + 1) * blk].reshape(slots, blk)
            res = jnp.dot(lhs, y_blk, preferred_element_type=jnp.float32)
            acc[:, q * blk:(q + 1) * blk] += res[:rows] + (res[rows:2 * rows] + res[2 * rows:3 * rows])
            acc[:, main:] += res[3 * rows:4 * rows] + (res[4 * rows:5 * rows] + res[5 * rows:])

    def one_step(step, carry):
        slot = lax.rem(step, depth)
        is_routed = step < experts_dev

        @pl.when(is_routed)
        def _():
            gather_rows(step)

        @pl.when(step == experts_dev)
        def _():
            tokx[:rows] = ublk[me, :, :, :width].reshape(rows, width)
            tokx[rows:] = jnp.zeros((slots - rows, width), jnp.bfloat16)

        weights_gu(step, 0, egate_hbm, sgate_hbm, "wait")
        weights_gu(step, 1, eup_hbm, sup_hbm, "wait")
        for c0 in range(0, ff, 512):
            c1 = min(c0 + 512, ff)
            gate_act = jnp.dot(tokx[...], gu_buf[slot, 0, :, c0:c1], preferred_element_type=jnp.float32)
            up_act = jnp.dot(tokx[...], gu_buf[slot, 1, :, c0:c1], preferred_element_type=jnp.float32)
            midx[:, c0:c1] = (silu(gate_act) * up_act).astype(jnp.bfloat16)

        @pl.when(step + depth < steps)
        def _():
            fetch(step + depth)

        weights_dn(step, "wait")
        tail[...] = jnp.dot(midx[...], dn_buf[slot, :, main:], preferred_element_type=jnp.float32)

        @pl.when(step >= experts_dev)
        def _():
            acc[:, main:] += tail[:rows]

        for q in range(3):
            y_main = jnp.dot(midx[...], dn_buf[slot, :, q * blk:(q + 1) * blk], preferred_element_type=jnp.float32)

            @pl.when(is_routed)
            def _():
                send[step, :, :, q * blk:(q + 1) * blk] = pack_block(y_main, q)

            @pl.when(step >= experts_dev)
            def _():
                acc[:, q * blk:(q + 1) * blk] += y_main[:rows]

        @pl.when(step + depth < steps)
        def _():
            weights_dn(step + depth, "start")

        @pl.when(is_routed)
        def _():
            recv[step, me] = send[step, me]
            for k in (4, 3, 5, 2, 6, 1, 7):
                return_copy(step, lax.rem(me + k, group)).start()

        @pl.when(step >= steps - experts_dev)
        def _():
            combine(step - (steps - experts_dev))

        return carry

    lax.fori_loop(0, steps, one_step, 0)
    out_ref[...] = acc[...].astype(out_ref.dtype)

    for copy in copies:
        copy.wait_send()

    def drain(step, carry):
        for k in range(1, group):
            return_copy(step, lax.rem(me + k, group)).wait_send()
        return carry

    lax.fori_loop(0, experts_dev, drain, 0)


def moe_layer(resid_out, expert_ids, cap, group, moe_gain, w_router, shared_gate, shared_up, shared_down, expert_gate, expert_up, expert_down):
    rows, width = resid_out.shape
    experts_dev, _, ff = expert_gate.shape
    experts = w_router.shape[1]
    depth = 3
    main = 3 * width // 4
    slots = group * 16
    dims = (group, experts_dev, experts, cap, depth, 'rep', 'dp')
    vmem = pl.BlockSpec(memory_space=pltpu.VMEM)
    hbm = pl.BlockSpec(memory_space=pl.ANY)
    return pl.pallas_call(
        functools.partial(moe_kernel, dims),
        out_shape=jax.ShapeDtypeStruct((rows, width), jnp.bfloat16),
        in_specs=[vmem] * 4 + [hbm] * 6,
        out_specs=vmem,
        scratch_shapes=[
            pltpu.VMEM((group, 2, rows // 2, width + 128), jnp.bfloat16),
            pltpu.VMEM((slots, width), jnp.bfloat16),
            pltpu.VMEM((slots, ff), jnp.bfloat16),
            pltpu.VMEM((experts_dev, group, 16, main), jnp.bfloat16),
            pltpu.VMEM((experts_dev, group, 16, main), jnp.bfloat16),
            pltpu.VMEM((rows, width), jnp.float32),
            pltpu.VMEM((4, rows, 128), jnp.bfloat16),
            pltpu.VMEM((slots, width - main), jnp.float32),
            pltpu.VMEM((depth, 2, width, ff), jnp.bfloat16),
            pltpu.VMEM((depth, ff, width), jnp.bfloat16),
            pltpu.SemaphoreType.DMA((depth, 2)),
            pltpu.SemaphoreType.DMA((depth,)),
            pltpu.SemaphoreType.DMA((14,)),
            pltpu.SemaphoreType.DMA((group, 2)),
            pltpu.SemaphoreType.DMA((experts_dev, group)),
            pltpu.SemaphoreType.DMA((experts_dev, group)),
        ],
        compiler_params=pltpu.CompilerParams(collective_id=0, has_side_effects=True, vmem_limit_bytes=67043328),
        name='moe_layer',
    )(resid_out, expert_ids, moe_gain.reshape(1, -1), w_router, shared_gate, shared_up, shared_down, expert_gate, expert_up, expert_down)


def solution(mesh):
    row_spec = P(('rep', 'dp'))
    full_spec = P()
    expert_spec = P('dp')

    def device_step(hidden, ckv_cache, kr_cache, seq_lens, expert_ids, attn_gain, kv_gain, moe_gain, w_q, w_dkv, w_uk, w_uv, w_o, w_router, shared_gate, shared_up, shared_down, expert_gate, expert_up, expert_down):
        capacity = max(2, 2 * hidden.shape[0] * expert_ids.shape[1] // w_router.shape[1])
        resid_out, ckv_new, kr_new = attention_block(hidden, ckv_cache, kr_cache, seq_lens, attn_gain, kv_gain, w_q, w_dkv, w_uk, w_uv, w_o)
        layer_out = moe_layer(resid_out, expert_ids, capacity, mesh.shape['dp'], moe_gain, w_router, shared_gate, shared_up, shared_down, expert_gate, expert_up, expert_down)
        return layer_out, ckv_new, kr_new

    in_specs = (row_spec,) * 5 + (full_spec,) * 12 + (expert_spec,) * 3
    return jax.shard_map(device_step, mesh=mesh, in_specs=in_specs, out_specs=(row_spec, row_spec, row_spec), check_vma=False)
```

```python
import functools
import math

import jax
import jax.numpy as jnp
from jax import lax
from jax.experimental import pallas as pl
from jax.experimental.pallas import tpu as pltpu
from jax.sharding import PartitionSpec as P

NORM_EPS = 1e-6
ROPE_THETA = 10000.0


MESH_ID = pl.DeviceIdType.MESH


def silu(value):
    return value * (1.0 / (1.0 + jnp.exp(-value)))


def moe_kernel(dims, resid_ref, ids_ref, gain_ref, router_ref, sgate_hbm, sup_hbm, sdown_hbm, egate_hbm, eup_hbm, edown_hbm, out_ref,
               ublk, tokx, midx, send, recv, acc, table, tail, gu_buf, dn_buf,
               gu_sem, dn_sem, us_sem, ur_sem, ys_sem, yr_sem):
    group, experts_dev, experts, cap, depth, rep_axis, dp_axis = dims
    rows, width = resid_ref.shape
    half = rows // 2
    ff = gu_buf.shape[-1]
    n_shared = sgate_hbm.shape[-1] // ff
    steps = experts_dev + n_shared
    slot16 = 16
    slots = group * slot16
    main = send.shape[-1]
    blk = main // 3
    top_k = ids_ref.shape[-1]
    lanes = 128
    me = lax.axis_index(dp_axis)
    chips = group // 2
    core = lax.rem(me, 2)
    chip = me // 2
    partner = chip * 2 + (1 - core)
    left = lax.rem(chip + chips - 1, chips) * 2 + core
    right = lax.rem(chip + 1, chips) * 2 + core
    far = lax.rem(chip + 2, chips) * 2 + core

    def weights_gu(step, which, hbm, shared_hbm, action):
        slot = lax.rem(step, depth)

        @pl.when(step < experts_dev)
        def _():
            getattr(pltpu.make_async_copy(hbm.at[step], gu_buf.at[slot, which], gu_sem.at[slot, which]), action)()

        @pl.when(step >= experts_dev)
        def _():
            cols = pl.ds(pl.multiple_of((step - experts_dev) * ff, 128), ff)
            getattr(pltpu.make_async_copy(shared_hbm.at[:, cols], gu_buf.at[slot, which], gu_sem.at[slot, which]), action)()

    def weights_dn(step, action):
        slot = lax.rem(step, depth)

        @pl.when(step < experts_dev)
        def _():
            getattr(pltpu.make_async_copy(edown_hbm.at[step], dn_buf.at[slot], dn_sem.at[slot]), action)()

        @pl.when(step >= experts_dev)
        def _():
            cols = pl.ds(pl.multiple_of((step - experts_dev) * ff, 128), ff)
            getattr(pltpu.make_async_copy(sdown_hbm.at[cols], dn_buf.at[slot], dn_sem.at[slot]), action)()

    def fetch(step):
        weights_gu(step, 0, egate_hbm, sgate_hbm, "start")
        weights_gu(step, 1, eup_hbm, sup_hbm, "start")

    for first in range(depth):
        fetch(jnp.int32(first))
        weights_dn(jnp.int32(first), "start")

    barrier = pltpu.get_barrier_semaphore()
    for k in range(1, group):
        pl.semaphore_signal(barrier, inc=1, device_id={dp_axis: lax.rem(me + k, group)}, device_id_type=MESH_ID)

    resid = resid_ref[...].astype(jnp.float32)
    inv = lax.rsqrt(jnp.mean(resid * resid, axis=-1, keepdims=True) + NORM_EPS)
    u = (resid * inv * gain_ref[...].astype(jnp.float32)).astype(jnp.bfloat16)
    lane = lax.broadcasted_iota(jnp.int32, (rows, lanes), 1)
    picked = jnp.zeros((rows, lanes), jnp.bool_)
    for k in range(top_k):
        picked = picked | (ids_ref[:, k:k + 1] == lane)
    lower = (lax.broadcasted_iota(jnp.int32, (rows, rows), 1) < lax.broadcasted_iota(jnp.int32, (rows, rows), 0)).astype(jnp.float32).astype(jnp.bfloat16)
    rank = jnp.dot(lower, jnp.where(picked, 1.0, 0.0).astype(jnp.bfloat16), preferred_element_type=jnp.float32)
    codes = jnp.where(picked, rank, -1.0).astype(jnp.bfloat16)
    for h in range(2):
        ublk[me, h, :, :width] = u[h * half:(h + 1) * half]
        ublk[me, h, :, width:] = codes[h * half:(h + 1) * half]
    logits = lax.dot_general(u, router_ref[...], (((1,), (1,)), ((), ())), preferred_element_type=jnp.float32)
    logits = logits - jnp.max(logits, axis=-1, keepdims=True)
    expl = jnp.exp(logits)
    prob = expl / jnp.sum(expl, axis=-1, keepdims=True)
    prob = jnp.concatenate([prob, jnp.zeros((rows, lanes - experts), jnp.float32)], axis=-1)
    p0 = prob.astype(jnp.bfloat16)
    rest = prob - p0.astype(jnp.float32)
    p1 = rest.astype(jnp.bfloat16)
    p2 = (rest - p1.astype(jnp.float32)).astype(jnp.bfloat16)
    table[0] = codes
    table[1] = p0
    table[2] = p1
    table[3] = p2
    acc[...] = resid

    pl.semaphore_wait(barrier, group - 1)

    def block_copy(block, h, dest, sem_no):
        return pltpu.make_async_remote_copy(src_ref=ublk.at[block, h], dst_ref=ublk.at[block, h], send_sem=us_sem.at[sem_no], recv_sem=ur_sem.at[block, h], device_id={dp_axis: dest}, device_id_type=MESH_ID)

    copies = []

    def send_block(block, h, dest):
        copy = block_copy(block, h, dest, len(copies))
        copy.start()
        copies.append(copy)

    def arrived(block, h):
        block_copy(block, h, partner, 0).wait_recv()

    send_block(me, 0, right)
    send_block(me, 1, left)
    send_block(me, 1, right)
    send_block(me, 0, left)
    send_block(me, 0, partner)
    send_block(me, 1, partner)
    arrived(left, 0)
    send_block(left, 0, right)
    send_block(left, 0, partner)
    arrived(right, 1)
    send_block(right, 1, left)
    send_block(right, 1, partner)
    arrived(left, 1)
    send_block(left, 1, partner)
    arrived(right, 0)
    send_block(right, 0, partner)
    arrived(far, 0)
    send_block(far, 0, partner)
    arrived(far, 1)
    send_block(far, 1, partner)
    for block in (partner, lax.rem(left + 1 - 2 * core + group, group), lax.rem(right + 1 - 2 * core + group, group), lax.rem(far + 1 - 2 * core + group, group)):
        for h in range(2):
            arrived(block, h)

    row_i = lax.broadcasted_iota(jnp.int32, (lanes, slots), 0)
    col_i = lax.broadcasted_iota(jnp.int32, (lanes, slots), 1)

    def return_copy(step, dest):
        return pltpu.make_async_remote_copy(src_ref=send.at[step, dest], dst_ref=recv.at[step, me], send_sem=ys_sem.at[step, dest], recv_sem=yr_sem.at[step, me], device_id={dp_axis: dest}, device_id_type=MESH_ID)

    def arrival(step, source):
        return pltpu.make_async_remote_copy(src_ref=send.at[step, source], dst_ref=recv.at[step, source], send_sem=ys_sem.at[step, source], recv_sem=yr_sem.at[step, source], device_id={dp_axis: source}, device_id_type=MESH_ID)

    def gather_rows(step):
        pick = (row_i == me * experts_dev + step).astype(jnp.float32).astype(jnp.bfloat16)
        code_all = ublk[:, :, :, width:].reshape(group * rows, lanes)
        code_b = jnp.dot(code_all, pick, preferred_element_type=jnp.float32)
        tok = lax.broadcasted_iota(jnp.int32, (group * rows, slots), 0)
        col = lax.broadcasted_iota(jnp.int32, (group * rows, slots), 1)
        hit = (code_b == lax.rem(col, slot16).astype(jnp.float32)) & (tok // rows == col // slot16)
        place = jnp.where(hit, 1.0, 0.0).astype(jnp.bfloat16)
        for c0 in range(0, width, 512):
            rows_u = ublk[:, :, :, c0:c0 + 512].reshape(group * rows, 512)
            picked_rows = lax.dot_general(place, rows_u, (((0,), (0,)), ((), ())), preferred_element_type=jnp.float32)
            tokx[:, c0:c0 + 512] = picked_rows.astype(jnp.bfloat16)

    def pack_block(y_main, q):
        y_main = y_main.reshape(group, 2, 8, blk)
        y_tail = tail[...].reshape(group, 2, 8, blk)
        sub = lax.broadcasted_iota(jnp.int32, (group, 8, blk), 1)
        part = y_tail[:, 1 if q == 2 else 0]
        if q != 1:
            part = pltpu.roll(part.reshape(group * 8, blk).reshape(group, 8, blk), 4, 1)
        low = jnp.where(sub >= 4, part, y_main[:, 1])
        return jnp.concatenate([y_main[:, 0], low], axis=1).astype(jnp.bfloat16)

    def combine(step):
        for k in range(1, group):
            arrival(step, lax.rem(me + k, group)).wait_recv()
        spread = (row_i == (col_i // slot16) * experts_dev + step).astype(jnp.float32).astype(jnp.bfloat16)
        wide = jnp.dot(table[...].reshape(4 * rows, lanes), spread, preferred_element_type=jnp.float32)
        code_b = wide[:rows]
        slot_i = lax.rem(lax.broadcasted_iota(jnp.int32, (rows, slots), 1), slot16)
        slot_f = slot_i.astype(jnp.float32)
        for q in range(3):
            hits = [code_b == slot_f, (slot_i >= cap) & (code_b == slot_f - cap + 4 * q)]
            lhs = jnp.concatenate([jnp.where(hit, wide[p * rows:(p + 1) * rows], 0.0) for hit in hits for p in (1, 2, 3)], axis=0).astype(jnp.bfloat16)
            y_blk = recv[step, :, :, q * blk:(q + 1) * blk].reshape(slots, blk)
            res = jnp.dot(lhs, y_blk, preferred_element_type=jnp.float32)
            acc[:, q * blk:(q + 1) * blk] += res[:rows] + (res[rows:2 * rows] + res[2 * rows:3 * rows])
            acc[:, main:] += res[3 * rows:4 * rows] + (res[4 * rows:5 * rows] + res[5 * rows:])

    def one_step(step, carry):
        slot = lax.rem(step, depth)
        is_routed = step < experts_dev

        @pl.when(is_routed)
        def _():
            gather_rows(step)

        @pl.when(step == experts_dev)
        def _():
            tokx[:rows] = ublk[me, :, :, :width].reshape(rows, width)
            tokx[rows:] = jnp.zeros((slots - rows, width), jnp.bfloat16)

        weights_gu(step, 0, egate_hbm, sgate_hbm, "wait")
        weights_gu(step, 1, eup_hbm, sup_hbm, "wait")
        for c0 in range(0, ff, 512):
            c1 = min(c0 + 512, ff)
            gate_act = jnp.dot(tokx[...], gu_buf[slot, 0, :, c0:c1], preferred_element_type=jnp.float32)
            up_act = jnp.dot(tokx[...], gu_buf[slot, 1, :, c0:c1], preferred_element_type=jnp.float32)
            midx[:, c0:c1] = (silu(gate_act) * up_act).astype(jnp.bfloat16)

        @pl.when(step + depth < steps)
        def _():
            fetch(step + depth)

        weights_dn(step, "wait")
        tail[...] = jnp.dot(midx[...], dn_buf[slot, :, main:], preferred_element_type=jnp.float32)

        @pl.when(step >= experts_dev)
        def _():
            acc[:, main:] += tail[:rows]

        for q in range(3):
            y_main = jnp.dot(midx[...], dn_buf[slot, :, q * blk:(q + 1) * blk], preferred_element_type=jnp.float32)

            @pl.when(is_routed)
            def _():
                send[step, :, :, q * blk:(q + 1) * blk] = pack_block(y_main, q)

            @pl.when(step >= experts_dev)
            def _():
                acc[:, q * blk:(q + 1) * blk] += y_main[:rows]

        @pl.when(step + depth < steps)
        def _():
            weights_dn(step + depth, "start")

        @pl.when(is_routed)
        def _():
            recv[step, me] = send[step, me]
            for k in (4, 3, 5, 2, 6, 1, 7):
                return_copy(step, lax.rem(me + k, group)).start()

        @pl.when(step >= steps - experts_dev)
        def _():
            combine(step - (steps - experts_dev))

        return carry

    lax.fori_loop(0, steps, one_step, 0)
    out_ref[...] = acc[...].astype(out_ref.dtype)

    for copy in copies:
        copy.wait_send()

    def drain(step, carry):
        for k in range(1, group):
            return_copy(step, lax.rem(me + k, group)).wait_send()
        return carry

    lax.fori_loop(0, experts_dev, drain, 0)


def moe_layer(resid_out, expert_ids, cap, group, moe_gain, w_router, shared_gate, shared_up, shared_down, expert_gate, expert_up, expert_down):
    rows, width = resid_out.shape
    experts_dev, _, ff = expert_gate.shape
    experts = w_router.shape[1]
    depth = 3
    main = 3 * width // 4
    slots = group * 16
    dims = (group, experts_dev, experts, cap, depth, 'rep', 'dp')
    vmem = pl.BlockSpec(memory_space=pltpu.VMEM)
    hbm = pl.BlockSpec(memory_space=pl.ANY)
    return pl.pallas_call(
        functools.partial(moe_kernel, dims),
        out_shape=jax.ShapeDtypeStruct((rows, width), jnp.bfloat16),
        in_specs=[vmem] * 4 + [hbm] * 6,
        out_specs=vmem,
        scratch_shapes=[
            pltpu.VMEM((group, 2, rows // 2, width + 128), jnp.bfloat16),
            pltpu.VMEM((slots, width), jnp.bfloat16),
            pltpu.VMEM((slots, ff), jnp.bfloat16),
            pltpu.VMEM((experts_dev, group, 16, main), jnp.bfloat16),
            pltpu.VMEM((experts_dev, group, 16, main), jnp.bfloat16),
            pltpu.VMEM((rows, width), jnp.float32),
            pltpu.VMEM((4, rows, 128), jnp.bfloat16),
            pltpu.VMEM((slots, width - main), jnp.float32),
            pltpu.VMEM((depth, 2, width, ff), jnp.bfloat16),
            pltpu.VMEM((depth, ff, width), jnp.bfloat16),
            pltpu.SemaphoreType.DMA((depth, 2)),
            pltpu.SemaphoreType.DMA((depth,)),
            pltpu.SemaphoreType.DMA((14,)),
            pltpu.SemaphoreType.DMA((group, 2)),
            pltpu.SemaphoreType.DMA((experts_dev, group)),
            pltpu.SemaphoreType.DMA((experts_dev, group)),
        ],
        compiler_params=pltpu.CompilerParams(collective_id=0, has_side_effects=True, vmem_limit_bytes=67043328),
        name='moe_layer',
    )(resid_out, expert_ids, moe_gain.reshape(1, -1), w_router.T, shared_gate, shared_up, shared_down, expert_gate, expert_up, expert_down)


def attention_phase(refs, hooks):
    (hidden_ref, lens_ref, again_ref, kgain_ref, ckv_hbm, krt_hbm, wq_hbm, dkvt_hbm, uk_hbm, uv_hbm, wo_hbm, cnew_ref, knew_ref,
     tokx, uvbuf, gu_buf, dn_buf, qlat, qrot, newc, newk, pos, a_sem, c_sem) = refs
    rows, width = hidden_ref.shape
    lora = qlat.shape[-1]
    heads = qlat.shape[1]
    rope_dim = krt_hbm.shape[0] // rows
    length = krt_hbm.shape[1]
    nope = uk_hbm.shape[0] // heads
    head_dim = nope + rope_dim
    qcols = wq_hbm.shape[1] // 4
    four = 4 * length
    value_dim = uv_hbm.shape[1]
    scale = head_dim ** -0.5
    lanes = 128
    lat0 = dn_buf.shape[1] - four
    lat1 = dkvt_hbm.shape[0] - lat0
    cache_cols = slice(qcols, qcols + lora)
    kr_cols = slice(width // 2, width // 2 + length)

    def query_copy(i):
        return pltpu.make_async_copy(wq_hbm.at[:, i * qcols:(i + 1) * qcols], gu_buf.at[i // 2, i % 2, :, 0:qcols], a_sem.at[i])

    latent_copies = [
        pltpu.make_async_copy(dkvt_hbm.at[0:lat0], dn_buf.at[1, four:four + lat0], a_sem.at[4]),
        pltpu.make_async_copy(dkvt_hbm.at[lat0:lat0 + lat1], dn_buf.at[2, four:four + lat1], a_sem.at[5]),
    ]
    uk_copy = pltpu.make_async_copy(uk_hbm, gu_buf.at[0, 1, :, cache_cols], a_sem.at[6])
    kr_copies = [pltpu.make_async_copy(krt_hbm.at[w * width:(w + 1) * width], gu_buf.at[2, w, :, kr_cols], a_sem.at[7 + w]) for w in range(2)]
    out_copies = [pltpu.make_async_copy(wo_hbm.at[:, w * (width // 2):(w + 1) * (width // 2)], gu_buf.at[2, w, :, 0:width // 2], a_sem.at[9 + w]) for w in range(2)]
    uv_copies = [pltpu.make_async_copy(uv_hbm.at[i * 2 * lora:(i + 1) * 2 * lora], uvbuf.at[:, i * value_dim:(i + 1) * value_dim], a_sem.at[11 + i]) for i in range(heads // 2)]
    wide_seqs = 48

    def cache_copy(n):
        if n >= 12:
            w, r = (n - 12) // 2, n % 2
            return pltpu.make_async_copy(ckv_hbm.at[n * four:(n + 1) * four], gu_buf.at[1, w, r * four:(r + 1) * four, cache_cols], c_sem.at[n])
        return pltpu.make_async_copy(ckv_hbm.at[n * four:(n + 1) * four], dn_buf.at[n // 4, 0:four, (n % 4) * lora:(n % 4 + 1) * lora], c_sem.at[n])

    query_copy(0).start()
    for copy in latent_copies:
        copy.start()
    uk_copy.start()
    for i in range(1, 4):
        query_copy(i).start()

    lane = lax.broadcasted_iota(jnp.int32, (rows, lanes), 1)
    hidden = hidden_ref[...].astype(jnp.float32)
    inv = lax.rsqrt(jnp.mean(hidden * hidden, axis=-1, keepdims=True) + NORM_EPS)
    tokx[0:rows] = (hidden * inv * again_ref[...].astype(jnp.float32)).astype(jnp.bfloat16)
    for b in range(rows):
        pos[b:b + 1, :] = jnp.full((1, lanes), lens_ref[b], jnp.int32).astype(jnp.float32)
    quarter = lax.rem(lane, rope_dim // 2).astype(jnp.float32)
    angle = pos[...] * jnp.exp(quarter * (-2.0 / rope_dim * math.log(ROPE_THETA)))
    rope_cos = jnp.cos(angle)
    low_half = lax.rem(lane, rope_dim) < rope_dim // 2
    rope_sin = jnp.where(low_half, -jnp.sin(angle), jnp.sin(angle))

    def rope(value):
        swapped = jnp.where(low_half, pltpu.roll(value, lanes - rope_dim // 2, 1), pltpu.roll(value, rope_dim // 2, 1))
        return value * rope_cos + swapped * rope_sin

    first_half = lane < rope_dim
    for i in range(4):
        query_copy(i).wait()
        q_cols = jnp.dot(tokx[0:rows], gu_buf[i // 2, i % 2, :, 0:qcols], preferred_element_type=jnp.float32)
        q_cols = q_cols.astype(jnp.bfloat16).astype(jnp.float32)
        if i == 0:
            for n in range(12, 16):
                cache_copy(n).start()
            for copy in kr_copies:
                copy.start()
            uk_copy.wait()
        if i == 1:
            for n in range(4):
                cache_copy(n).start()
        for pair in range(qcols // (2 * head_dim)):
            base = pair * 2 * head_dim
            tile0, tile1, tile2 = (q_cols[:, base + k * lanes:base + (k + 1) * lanes] for k in range(3))
            head = i * (qcols // head_dim) + 2 * pair
            nopes = (tile0, pltpu.roll(jnp.where(first_half, tile2, tile1), lanes // 2, 1))
            turned = rope(jnp.where(first_half, tile1, tile2))
            for odd in range(2):
                h = head + odd
                qrot[:, h, :] = pltpu.roll(turned, lanes // 2, 1) if odd else turned
                uk_head = gu_buf[0, 1, h * nope:(h + 1) * nope, cache_cols]
                qlat[:, h, :] = jnp.dot(nopes[odd].astype(jnp.bfloat16), uk_head, preferred_element_type=jnp.float32)
    for n in range(4, 12):
        cache_copy(n).start()
    for copy in uv_copies + out_copies:
        copy.start()
    hooks[0]()

    for copy in latent_copies:
        copy.wait()
    contract = (((1,), (1,)), ((), ()))
    part0 = lax.dot_general(tokx[0:rows], dn_buf[1, four:four + lat0], contract, preferred_element_type=jnp.float32)
    part1 = lax.dot_general(tokx[0:rows], dn_buf[2, four:four + lat1], contract, preferred_element_type=jnp.float32)
    latent = jnp.concatenate([part0, part1[:, :lora - lat0]], axis=-1)
    inv = lax.rsqrt(jnp.mean(latent * latent, axis=-1, keepdims=True) + NORM_EPS)
    c_new = (latent * inv * kgain_ref[...].astype(jnp.float32)).astype(jnp.bfloat16)
    cnew_ref[...] = c_new
    newc[...] = c_new.astype(jnp.float32)
    key_part = jnp.concatenate([part1[:, lora - lat0:], jnp.zeros((rows, lanes - rope_dim), jnp.float32)], axis=-1)
    k_new = rope(key_part)[:, :rope_dim].astype(jnp.bfloat16)
    knew_ref[...] = k_new
    newk[...] = jnp.concatenate([k_new.astype(jnp.float32), jnp.zeros((rows, lanes - rope_dim), jnp.float32)], axis=-1)

    column = lax.broadcasted_iota(jnp.int32, (heads, length), 1)

    def attend(seq0, keys, rope_keys):
        scores, news = [], []
        for s in range(8):
            b = seq0 + s
            q_b = qlat[b].astype(jnp.bfloat16)
            r_b = qrot[b].astype(jnp.bfloat16)
            score = lax.dot_general(q_b, keys(s), contract, preferred_element_type=jnp.float32)
            score += jnp.dot(r_b[:, :rope_dim], rope_keys(s), preferred_element_type=jnp.float32)
            scores.append(jnp.where(column < lens_ref[b], score * scale, -jnp.inf))
            r_f = jnp.where(lax.broadcasted_iota(jnp.int32, (heads, lanes), 1) < rope_dim, r_b.astype(jnp.float32), 0.0)
            new = jnp.sum(q_b.astype(jnp.float32) * newc[pl.ds(b, 1), :], axis=-1, keepdims=True)
            news.append((new + jnp.sum(r_f * newk[pl.ds(b, 1), :], axis=-1, keepdims=True)) * scale)
        scores = jnp.concatenate(scores, axis=0)
        news = jnp.concatenate(news, axis=0)
        top = jnp.maximum(jnp.max(scores, axis=-1, keepdims=True), news)
        exp_cache = jnp.exp(scores - top)
        exp_new = jnp.exp(news - top)
        total = jnp.sum(exp_cache, axis=-1, keepdims=True) + exp_new
        prob = (exp_cache / total).astype(jnp.bfloat16)
        prob_new = (exp_new / total).astype(jnp.bfloat16).astype(jnp.float32)
        for s in range(8):
            b = seq0 + s
            out = jnp.dot(prob[s * heads:(s + 1) * heads], keys(s), preferred_element_type=jnp.float32)
            qlat[b] = out + prob_new[s * heads:(s + 1) * heads] * newc[pl.ds(b, 1), :]

    for copy in kr_copies:
        copy.wait()
    for n in range(12, 16):
        cache_copy(n).wait()
    seqs_half = width // rope_dim

    def wide_step(w, carry):
        seq0 = wide_seqs + 8 * w

        def keys(s):
            return gu_buf[1, w, s * length:(s + 1) * length, cache_cols]

        def rope_keys(s):
            return gu_buf[2, 1, pl.ds((seq0 - seqs_half + s) * rope_dim, rope_dim), kr_cols]

        attend(seq0, keys, rope_keys)
        return carry

    lax.fori_loop(0, 2, wide_step, 0)
    hooks[1]()

    def deep_step(it, carry):
        d, i2 = it // 2, lax.rem(it, 2)
        for k in range(2):
            pltpu.make_async_copy(ckv_hbm.at[0:four], dn_buf.at[d, 0:four, pl.ds(pl.multiple_of((2 * i2 + k) * lora, lora), lora)], c_sem.at[2 * it + k]).wait()

        def keys(s):
            cols = pl.ds(pl.multiple_of((2 * i2 + s // 4) * lora, lora), lora)
            return dn_buf[d, (s % 4) * length:(s % 4 + 1) * length, cols]

        def rope_keys(s):
            return gu_buf[2, it // 4, pl.ds((8 * lax.rem(it, 4) + s) * rope_dim, rope_dim), kr_cols]

        attend(8 * it, keys, rope_keys)
        hooks[2](it)
        return carry

    lax.fori_loop(0, wide_seqs // 8, deep_step, 0)

    for copy in uv_copies:
        copy.wait()
    for h in range(heads):
        o_lat = qlat[:, h, :].astype(jnp.bfloat16)
        uv_head = uvbuf[(h % 2) * lora:(h % 2 + 1) * lora, (h // 2) * value_dim:(h // 2 + 1) * value_dim]
        tokx[rows:2 * rows, h * value_dim:(h + 1) * value_dim] = jnp.dot(o_lat, uv_head, preferred_element_type=jnp.float32).astype(jnp.bfloat16)
    parts = []
    for w in range(2):
        out_copies[w].wait()
        parts.append(jnp.dot(tokx[rows:2 * rows], gu_buf[2, w, :, 0:width // 2], preferred_element_type=jnp.float32))
    resid = hidden_ref[...].astype(jnp.float32) + jnp.concatenate(parts, axis=-1)
    return resid.astype(jnp.bfloat16)


def attention_kernel(*refs):
    hidden_ref, lens_ref, again_ref, kgain_ref, ckv, krt, wq, dkvt, uk, uv, wo, resid_ref, *rest = refs
    nothing = lambda *a: None
    resid_ref[...] = attention_phase((hidden_ref, lens_ref, again_ref, kgain_ref, ckv, krt, wq, dkvt, uk, uv, wo, *rest), (nothing, nothing, nothing))


def attention_layer(hidden, ckv_cache, kr_cache, seq_lens, attn_gain, kv_gain, w_q, w_dkv, w_uk, w_uv, w_o, ff):
    rows, width = hidden.shape
    heads, nope, lora = w_uk.shape
    length, rope_dim = kr_cache.shape[1:]
    vmem = pl.BlockSpec(memory_space=pltpu.VMEM)
    hbm = pl.BlockSpec(memory_space=pl.ANY)
    return pl.pallas_call(
        attention_kernel,
        out_shape=(jax.ShapeDtypeStruct((rows, width), jnp.bfloat16), jax.ShapeDtypeStruct((rows, lora), jnp.bfloat16), jax.ShapeDtypeStruct((rows, rope_dim), jnp.bfloat16)),
        in_specs=[vmem, pl.BlockSpec(memory_space=pltpu.SMEM), vmem, vmem] + [hbm] * 7,
        out_specs=(vmem, vmem, vmem),
        scratch_shapes=[
            pltpu.VMEM((128, width), jnp.bfloat16),
            pltpu.VMEM((1024, 1536), jnp.bfloat16),
            pltpu.VMEM((3, 2, width, ff), jnp.bfloat16),
            pltpu.VMEM((3, ff, width), jnp.bfloat16),
            pltpu.VMEM((rows, heads, lora), jnp.float32),
            pltpu.VMEM((rows, heads, 128), jnp.float32),
            pltpu.VMEM((rows, lora), jnp.float32),
            pltpu.VMEM((rows, 128), jnp.float32),
            pltpu.VMEM((rows, 128), jnp.float32),
            pltpu.SemaphoreType.DMA((19,)),
            pltpu.SemaphoreType.DMA((16,)),
        ],
        compiler_params=pltpu.CompilerParams(vmem_limit_bytes=67043328),
        name='latent_attention',
    )(hidden, seq_lens, attn_gain.reshape(1, -1), kv_gain.reshape(1, -1), ckv_cache.reshape(rows * length, lora), jnp.swapaxes(kr_cache, 1, 2).reshape(rows * rope_dim, length), w_q, w_dkv.T, w_uk.reshape(heads * nope, lora), w_uv.reshape(heads * lora, -1), w_o)


def solution(mesh):
    row_spec = P(('rep', 'dp'))
    full_spec = P()
    expert_spec = P('dp')

    def device_step(hidden, ckv_cache, kr_cache, seq_lens, expert_ids, attn_gain, kv_gain, moe_gain, w_q, w_dkv, w_uk, w_uv, w_o, w_router, shared_gate, shared_up, shared_down, expert_gate, expert_up, expert_down):
        capacity = max(2, 2 * hidden.shape[0] * expert_ids.shape[1] // w_router.shape[1])
        resid_out, ckv_new, kr_new = attention_layer(hidden, ckv_cache, kr_cache, seq_lens, attn_gain, kv_gain, w_q, w_dkv, w_uk, w_uv, w_o, expert_gate.shape[2])
        layer_out = moe_layer(resid_out, expert_ids, capacity, mesh.shape['dp'], moe_gain, w_router, shared_gate, shared_up, shared_down, expert_gate, expert_up, expert_down)
        return layer_out, ckv_new, kr_new

    in_specs = (row_spec,) * 5 + (full_spec,) * 12 + (expert_spec,) * 3
    return jax.shard_map(device_step, mesh=mesh, in_specs=in_specs, out_specs=(row_spec, row_spec, row_spec), check_vma=False)
```

```python
import functools
import math

import jax
import jax.numpy as jnp
from jax import lax
from jax.experimental import pallas as pl
from jax.experimental.pallas import tpu as pltpu
from jax.sharding import PartitionSpec as P

NORM_EPS = 1e-6
ROPE_THETA = 10000.0


MESH_ID = pl.DeviceIdType.MESH


def attention_phase(refs, hooks):
    (hidden_hbm, hidden_ref, lens_ref, again_ref, kgain_ref, ckv_hbm, krt_hbm, wq_hbm, dkvt_hbm, uk_hbm, uv_hbm, wo_hbm, cnew_ref, knew_ref,
     tokx, uvbuf, gu_buf, dn_buf, qlat, qrot, newc, newk, pos, a_sem, c_sem) = refs
    rows, width = hidden_ref.shape
    lora = qlat.shape[-1]
    heads = qlat.shape[1]
    rope_dim = krt_hbm.shape[0] // rows
    length = krt_hbm.shape[1]
    nope = uk_hbm.shape[0] // heads
    head_dim = nope + rope_dim
    qcols = wq_hbm.shape[1] // 4
    four = 4 * length
    value_dim = uv_hbm.shape[-1]
    scale = head_dim ** -0.5
    lanes = 128
    lat0 = dn_buf.shape[1] - four
    lat1 = dkvt_hbm.shape[0] - lat0
    cache_cols = slice(qcols, qcols + lora)
    kr_cols = slice(width // 2, width // 2 + length)

    def query_copy(i):
        return pltpu.make_async_copy(wq_hbm.at[:, i * qcols:(i + 1) * qcols], gu_buf.at[i // 2, i % 2, :, 0:qcols], a_sem.at[i])

    latent_copies = [
        pltpu.make_async_copy(dkvt_hbm.at[0:lat0], dn_buf.at[1, four:four + lat0], a_sem.at[4]),
        pltpu.make_async_copy(dkvt_hbm.at[lat0:lat0 + lat1], dn_buf.at[2, four:four + lat1], a_sem.at[5]),
    ]
    uk_copy = pltpu.make_async_copy(uk_hbm, gu_buf.at[0, 1, :, cache_cols], a_sem.at[6])
    kr_copies = [pltpu.make_async_copy(krt_hbm.at[w * width:(w + 1) * width], gu_buf.at[2, w, :, kr_cols], a_sem.at[7 + w]) for w in range(2)]
    out_copies = [pltpu.make_async_copy(wo_hbm.at[:, w * (width // 2):(w + 1) * (width // 2)], gu_buf.at[2, w, :, 0:width // 2], a_sem.at[9 + w]) for w in range(2)]
    uv_copies = [pltpu.make_async_copy(uv_hbm.at[i], uvbuf.at[:, :, :, i * value_dim:(i + 1) * value_dim], a_sem.at[11 + i]) for i in range(heads // 2)]
    wide_seqs = 48

    def cache_copy(n):
        if n >= 12:
            w, r = (n - 12) // 2, n % 2
            return pltpu.make_async_copy(ckv_hbm.at[n * four:(n + 1) * four], gu_buf.at[1, w, r * four:(r + 1) * four, cache_cols], c_sem.at[n])
        return pltpu.make_async_copy(ckv_hbm.at[n * four:(n + 1) * four], dn_buf.at[n // 4, 0:four, (n % 4) * lora:(n % 4 + 1) * lora], c_sem.at[n])

    hidden_copy = pltpu.make_async_copy(hidden_hbm, hidden_ref, a_sem.at[19])
    hidden_copy.start()
    query_copy(0).start()
    for copy in latent_copies:
        copy.start()
    uk_copy.start()
    for i in range(1, 4):
        query_copy(i).start()

    lane = lax.broadcasted_iota(jnp.int32, (rows, lanes), 1)
    hidden_copy.wait()
    hidden = hidden_ref[...].astype(jnp.float32)
    inv = lax.rsqrt(jnp.mean(hidden * hidden, axis=-1, keepdims=True) + NORM_EPS)
    tokx[0:rows] = (hidden * inv * again_ref[...].astype(jnp.float32)).astype(jnp.bfloat16)
    for b in range(rows):
        pos[b:b + 1, :] = jnp.full((1, lanes), lens_ref[b], jnp.int32).astype(jnp.float32)
    quarter = lax.rem(lane, rope_dim // 2).astype(jnp.float32)
    angle = pos[...] * jnp.exp(quarter * (-2.0 / rope_dim * math.log(ROPE_THETA)))
    rope_cos = jnp.cos(angle)
    low_half = lax.rem(lane, rope_dim) < rope_dim // 2
    rope_sin = jnp.where(low_half, -jnp.sin(angle), jnp.sin(angle))

    def rope(value):
        swapped = jnp.where(low_half, pltpu.roll(value, lanes - rope_dim // 2, 1), pltpu.roll(value, rope_dim // 2, 1))
        return value * rope_cos + swapped * rope_sin

    first_half = lane < rope_dim

    def row_of(h):
        return (h % 2) * (heads // 2) + h // 2

    for i in range(4):
        query_copy(i).wait()
        q_cols = jnp.dot(tokx[0:rows], gu_buf[i // 2, i % 2, :, 0:qcols], preferred_element_type=jnp.float32)
        q_cols = q_cols.astype(jnp.bfloat16).astype(jnp.float32)
        if i == 0:
            for n in range(12, 16):
                cache_copy(n).start()
            for copy in kr_copies:
                copy.start()
            uk_copy.wait()
        if i == 1:
            for n in range(4):
                cache_copy(n).start()
        for pair in range(qcols // (2 * head_dim)):
            base = pair * 2 * head_dim
            tile0, tile1, tile2 = (q_cols[:, base + k * lanes:base + (k + 1) * lanes] for k in range(3))
            head = i * (qcols // head_dim) + 2 * pair
            nopes = (tile0, pltpu.roll(jnp.where(first_half, tile2, tile1), lanes // 2, 1))
            turned = rope(jnp.where(first_half, tile1, tile2))
            qrot[:, head // 2, :] = turned
            for odd in range(2):
                h = head + odd
                uk_head = gu_buf[0, 1, h * nope:(h + 1) * nope, cache_cols]
                qlat[:, row_of(h), :] = jnp.dot(nopes[odd].astype(jnp.bfloat16), uk_head, preferred_element_type=jnp.float32)
    for n in range(4, 12):
        cache_copy(n).start()
    for copy in uv_copies + out_copies:
        copy.start()
    hooks[0]()

    for copy in latent_copies:
        copy.wait()
    contract = (((1,), (1,)), ((), ()))
    part0 = lax.dot_general(tokx[0:rows], dn_buf[1, four:four + lat0], contract, preferred_element_type=jnp.float32)
    part1 = lax.dot_general(tokx[0:rows], dn_buf[2, four:four + lat1], contract, preferred_element_type=jnp.float32)
    latent = jnp.concatenate([part0, part1[:, :lora - lat0]], axis=-1)
    inv = lax.rsqrt(jnp.mean(latent * latent, axis=-1, keepdims=True) + NORM_EPS)
    c_new = (latent * inv * kgain_ref[...].astype(jnp.float32)).astype(jnp.bfloat16)
    cnew_ref[...] = c_new
    newc[...] = c_new.astype(jnp.float32)
    key_part = jnp.concatenate([part1[:, lora - lat0:], jnp.zeros((rows, lanes - rope_dim), jnp.float32)], axis=-1)
    k_new = rope(key_part)[:, :rope_dim].astype(jnp.bfloat16)
    knew_ref[...] = k_new
    newk[...] = jnp.concatenate([k_new.astype(jnp.float32), jnp.zeros((rows, lanes - rope_dim), jnp.float32)], axis=-1)

    column = lax.broadcasted_iota(jnp.int32, (heads, length), 1)

    def attend(seq0, keys, rope_keys):
        scores, news = [], []
        for s in range(8):
            b = seq0 + s
            q_b = qlat[b].astype(jnp.bfloat16)
            pairs = qrot[b]
            r_b = jnp.concatenate([pairs, pltpu.roll(pairs, lanes // 2, 1)], axis=0).astype(jnp.bfloat16)
            score = lax.dot_general(q_b, keys(s), contract, preferred_element_type=jnp.float32)
            score += jnp.dot(r_b[:, :rope_dim], rope_keys(s), preferred_element_type=jnp.float32)
            scores.append(jnp.where(column < lens_ref[b], score * scale, -jnp.inf))
            r_f = jnp.where(lax.broadcasted_iota(jnp.int32, (heads, lanes), 1) < rope_dim, r_b.astype(jnp.float32), 0.0)
            new = jnp.sum(q_b.astype(jnp.float32) * newc[pl.ds(b, 1), :], axis=-1, keepdims=True)
            news.append((new + jnp.sum(r_f * newk[pl.ds(b, 1), :], axis=-1, keepdims=True)) * scale)
        scores = jnp.concatenate(scores, axis=0)
        news = jnp.concatenate(news, axis=0)
        top = jnp.maximum(jnp.max(scores, axis=-1, keepdims=True), news)
        exp_cache = jnp.exp(scores - top)
        exp_new = jnp.exp(news - top)
        total = jnp.sum(exp_cache, axis=-1, keepdims=True) + exp_new
        prob = (exp_cache / total).astype(jnp.bfloat16)
        prob_new = (exp_new / total).astype(jnp.bfloat16).astype(jnp.float32)
        for s in range(8):
            b = seq0 + s
            out = jnp.dot(prob[s * heads:(s + 1) * heads], keys(s), preferred_element_type=jnp.float32)
            qlat[b] = out + prob_new[s * heads:(s + 1) * heads] * newc[pl.ds(b, 1), :]

    for copy in kr_copies:
        copy.wait()
    for n in range(12, 16):
        cache_copy(n).wait()
    seqs_half = width // rope_dim

    def wide_step(w, carry):
        seq0 = wide_seqs + 8 * w

        def keys(s):
            return gu_buf[1, w, s * length:(s + 1) * length, cache_cols]

        def rope_keys(s):
            return gu_buf[2, 1, pl.ds((seq0 - seqs_half + s) * rope_dim, rope_dim), kr_cols]

        attend(seq0, keys, rope_keys)
        return carry

    lax.fori_loop(0, 2, wide_step, 0)
    hooks[1]()

    def deep_step(it, carry):
        d, i2 = it // 2, lax.rem(it, 2)
        for k in range(2):
            pltpu.make_async_copy(ckv_hbm.at[0:four], dn_buf.at[d, 0:four, pl.ds(pl.multiple_of((2 * i2 + k) * lora, lora), lora)], c_sem.at[2 * it + k]).wait()

        def keys(s):
            cols = pl.ds(pl.multiple_of((2 * i2 + s // 4) * lora, lora), lora)
            return dn_buf[d, (s % 4) * length:(s % 4 + 1) * length, cols]

        def rope_keys(s):
            return gu_buf[2, it // 4, pl.ds((8 * lax.rem(it, 4) + s) * rope_dim, rope_dim), kr_cols]

        attend(8 * it, keys, rope_keys)
        hooks[2](it)
        return carry

    lax.fori_loop(0, wide_seqs // 8, deep_step, 0)

    for copy in uv_copies:
        copy.wait()
    for h in range(heads):
        o_lat = qlat[:, row_of(h), :].astype(jnp.bfloat16)
        uv_half = uvbuf.shape[0] // 2
        uv_head = uvbuf[(h % 2) * uv_half:(h % 2 + 1) * uv_half, :, :, (h // 2) * value_dim:(h // 2 + 1) * value_dim].reshape(lora, value_dim)
        tokx[rows:2 * rows, h * value_dim:(h + 1) * value_dim] = jnp.dot(o_lat, uv_head, preferred_element_type=jnp.float32).astype(jnp.bfloat16)
    parts = []
    for w in range(2):
        out_copies[w].wait()
        parts.append(jnp.dot(tokx[rows:2 * rows], gu_buf[2, w, :, 0:width // 2], preferred_element_type=jnp.float32))
    hooks[3]()
    resid = hidden_ref[...].astype(jnp.float32) + jnp.concatenate(parts, axis=-1)
    return resid.astype(jnp.bfloat16)


def silu(value):
    return value * (1.0 / (1.0 + jnp.exp(-value)))


def layer_kernel(dims, hidden_hbm, lens_ref, ids_ref, again_ref, kgain_ref, gain_ref, router_ref, ckv_hbm, krt_hbm, wq_hbm, dkvt_hbm, uk_hbm, uv_hbm, wo_hbm,
                 sgate_hbm, sup_hbm, sdown_hbm, egate_hbm, eup_hbm, edown_hbm, out_ref, cnew_ref, knew_ref,
                 ublk, tokx, midx, send, recv, acc, table, tail, gu_buf, dn_buf, qlat, qrot, newc, newk,
                 gu_sem, dn_sem, us_sem, ur_sem, ys_sem, yr_sem, a_sem, c_sem):
    group, experts_dev, experts, cap, depth, dp_axis = dims
    rows, width = hidden_hbm.shape
    half = rows // 2
    ff = gu_buf.shape[-1]
    n_shared = sgate_hbm.shape[-1] // ff
    steps = experts_dev + n_shared
    slot16 = 16
    slots = group * slot16
    main = send.shape[-1]
    blk = main // 3
    top_k = ids_ref.shape[0]
    lag = 4
    lanes = 128
    me = lax.axis_index(dp_axis)
    chips = group // 2
    core = lax.rem(me, 2)
    chip = me // 2
    partner = chip * 2 + (1 - core)
    left = lax.rem(chip + chips - 1, chips) * 2 + core
    right = lax.rem(chip + 1, chips) * 2 + core
    far = lax.rem(chip + 2, chips) * 2 + core

    def routed(step):
        return (step >= 1) & (step <= experts_dev)

    def either(condition, action_a, action_b):
        if isinstance(condition, bool):
            (action_a if condition else action_b)()
        else:
            pl.when(condition)(action_a)
            pl.when(jnp.logical_not(condition))(action_b)

    def weights_gu(step, which, hbm, shared_hbm, action):
        slot = step % depth if isinstance(step, int) else lax.rem(step, depth)

        def own():
            getattr(pltpu.make_async_copy(hbm.at[step - 1], gu_buf.at[slot, which], gu_sem.at[slot, which]), action)()

        def shared():
            start = step // (steps - 1) * ff
            cols = pl.ds(start if isinstance(step, int) else pl.multiple_of(start, 128), ff)
            getattr(pltpu.make_async_copy(shared_hbm.at[:, cols], gu_buf.at[slot, which], gu_sem.at[slot, which]), action)()

        either(routed(step), own, shared)

    def weights_dn(step, action):
        slot = step % depth if isinstance(step, int) else lax.rem(step, depth)

        def own():
            getattr(pltpu.make_async_copy(edown_hbm.at[step - 1], dn_buf.at[slot], dn_sem.at[slot]), action)()

        def shared():
            start = step // (steps - 1) * ff
            cols = pl.ds(start if isinstance(step, int) else pl.multiple_of(start, 128), ff)
            getattr(pltpu.make_async_copy(sdown_hbm.at[cols], dn_buf.at[slot], dn_sem.at[slot]), action)()

        either(routed(step), own, shared)

    def fetch(step):
        weights_gu(step, 0, egate_hbm, sgate_hbm, "start")
        weights_gu(step, 1, eup_hbm, sup_hbm, "start")

    barrier = pltpu.get_barrier_semaphore()
    for k in range(1, group):
        pl.semaphore_signal(barrier, inc=1, device_id={dp_axis: lax.rem(me + k, group)}, device_id_type=MESH_ID)

    def freed_deep(it):
        for d in range(depth):
            @pl.when(it == 2 * d + 1)
            def _():
                weights_dn(d, "start")

    hooks = (lambda: fetch(0), lambda: fetch(1), freed_deep, lambda: fetch(2))
    resid = attention_phase((hidden_hbm, out_ref, lens_ref, again_ref, kgain_ref, ckv_hbm, krt_hbm, wq_hbm, dkvt_hbm, uk_hbm, uv_hbm, wo_hbm, cnew_ref, knew_ref,
                             tokx, send, gu_buf, dn_buf, qlat, qrot, newc, newk, acc.at[:, 0:128], a_sem, c_sem), hooks)

    resid = resid.astype(jnp.float32)
    inv = lax.rsqrt(jnp.mean(resid * resid, axis=-1, keepdims=True) + NORM_EPS)
    u = (resid * inv * gain_ref[...].astype(jnp.float32)).astype(jnp.bfloat16)
    expert_i = lax.broadcasted_iota(jnp.int32, (lanes, rows), 0)
    picked = ids_ref[0:1, :] == expert_i
    for k in range(1, top_k):
        picked = picked | (ids_ref[k:k + 1, :] == expert_i)
    tok_a = lax.broadcasted_iota(jnp.int32, (rows, rows), 0)
    tok_b = lax.broadcasted_iota(jnp.int32, (rows, rows), 1)
    before = jnp.where(tok_a < tok_b, 1.0, 0.0).astype(jnp.bfloat16)
    rank = jnp.dot(jnp.where(picked, 1.0, 0.0).astype(jnp.bfloat16), before, preferred_element_type=jnp.float32)
    codes_t = jnp.where(picked, rank, -1.0).astype(jnp.bfloat16)
    same = jnp.where(tok_a == tok_b, 1.0, 0.0).astype(jnp.bfloat16)
    codes = lax.dot_general(same, codes_t, (((1,), (1,)), ((), ())), preferred_element_type=jnp.float32).astype(jnp.bfloat16)
    for h in range(2):
        ublk[me, h, :, :width] = u[h * half:(h + 1) * half]
        ublk[me, h, :, width:] = codes[h * half:(h + 1) * half]
    logits = lax.dot_general(u, router_ref[...], (((1,), (1,)), ((), ())), preferred_element_type=jnp.float32)
    logits = logits - jnp.max(logits, axis=-1, keepdims=True)
    expl = jnp.exp(logits)
    prob = expl / jnp.sum(expl, axis=-1, keepdims=True)
    prob = jnp.concatenate([prob, jnp.zeros((rows, lanes - experts), jnp.float32)], axis=-1)
    p0 = prob.astype(jnp.bfloat16)
    rest = prob - p0.astype(jnp.float32)
    p1 = rest.astype(jnp.bfloat16)
    p2 = (rest - p1.astype(jnp.float32)).astype(jnp.bfloat16)
    table[0] = codes
    table[1] = p0
    table[2] = p1
    table[3] = p2
    acc[...] = resid

    pl.semaphore_wait(barrier, group - 1)

    def block_copy(block, h, dest, sem_no):
        return pltpu.make_async_remote_copy(src_ref=ublk.at[block, h], dst_ref=ublk.at[block, h], send_sem=us_sem.at[sem_no], recv_sem=ur_sem.at[block, h], device_id={dp_axis: dest}, device_id_type=MESH_ID)

    def crossed(block):
        return lax.rem(block + 1 - 2 * core + group, group)

    first_sends = ((me, 0, right), (me, 1, left), (me, 1, right), (me, 0, left), (me, 0, partner), (me, 1, partner))
    relays = ((left, 0, right), (left, 0, partner), (right, 1, left), (right, 1, partner), (left, 1, partner), (right, 0, partner), (far, 0, partner), (far, 1, partner))
    all_sends = first_sends + relays

    def send_block(n):
        block, h, dest = all_sends[n]
        block_copy(block, h, dest, n).start()

    def arrived(block, h):
        block_copy(block, h, partner, 0).wait_recv()

    for n in range(len(first_sends)):
        send_block(n)

    def relay():
        seen = set()
        for n in range(len(first_sends), len(all_sends)):
            block, h, _ = all_sends[n]
            if (id(block), h) not in seen:
                seen.add((id(block), h))
                arrived(block, h)
            send_block(n)
        for block in (partner, crossed(left), crossed(right), crossed(far)):
            for h in range(2):
                arrived(block, h)

    row_i = lax.broadcasted_iota(jnp.int32, (lanes, slots), 0)
    col_i = lax.broadcasted_iota(jnp.int32, (lanes, slots), 1)

    def return_copy(step, dest):
        return pltpu.make_async_remote_copy(src_ref=send.at[step, dest], dst_ref=recv.at[step, me], send_sem=ys_sem.at[step, dest], recv_sem=yr_sem.at[step, me], device_id={dp_axis: dest}, device_id_type=MESH_ID)

    def arrival(step, source):
        return pltpu.make_async_remote_copy(src_ref=send.at[step, source], dst_ref=recv.at[step, source], send_sem=ys_sem.at[step, source], recv_sem=yr_sem.at[step, source], device_id={dp_axis: source}, device_id_type=MESH_ID)

    def gather_rows(expert):
        pick = (row_i == me * experts_dev + expert).astype(jnp.float32).astype(jnp.bfloat16)
        code_all = ublk[:, :, :, width:].reshape(group * rows, lanes)
        code_b = jnp.dot(code_all, pick, preferred_element_type=jnp.float32)
        tok = lax.broadcasted_iota(jnp.int32, (group * rows, slots), 0)
        col = lax.broadcasted_iota(jnp.int32, (group * rows, slots), 1)
        hit = (code_b == lax.rem(col, slot16).astype(jnp.float32)) & (tok // rows == col // slot16)
        place = jnp.where(hit, 1.0, 0.0).astype(jnp.bfloat16)
        for c0 in range(0, width, 512):
            rows_u = ublk[:, :, :, c0:c0 + 512].reshape(group * rows, 512)
            picked_rows = lax.dot_general(place, rows_u, (((0,), (0,)), ((), ())), preferred_element_type=jnp.float32)
            tokx[:, c0:c0 + 512] = picked_rows.astype(jnp.bfloat16)

    def pack_block(y_main, q):
        y_main = y_main.reshape(group, 2, 8, blk)
        y_tail = tail[...].reshape(group, 2, 8, blk)
        sub = lax.broadcasted_iota(jnp.int32, (group, 8, blk), 1)
        part = y_tail[:, 1 if q == 2 else 0]
        if q != 1:
            part = pltpu.roll(part.reshape(group * 8, blk).reshape(group, 8, blk), 4, 1)
        low = jnp.where(sub >= 4, part, y_main[:, 1])
        return jnp.concatenate([y_main[:, 0], low], axis=1).astype(jnp.bfloat16)

    def combine(step):
        for k in range(1, group):
            arrival(step, lax.rem(me + k, group)).wait_recv()
        spread = (row_i == (col_i // slot16) * experts_dev + step).astype(jnp.float32).astype(jnp.bfloat16)
        wide = jnp.dot(table[...].reshape(4 * rows, lanes), spread, preferred_element_type=jnp.float32)
        code_b = wide[:rows]
        slot_i = lax.rem(lax.broadcasted_iota(jnp.int32, (rows, slots), 1), slot16)
        slot_f = slot_i.astype(jnp.float32)
        for q in range(3):
            hits = [code_b == slot_f, (slot_i >= cap) & (code_b == slot_f - cap + 4 * q)]
            lhs = jnp.concatenate([jnp.where(hit, wide[p * rows:(p + 1) * rows], 0.0) for hit in hits for p in (1, 2, 3)], axis=0).astype(jnp.bfloat16)
            y_blk = recv[step, :, :, q * blk:(q + 1) * blk].reshape(slots, blk)
            res = jnp.dot(lhs, y_blk, preferred_element_type=jnp.float32)
            acc[:, q * blk:(q + 1) * blk] += res[:rows] + (res[rows:2 * rows] + res[2 * rows:3 * rows])
            acc[:, main:] += res[3 * rows:4 * rows] + (res[4 * rows:5 * rows] + res[5 * rows:])

    def one_step(step, carry):
        slot = lax.rem(step, depth)
        expert = step - 1
        is_routed = routed(step)

        @pl.when(step == 1)
        def _():
            relay()

        @pl.when(is_routed)
        def _():
            gather_rows(expert)

        @pl.when(jnp.logical_not(is_routed))
        def _():
            tokx[:rows] = ublk[me, :, :, :width].reshape(rows, width)
            tokx[rows:] = jnp.zeros((slots - rows, width), jnp.bfloat16)

        weights_gu(step, 0, egate_hbm, sgate_hbm, "wait")
        weights_gu(step, 1, eup_hbm, sup_hbm, "wait")
        for c0 in range(0, ff, 512):
            c1 = min(c0 + 512, ff)
            gate_act = jnp.dot(tokx[...], gu_buf[slot, 0, :, c0:c1], preferred_element_type=jnp.float32)
            up_act = jnp.dot(tokx[...], gu_buf[slot, 1, :, c0:c1], preferred_element_type=jnp.float32)
            midx[:, c0:c1] = (silu(gate_act) * up_act).astype(jnp.bfloat16)

        @pl.when(step + depth < steps)
        def _():
            fetch(step + depth)

        weights_dn(step, "wait")
        tail[...] = jnp.dot(midx[...], dn_buf[slot, :, main:], preferred_element_type=jnp.float32)

        @pl.when(jnp.logical_not(is_routed))
        def _():
            acc[:, main:] += tail[:rows]

        for q in range(3):
            y_main = jnp.dot(midx[...], dn_buf[slot, :, q * blk:(q + 1) * blk], preferred_element_type=jnp.float32)

            @pl.when(is_routed)
            def _():
                send[expert, :, :, q * blk:(q + 1) * blk] = pack_block(y_main, q)

            @pl.when(jnp.logical_not(is_routed))
            def _():
                acc[:, q * blk:(q + 1) * blk] += y_main[:rows]

        @pl.when(step + depth < steps)
        def _():
            weights_dn(step + depth, "start")

        @pl.when(is_routed)
        def _():
            recv[expert, me] = send[expert, me]
            for k in (4, 3, 5, 2, 6, 1, 7):
                return_copy(expert, lax.rem(me + k, group)).start()

        @pl.when(expert >= lag)
        def _():
            combine(expert - lag)

        return carry

    lax.fori_loop(0, steps, one_step, 0)

    def last_combine(step, carry):
        combine(step)
        return carry

    lax.fori_loop(steps - 1 - lag, experts_dev, last_combine, 0)
    out_ref[...] = acc[...].astype(out_ref.dtype)

    for n, (block, h, dest) in enumerate(all_sends):
        block_copy(block, h, dest, n).wait_send()

    def drain(step, carry):
        for k in range(1, group):
            return_copy(step, lax.rem(me + k, group)).wait_send()
        return carry

    lax.fori_loop(0, experts_dev, drain, 0)


def layer(group, cap, hidden, ckv_cache, kr_cache, seq_lens, expert_ids, attn_gain, kv_gain, moe_gain, w_q, w_dkv, w_uk, w_uv, w_o, w_router, shared_gate, shared_up, shared_down, expert_gate, expert_up, expert_down):
    rows, width = hidden.shape
    heads, nope, lora = w_uk.shape
    length, rope_dim = kr_cache.shape[1:]
    experts_dev, _, ff = expert_gate.shape
    experts = w_router.shape[1]
    depth = 3
    main = 3 * width // 4
    slots = group * 16
    dims = (group, experts_dev, experts, cap, depth, 'dp')
    vmem = pl.BlockSpec(memory_space=pltpu.VMEM)
    hbm = pl.BlockSpec(memory_space=pl.ANY)
    return pl.pallas_call(
        functools.partial(layer_kernel, dims),
        out_shape=(jax.ShapeDtypeStruct((rows, width), jnp.bfloat16), jax.ShapeDtypeStruct((rows, lora), jnp.bfloat16), jax.ShapeDtypeStruct((rows, rope_dim), jnp.bfloat16)),
        in_specs=[hbm, pl.BlockSpec(memory_space=pltpu.SMEM)] + [vmem] * 5 + [hbm] * 13,
        out_specs=(vmem, vmem, vmem),
        scratch_shapes=[
            pltpu.VMEM((group, 2, rows // 2, width + 128), jnp.bfloat16),
            pltpu.VMEM((slots, width), jnp.bfloat16),
            pltpu.VMEM((slots, ff), jnp.bfloat16),
            pltpu.VMEM((experts_dev, group, 16, main), jnp.bfloat16),
            pltpu.VMEM((experts_dev, group, 16, main), jnp.bfloat16),
            pltpu.VMEM((rows, width), jnp.float32),
            pltpu.VMEM((4, rows, 128), jnp.bfloat16),
            pltpu.VMEM((slots, width - main), jnp.float32),
            pltpu.VMEM((depth, 2, width, ff), jnp.bfloat16),
            pltpu.VMEM((depth, ff, width), jnp.bfloat16),
            pltpu.VMEM((rows, heads, lora), jnp.float32),
            pltpu.VMEM((rows, heads // 2, 128), jnp.float32),
            pltpu.VMEM((rows, lora), jnp.float32),
            pltpu.VMEM((rows, 128), jnp.float32),
            pltpu.SemaphoreType.DMA((depth, 2)),
            pltpu.SemaphoreType.DMA((depth,)),
            pltpu.SemaphoreType.DMA((14,)),
            pltpu.SemaphoreType.DMA((group, 2)),
            pltpu.SemaphoreType.DMA((experts_dev, group)),
            pltpu.SemaphoreType.DMA((experts_dev, group)),
            pltpu.SemaphoreType.DMA((20,)),
            pltpu.SemaphoreType.DMA((16,)),
        ],
        compiler_params=pltpu.CompilerParams(collective_id=0, has_side_effects=True, vmem_limit_bytes=67043328),
        name='decoder_layer',
    )(hidden, seq_lens, expert_ids.T, attn_gain.reshape(1, -1), kv_gain.reshape(1, -1), moe_gain.reshape(1, -1), w_router.T,
      ckv_cache.reshape(rows * length, lora), jnp.swapaxes(kr_cache, 1, 2).reshape(rows * rope_dim, length), w_q, w_dkv.T, w_uk.reshape(heads * nope, lora),
      w_uv.reshape(heads // 2, experts_dev, group, 16, -1), w_o, shared_gate, shared_up, shared_down, expert_gate, expert_up, expert_down)


def solution(mesh):
    row_spec = P(('rep', 'dp'))
    full_spec = P()
    expert_spec = P('dp')

    def device_step(hidden, ckv_cache, kr_cache, seq_lens, expert_ids, attn_gain, kv_gain, moe_gain, w_q, w_dkv, w_uk, w_uv, w_o, w_router, shared_gate, shared_up, shared_down, expert_gate, expert_up, expert_down):
        capacity = max(2, 2 * hidden.shape[0] * expert_ids.shape[1] // w_router.shape[1])
        return layer(mesh.shape['dp'], capacity, hidden, ckv_cache, kr_cache, seq_lens, expert_ids, attn_gain, kv_gain, moe_gain, w_q, w_dkv, w_uk, w_uv, w_o, w_router, shared_gate, shared_up, shared_down, expert_gate, expert_up, expert_down)

    in_specs = (row_spec,) * 5 + (full_spec,) * 12 + (expert_spec,) * 3
    return jax.shard_map(device_step, mesh=mesh, in_specs=in_specs, out_specs=(row_spec, row_spec, row_spec), check_vma=False)
```

```python
import functools
import math

import jax
import jax.numpy as jnp
from jax import lax
from jax.experimental import pallas as pl
from jax.experimental.pallas import tpu as pltpu
from jax.sharding import PartitionSpec as P

NORM_EPS = 1e-6
ROPE_THETA = 10000.0


MESH_ID = pl.DeviceIdType.MESH


def attention_phase(refs, hooks):
    (hidden_hbm, hidden_ref, lens_ref, again_ref, kgain_ref, ckv_hbm, krt_hbm, wq_hbm, dkvt_hbm, uk_hbm, uv_hbm, wo_hbm, cnew_ref, knew_ref,
     tokx, uvbuf, gu_buf, dn_buf, qlat, qrot, newc, newk, pos, a_sem, c_sem) = refs
    rows, width = hidden_ref.shape
    lora = qlat.shape[-1]
    heads = qlat.shape[1]
    rope_dim = krt_hbm.shape[0] // rows
    length = krt_hbm.shape[1]
    nope = uk_hbm.shape[0] // heads
    head_dim = nope + rope_dim
    qcols = wq_hbm.shape[1] // 4
    four = 4 * length
    value_dim = uv_hbm.shape[-1]
    scale = head_dim ** -0.5
    lanes = 128
    lat0 = dn_buf.shape[1] - four
    lat1 = dkvt_hbm.shape[0] - lat0
    cache_cols = slice(qcols, qcols + lora)
    kr_cols = slice(width // 2, width // 2 + length)

    def query_copy(i):
        return pltpu.make_async_copy(wq_hbm.at[:, i * qcols:(i + 1) * qcols], gu_buf.at[i // 2, i % 2, :, 0:qcols], a_sem.at[i])

    latent_copies = [
        pltpu.make_async_copy(dkvt_hbm.at[0:lat0], dn_buf.at[1, four:four + lat0], a_sem.at[4]),
        pltpu.make_async_copy(dkvt_hbm.at[lat0:lat0 + lat1], dn_buf.at[2, four:four + lat1], a_sem.at[5]),
    ]
    uk_copy = pltpu.make_async_copy(uk_hbm, gu_buf.at[0, 1, :, cache_cols], a_sem.at[6])
    kr_copies = [pltpu.make_async_copy(krt_hbm.at[w * width:(w + 1) * width], gu_buf.at[2, w, :, kr_cols], a_sem.at[7 + w]) for w in range(2)]
    out_copies = [pltpu.make_async_copy(wo_hbm.at[:, w * (width // 2):(w + 1) * (width // 2)], gu_buf.at[2, w, :, 0:width // 2], a_sem.at[9 + w]) for w in range(2)]
    uv_copies = [pltpu.make_async_copy(uv_hbm.at[i], uvbuf.at[:, :, :, i * value_dim:(i + 1) * value_dim], a_sem.at[11 + i]) for i in range(heads // 2)]
    wide_seqs = 48

    def cache_copy(n):
        if n >= 12:
            w, r = (n - 12) // 2, n % 2
            return pltpu.make_async_copy(ckv_hbm.at[n * four:(n + 1) * four], gu_buf.at[1, w, r * four:(r + 1) * four, cache_cols], c_sem.at[n])
        return pltpu.make_async_copy(ckv_hbm.at[n * four:(n + 1) * four], dn_buf.at[n // 4, 0:four, (n % 4) * lora:(n % 4 + 1) * lora], c_sem.at[n])

    hidden_copy = pltpu.make_async_copy(hidden_hbm, hidden_ref, a_sem.at[19])
    hidden_copy.start()
    query_copy(0).start()
    for copy in latent_copies:
        copy.start()
    uk_copy.start()
    for i in range(1, 4):
        query_copy(i).start()
    for n in range(12, 16):
        cache_copy(n).start()
    for copy in kr_copies:
        copy.start()
    for n in range(8):
        cache_copy(n).start()

    lane = lax.broadcasted_iota(jnp.int32, (rows, lanes), 1)
    hidden_copy.wait()
    hidden = hidden_ref[...].astype(jnp.float32)
    inv = lax.rsqrt(jnp.mean(hidden * hidden, axis=-1, keepdims=True) + NORM_EPS)
    tokx[0:rows] = (hidden * inv * again_ref[...].astype(jnp.float32).reshape(1, -1)).astype(jnp.bfloat16)
    for b in range(rows):
        pos[b:b + 1, :] = jnp.full((1, lanes), lens_ref[b], jnp.int32).astype(jnp.float32)
    quarter = lax.rem(lane, rope_dim // 2).astype(jnp.float32)
    angle = pos[...] * jnp.exp(quarter * (-2.0 / rope_dim * math.log(ROPE_THETA)))
    rope_cos = jnp.cos(angle)
    low_half = lax.rem(lane, rope_dim) < rope_dim // 2
    rope_sin = jnp.where(low_half, -jnp.sin(angle), jnp.sin(angle))

    def rope(value):
        swapped = jnp.where(low_half, pltpu.roll(value, lanes - rope_dim // 2, 1), pltpu.roll(value, rope_dim // 2, 1))
        return value * rope_cos + swapped * rope_sin

    first_half = lane < rope_dim

    def row_of(h):
        return (h % 2) * (heads // 2) + h // 2

    for i in range(4):
        query_copy(i).wait()
        q_cols = jnp.dot(tokx[0:rows], gu_buf[i // 2, i % 2, :, 0:qcols], preferred_element_type=jnp.float32)
        q_cols = q_cols.astype(jnp.bfloat16).astype(jnp.float32)
        if i == 0:
            for copy in uv_copies + out_copies:
                copy.start()
            for n in range(8, 12):
                cache_copy(n).start()
            uk_copy.wait()
        for pair in range(qcols // (2 * head_dim)):
            base = pair * 2 * head_dim
            tile0, tile1, tile2 = (q_cols[:, base + k * lanes:base + (k + 1) * lanes] for k in range(3))
            head = i * (qcols // head_dim) + 2 * pair
            nopes = (tile0, pltpu.roll(jnp.where(first_half, tile2, tile1), lanes // 2, 1))
            turned = rope(jnp.where(first_half, tile1, tile2))
            qrot[:, head // 2, :] = turned
            for odd in range(2):
                h = head + odd
                uk_head = gu_buf[0, 1, h * nope:(h + 1) * nope, cache_cols]
                qlat[:, row_of(h), :] = jnp.dot(nopes[odd].astype(jnp.bfloat16), uk_head, preferred_element_type=jnp.float32)
    hooks[0]()

    for copy in latent_copies:
        copy.wait()
    contract = (((1,), (1,)), ((), ()))
    part0 = lax.dot_general(tokx[0:rows], dn_buf[1, four:four + lat0], contract, preferred_element_type=jnp.float32)
    part1 = lax.dot_general(tokx[0:rows], dn_buf[2, four:four + lat1], contract, preferred_element_type=jnp.float32)
    latent = jnp.concatenate([part0, part1[:, :lora - lat0]], axis=-1)
    inv = lax.rsqrt(jnp.mean(latent * latent, axis=-1, keepdims=True) + NORM_EPS)
    c_new = (latent * inv * kgain_ref[...].astype(jnp.float32).reshape(1, -1)).astype(jnp.bfloat16)
    cnew_ref[...] = c_new
    newc[...] = c_new.astype(jnp.float32)
    key_part = jnp.concatenate([part1[:, lora - lat0:], jnp.zeros((rows, lanes - rope_dim), jnp.float32)], axis=-1)
    k_new = rope(key_part)[:, :rope_dim].astype(jnp.bfloat16)
    knew_ref[...] = k_new
    newk[...] = jnp.concatenate([k_new.astype(jnp.float32), jnp.zeros((rows, lanes - rope_dim), jnp.float32)], axis=-1)

    column = lax.broadcasted_iota(jnp.int32, (heads, length), 1)

    def attend(seq0, keys, rope_keys):
        scores, news = [], []
        for s in range(8):
            b = seq0 + s
            q_b = qlat[b].astype(jnp.bfloat16)
            pairs = qrot[b]
            r_b = jnp.concatenate([pairs, pltpu.roll(pairs, lanes // 2, 1)], axis=0).astype(jnp.bfloat16)
            score = lax.dot_general(q_b, keys(s), contract, preferred_element_type=jnp.float32)
            score += jnp.dot(r_b[:, :rope_dim], rope_keys(s), preferred_element_type=jnp.float32)
            scores.append(jnp.where(column < lens_ref[b], score * scale, -jnp.inf))
            r_f = jnp.where(lax.broadcasted_iota(jnp.int32, (heads, lanes), 1) < rope_dim, r_b.astype(jnp.float32), 0.0)
            new = jnp.sum(q_b.astype(jnp.float32) * newc[pl.ds(b, 1), :], axis=-1, keepdims=True)
            news.append((new + jnp.sum(r_f * newk[pl.ds(b, 1), :], axis=-1, keepdims=True)) * scale)
        scores = jnp.concatenate(scores, axis=0)
        news = jnp.concatenate(news, axis=0)
        top = jnp.maximum(jnp.max(scores, axis=-1, keepdims=True), news)
        exp_cache = jnp.exp(scores - top)
        exp_new = jnp.exp(news - top)
        total = jnp.sum(exp_cache, axis=-1, keepdims=True) + exp_new
        prob = (exp_cache / total).astype(jnp.bfloat16)
        prob_new = (exp_new / total).astype(jnp.bfloat16).astype(jnp.float32)
        for s in range(8):
            b = seq0 + s
            out = jnp.dot(prob[s * heads:(s + 1) * heads], keys(s), preferred_element_type=jnp.float32)
            qlat[b] = out + prob_new[s * heads:(s + 1) * heads] * newc[pl.ds(b, 1), :]

    for copy in kr_copies:
        copy.wait()
    for n in range(12, 16):
        cache_copy(n).wait()
    seqs_half = width // rope_dim

    def wide_step(w, carry):
        seq0 = wide_seqs + 8 * w

        def keys(s):
            return gu_buf[1, w, s * length:(s + 1) * length, cache_cols]

        def rope_keys(s):
            return gu_buf[2, 1, pl.ds((seq0 - seqs_half + s) * rope_dim, rope_dim), kr_cols]

        attend(seq0, keys, rope_keys)
        return carry

    lax.fori_loop(0, 2, wide_step, 0)
    hooks[1]()

    def deep_step(it, carry):
        d, i2 = it // 2, lax.rem(it, 2)
        for k in range(2):
            pltpu.make_async_copy(ckv_hbm.at[0:four], dn_buf.at[d, 0:four, pl.ds(pl.multiple_of((2 * i2 + k) * lora, lora), lora)], c_sem.at[2 * it + k]).wait()

        def keys(s):
            cols = pl.ds(pl.multiple_of((2 * i2 + s // 4) * lora, lora), lora)
            return dn_buf[d, (s % 4) * length:(s % 4 + 1) * length, cols]

        def rope_keys(s):
            return gu_buf[2, it // 4, pl.ds((8 * lax.rem(it, 4) + s) * rope_dim, rope_dim), kr_cols]

        attend(8 * it, keys, rope_keys)
        hooks[2](it)
        return carry

    lax.fori_loop(0, wide_seqs // 8, deep_step, 0)

    for copy in uv_copies:
        copy.wait()
    for h in range(heads):
        o_lat = qlat[:, row_of(h), :].astype(jnp.bfloat16)
        uv_half = uvbuf.shape[0] // 2
        uv_head = uvbuf[(h % 2) * uv_half:(h % 2 + 1) * uv_half, :, :, (h // 2) * value_dim:(h // 2 + 1) * value_dim].reshape(lora, value_dim)
        tokx[rows:2 * rows, h * value_dim:(h + 1) * value_dim] = jnp.dot(o_lat, uv_head, preferred_element_type=jnp.float32).astype(jnp.bfloat16)
    parts = []
    for w in range(2):
        out_copies[w].wait()
        parts.append(jnp.dot(tokx[rows:2 * rows], gu_buf[2, w, :, 0:width // 2], preferred_element_type=jnp.float32))
    hooks[3]()
    resid = hidden_ref[...].astype(jnp.float32) + jnp.concatenate(parts, axis=-1)
    return resid.astype(jnp.bfloat16)


def silu(value):
    return value * (1.0 / (1.0 + jnp.exp(-value)))


def layer_kernel(dims, hidden_hbm, lens_ref, ids_ref, again_ref, kgain_ref, gain_ref, router_ref, ckv_hbm, krt_hbm, wq_hbm, dkvt_hbm, uk_hbm, uv_hbm, wo_hbm,
                 sgate_hbm, sup_hbm, sdown_hbm, egate_hbm, eup_hbm, edown_hbm, out_ref, cnew_ref, knew_ref,
                 ublk, tokx, midx, send, recv, acc, table, tail, gu_buf, dn_buf, qlat, qrot, newc, newk,
                 gu_sem, dn_sem, us_sem, ur_sem, ys_sem, yr_sem, a_sem, c_sem):
    group, experts_dev, experts, cap, depth, dp_axis = dims
    rows, width = hidden_hbm.shape
    half = rows // 2
    ff = gu_buf.shape[-1]
    n_shared = sgate_hbm.shape[-1] // ff
    steps = experts_dev + n_shared
    slot16 = 16
    slots = group * slot16
    main = send.shape[-1]
    blk = main // 3
    top_k = ids_ref.shape[0]
    lag = 4
    lanes = 128
    me = lax.axis_index(dp_axis)
    chips = group // 2
    core = lax.rem(me, 2)
    chip = me // 2
    partner = chip * 2 + (1 - core)
    left = lax.rem(chip + chips - 1, chips) * 2 + core
    right = lax.rem(chip + 1, chips) * 2 + core
    far = lax.rem(chip + 2, chips) * 2 + core

    def routed(step):
        return (step >= 1) & (step <= experts_dev)

    def either(condition, action_a, action_b):
        if isinstance(condition, bool):
            (action_a if condition else action_b)()
        else:
            pl.when(condition)(action_a)
            pl.when(jnp.logical_not(condition))(action_b)

    def weights_gu(step, which, hbm, shared_hbm, action):
        slot = step % depth if isinstance(step, int) else lax.rem(step, depth)

        def own():
            getattr(pltpu.make_async_copy(hbm.at[step - 1], gu_buf.at[slot, which], gu_sem.at[slot, which]), action)()

        def shared():
            start = step // (steps - 1) * ff
            cols = pl.ds(start if isinstance(step, int) else pl.multiple_of(start, 128), ff)
            getattr(pltpu.make_async_copy(shared_hbm.at[:, cols], gu_buf.at[slot, which], gu_sem.at[slot, which]), action)()

        either(routed(step), own, shared)

    def weights_dn(step, action):
        slot = step % depth if isinstance(step, int) else lax.rem(step, depth)

        def own():
            getattr(pltpu.make_async_copy(edown_hbm.at[step - 1], dn_buf.at[slot], dn_sem.at[slot]), action)()

        def shared():
            start = step // (steps - 1) * ff
            cols = pl.ds(start if isinstance(step, int) else pl.multiple_of(start, 128), ff)
            getattr(pltpu.make_async_copy(sdown_hbm.at[cols], dn_buf.at[slot], dn_sem.at[slot]), action)()

        either(routed(step), own, shared)

    def fetch(step):
        weights_gu(step, 0, egate_hbm, sgate_hbm, "start")
        weights_gu(step, 1, eup_hbm, sup_hbm, "start")

    barrier = pltpu.get_barrier_semaphore()
    for k in range(1, group):
        pl.semaphore_signal(barrier, inc=1, device_id={dp_axis: lax.rem(me + k, group)}, device_id_type=MESH_ID)

    def freed_deep(it):
        for d in range(depth):
            @pl.when(it == 2 * d + 1)
            def _():
                weights_dn(d, "start")

    hooks = (lambda: fetch(0), lambda: fetch(1), freed_deep, lambda: fetch(2))
    resid = attention_phase((hidden_hbm, out_ref, lens_ref, again_ref, kgain_ref, ckv_hbm, krt_hbm, wq_hbm, dkvt_hbm, uk_hbm, uv_hbm, wo_hbm, cnew_ref, knew_ref,
                             tokx, send, gu_buf, dn_buf, qlat, qrot, newc, newk, acc.at[:, 0:128], a_sem, c_sem), hooks)

    resid = resid.astype(jnp.float32)
    inv = lax.rsqrt(jnp.mean(resid * resid, axis=-1, keepdims=True) + NORM_EPS)
    u = (resid * inv * gain_ref[...].astype(jnp.float32).reshape(1, -1)).astype(jnp.bfloat16)
    expert_i = lax.broadcasted_iota(jnp.int32, (lanes, rows), 0)
    picked = ids_ref[0:1, :] == expert_i
    for k in range(1, top_k):
        picked = picked | (ids_ref[k:k + 1, :] == expert_i)
    tok_a = lax.broadcasted_iota(jnp.int32, (rows, rows), 0)
    tok_b = lax.broadcasted_iota(jnp.int32, (rows, rows), 1)
    before = jnp.where(tok_a < tok_b, 1.0, 0.0).astype(jnp.bfloat16)
    rank = jnp.dot(jnp.where(picked, 1.0, 0.0).astype(jnp.bfloat16), before, preferred_element_type=jnp.float32)
    codes_t = jnp.where(picked, rank, -1.0).astype(jnp.bfloat16)
    same = jnp.where(tok_a == tok_b, 1.0, 0.0).astype(jnp.bfloat16)
    codes = lax.dot_general(same, codes_t, (((1,), (1,)), ((), ())), preferred_element_type=jnp.float32).astype(jnp.bfloat16)
    for h in range(2):
        ublk[me, h, :, :width] = u[h * half:(h + 1) * half]
        ublk[me, h, :, width:] = codes[h * half:(h + 1) * half]
    pl.semaphore_wait(barrier, group - 1)

    def block_copy(block, h, dest, sem_no):
        return pltpu.make_async_remote_copy(src_ref=ublk.at[block, h], dst_ref=ublk.at[block, h], send_sem=us_sem.at[sem_no], recv_sem=ur_sem.at[block, h], device_id={dp_axis: dest}, device_id_type=MESH_ID)

    def crossed(block):
        return lax.rem(block + 1 - 2 * core + group, group)

    first_sends = ((me, 0, right), (me, 1, left), (me, 1, right), (me, 0, left), (me, 0, partner), (me, 1, partner))
    relays = ((left, 0, right), (left, 0, partner), (right, 1, left), (right, 1, partner), (left, 1, partner), (right, 0, partner), (far, 0, partner), (far, 1, partner))
    all_sends = first_sends + relays

    def send_block(n):
        block, h, dest = all_sends[n]
        block_copy(block, h, dest, n).start()

    def arrived(block, h):
        block_copy(block, h, partner, 0).wait_recv()

    for n in range(len(first_sends)):
        send_block(n)

    logits = lax.dot_general(u, router_ref[...], (((1,), (1,)), ((), ())), preferred_element_type=jnp.float32)
    logits = logits - jnp.max(logits, axis=-1, keepdims=True)
    expl = jnp.exp(logits)
    prob = expl / jnp.sum(expl, axis=-1, keepdims=True)
    prob = jnp.concatenate([prob, jnp.zeros((rows, lanes - experts), jnp.float32)], axis=-1)
    p0 = prob.astype(jnp.bfloat16)
    rest = prob - p0.astype(jnp.float32)
    p1 = rest.astype(jnp.bfloat16)
    p2 = (rest - p1.astype(jnp.float32)).astype(jnp.bfloat16)
    table[0] = codes
    table[1] = p0
    table[2] = p1
    table[3] = p2
    acc[...] = resid

    def relay():
        seen = set()
        for n in range(len(first_sends), len(all_sends)):
            block, h, _ = all_sends[n]
            if (id(block), h) not in seen:
                seen.add((id(block), h))
                arrived(block, h)
            send_block(n)
        for block in (partner, crossed(left), crossed(right), crossed(far)):
            for h in range(2):
                arrived(block, h)

    row_i = lax.broadcasted_iota(jnp.int32, (lanes, slots), 0)
    col_i = lax.broadcasted_iota(jnp.int32, (lanes, slots), 1)

    def return_copy(step, dest):
        return pltpu.make_async_remote_copy(src_ref=send.at[step, dest], dst_ref=recv.at[step, me], send_sem=ys_sem.at[step, dest], recv_sem=yr_sem.at[step, me], device_id={dp_axis: dest}, device_id_type=MESH_ID)

    def arrival(step, source):
        return pltpu.make_async_remote_copy(src_ref=send.at[step, source], dst_ref=recv.at[step, source], send_sem=ys_sem.at[step, source], recv_sem=yr_sem.at[step, source], device_id={dp_axis: source}, device_id_type=MESH_ID)

    def gather_rows(expert):
        pick = (row_i == me * experts_dev + expert).astype(jnp.float32).astype(jnp.bfloat16)
        code_all = ublk[:, :, :, width:].reshape(group * rows, lanes)
        code_b = jnp.dot(code_all, pick, preferred_element_type=jnp.float32)
        tok = lax.broadcasted_iota(jnp.int32, (group * rows, slots), 0)
        col = lax.broadcasted_iota(jnp.int32, (group * rows, slots), 1)
        hit = (code_b == lax.rem(col, slot16).astype(jnp.float32)) & (tok // rows == col // slot16)
        place = jnp.where(hit, 1.0, 0.0).astype(jnp.bfloat16)
        for c0 in range(0, width, 512):
            rows_u = ublk[:, :, :, c0:c0 + 512].reshape(group * rows, 512)
            picked_rows = lax.dot_general(place, rows_u, (((0,), (0,)), ((), ())), preferred_element_type=jnp.float32)
            tokx[:, c0:c0 + 512] = picked_rows.astype(jnp.bfloat16)

    def pack_block(y_main, q):
        y_main = y_main.reshape(group, 2, 8, blk)
        y_tail = tail[...].reshape(group, 2, 8, blk)
        sub = lax.broadcasted_iota(jnp.int32, (group, 8, blk), 1)
        part = y_tail[:, 1 if q == 2 else 0]
        if q != 1:
            part = pltpu.roll(part.reshape(group * 8, blk).reshape(group, 8, blk), 4, 1)
        low = jnp.where(sub >= 4, part, y_main[:, 1])
        return jnp.concatenate([y_main[:, 0], low], axis=1).astype(jnp.bfloat16)

    def combine(step):
        for k in range(1, group):
            arrival(step, lax.rem(me + k, group)).wait_recv()
        spread = (row_i == (col_i // slot16) * experts_dev + step).astype(jnp.float32).astype(jnp.bfloat16)
        wide = jnp.dot(table[...].reshape(4 * rows, lanes), spread, preferred_element_type=jnp.float32)
        code_b = wide[:rows]
        slot_i = lax.rem(lax.broadcasted_iota(jnp.int32, (rows, slots), 1), slot16)
        slot_f = slot_i.astype(jnp.float32)
        for q in range(3):
            hits = [code_b == slot_f, (slot_i >= cap) & (code_b == slot_f - cap + 4 * q)]
            lhs = jnp.concatenate([jnp.where(hit, wide[p * rows:(p + 1) * rows], 0.0) for hit in hits for p in (1, 2, 3)], axis=0).astype(jnp.bfloat16)
            y_blk = recv[step, :, :, q * blk:(q + 1) * blk].reshape(slots, blk)
            res = jnp.dot(lhs, y_blk, preferred_element_type=jnp.float32)
            acc[:, q * blk:(q + 1) * blk] += res[:rows] + (res[rows:2 * rows] + res[2 * rows:3 * rows])
            acc[:, main:] += res[3 * rows:4 * rows] + (res[4 * rows:5 * rows] + res[5 * rows:])

    def one_step(step, carry):
        slot = lax.rem(step, depth)
        expert = step - 1
        is_routed = routed(step)

        @pl.when(step == 1)
        def _():
            relay()

        @pl.when(is_routed)
        def _():
            gather_rows(expert)

        @pl.when(jnp.logical_not(is_routed))
        def _():
            tokx[:rows] = ublk[me, :, :, :width].reshape(rows, width)
            tokx[rows:] = jnp.zeros((slots - rows, width), jnp.bfloat16)

        weights_gu(step, 0, egate_hbm, sgate_hbm, "wait")
        weights_gu(step, 1, eup_hbm, sup_hbm, "wait")
        for c0 in range(0, ff, 512):
            c1 = min(c0 + 512, ff)
            gate_act = jnp.dot(tokx[...], gu_buf[slot, 0, :, c0:c1], preferred_element_type=jnp.float32)
            up_act = jnp.dot(tokx[...], gu_buf[slot, 1, :, c0:c1], preferred_element_type=jnp.float32)
            midx[:, c0:c1] = (silu(gate_act) * up_act).astype(jnp.bfloat16)

        @pl.when(step + depth < steps)
        def _():
            fetch(step + depth)

        weights_dn(step, "wait")
        tail[...] = jnp.dot(midx[...], dn_buf[slot, :, main:], preferred_element_type=jnp.float32)

        @pl.when(jnp.logical_not(is_routed))
        def _():
            acc[:, main:] += tail[:rows]

        for q in range(3):
            y_main = jnp.dot(midx[...], dn_buf[slot, :, q * blk:(q + 1) * blk], preferred_element_type=jnp.float32)

            @pl.when(is_routed)
            def _():
                send[expert, :, :, q * blk:(q + 1) * blk] = pack_block(y_main, q)

            @pl.when(jnp.logical_not(is_routed))
            def _():
                acc[:, q * blk:(q + 1) * blk] += y_main[:rows]

        @pl.when(step + depth < steps)
        def _():
            weights_dn(step + depth, "start")

        @pl.when(is_routed)
        def _():
            recv[expert, me] = send[expert, me]
            for k in (4, 3, 5, 2, 6, 1, 7):
                return_copy(expert, lax.rem(me + k, group)).start()

        @pl.when(expert >= lag)
        def _():
            combine(expert - lag)

        return carry

    lax.fori_loop(0, steps, one_step, 0)

    def last_combine(step, carry):
        combine(step)
        return carry

    lax.fori_loop(steps - 1 - lag, experts_dev, last_combine, 0)
    out_ref[...] = acc[...].astype(out_ref.dtype)

    for n, (block, h, dest) in enumerate(all_sends):
        block_copy(block, h, dest, n).wait_send()

    def drain(step, carry):
        for k in range(1, group):
            return_copy(step, lax.rem(me + k, group)).wait_send()
        return carry

    lax.fori_loop(0, experts_dev, drain, 0)


def hand_on(*refs):
    for k in range(3):
        refs[3 + k][...] = refs[k][...]


def layer(group, cap, hidden, ckv_cache, kr_cache, seq_lens, expert_ids, attn_gain, kv_gain, moe_gain, w_q, w_dkv, w_uk, w_uv, w_o, w_router, shared_gate, shared_up, shared_down, expert_gate, expert_up, expert_down):
    rows, width = hidden.shape
    heads, nope, lora = w_uk.shape
    length, rope_dim = kr_cache.shape[1:]
    experts_dev, _, ff = expert_gate.shape
    experts = w_router.shape[1]
    depth = 3
    main = 3 * width // 4
    slots = group * 16
    dims = (group, experts_dev, experts, cap, depth, 'dp')
    vmem = pl.BlockSpec(memory_space=pltpu.VMEM)
    hbm = pl.BlockSpec(memory_space=pl.ANY)
    results = pl.pallas_call(
        functools.partial(layer_kernel, dims),
        out_shape=(jax.ShapeDtypeStruct((rows, width), jnp.bfloat16), jax.ShapeDtypeStruct((rows, lora), jnp.bfloat16), jax.ShapeDtypeStruct((rows, rope_dim), jnp.bfloat16)),
        in_specs=[hbm, pl.BlockSpec(memory_space=pltpu.SMEM)] + [vmem] * 5 + [hbm] * 13,
        out_specs=(vmem, vmem, vmem),
        scratch_shapes=[
            pltpu.VMEM((group, 2, rows // 2, width + 128), jnp.bfloat16),
            pltpu.VMEM((slots, width), jnp.bfloat16),
            pltpu.VMEM((slots, ff), jnp.bfloat16),
            pltpu.VMEM((experts_dev, group, 16, main), jnp.bfloat16),
            pltpu.VMEM((experts_dev, group, 16, main), jnp.bfloat16),
            pltpu.VMEM((rows, width), jnp.float32),
            pltpu.VMEM((4, rows, 128), jnp.bfloat16),
            pltpu.VMEM((slots, width - main), jnp.float32),
            pltpu.VMEM((depth, 2, width, ff), jnp.bfloat16),
            pltpu.VMEM((depth, ff, width), jnp.bfloat16),
            pltpu.VMEM((rows, heads, lora), jnp.float32),
            pltpu.VMEM((rows, heads // 2, 128), jnp.float32),
            pltpu.VMEM((rows, lora), jnp.float32),
            pltpu.VMEM((rows, 128), jnp.float32),
            pltpu.SemaphoreType.DMA((depth, 2)),
            pltpu.SemaphoreType.DMA((depth,)),
            pltpu.SemaphoreType.DMA((14,)),
            pltpu.SemaphoreType.DMA((group, 2)),
            pltpu.SemaphoreType.DMA((experts_dev, group)),
            pltpu.SemaphoreType.DMA((experts_dev, group)),
            pltpu.SemaphoreType.DMA((20,)),
            pltpu.SemaphoreType.DMA((16,)),
        ],
        compiler_params=pltpu.CompilerParams(collective_id=0, has_side_effects=True, vmem_limit_bytes=67043328),
        name='decoder_layer',
    )(hidden, seq_lens, expert_ids.T, attn_gain, kv_gain, moe_gain, w_router.T,
      ckv_cache.reshape(rows * length, lora), jnp.swapaxes(kr_cache, 1, 2).reshape(rows * rope_dim, length), w_q, w_dkv.T, w_uk.reshape(heads * nope, lora),
      w_uv.reshape(heads // 2, experts_dev, group, 16, -1), w_o, shared_gate, shared_up, shared_down, expert_gate, expert_up, expert_down)
    return pl.pallas_call(
        hand_on,
        out_shape=tuple(jax.ShapeDtypeStruct(r.shape, r.dtype) for r in results),
        in_specs=[vmem] * 3,
        out_specs=(vmem,) * 3,
        name='hand_on',
    )(*results)


def solution(mesh):
    row_spec = P(('rep', 'dp'))
    full_spec = P()
    expert_spec = P('dp')

    def device_step(hidden, ckv_cache, kr_cache, seq_lens, expert_ids, attn_gain, kv_gain, moe_gain, w_q, w_dkv, w_uk, w_uv, w_o, w_router, shared_gate, shared_up, shared_down, expert_gate, expert_up, expert_down):
        capacity = max(2, 2 * hidden.shape[0] * expert_ids.shape[1] // w_router.shape[1])
        return layer(mesh.shape['dp'], capacity, hidden, ckv_cache, kr_cache, seq_lens, expert_ids, attn_gain, kv_gain, moe_gain, w_q, w_dkv, w_uk, w_uv, w_o, w_router, shared_gate, shared_up, shared_down, expert_gate, expert_up, expert_down)

    in_specs = (row_spec,) * 5 + (full_spec,) * 12 + (expert_spec,) * 3
    return jax.shard_map(device_step, mesh=mesh, in_specs=in_specs, out_specs=(row_spec, row_spec, row_spec), check_vma=False)
```

```python
import functools
import math

import jax
import jax.numpy as jnp
from jax import lax
from jax.experimental import pallas as pl
from jax.experimental.pallas import tpu as pltpu
from jax.sharding import PartitionSpec as P

NORM_EPS = 1e-6
ROPE_THETA = 10000.0


MESH_ID = pl.DeviceIdType.MESH


def attention_phase(refs, hooks):
    (hidden_hbm, hidden_ref, lens_ref, again_ref, kgain_ref, ckv_hbm, krt_hbm, wq_hbm, dkvt_hbm, uk_hbm, uv_hbm, wo_hbm, cnew_ref, knew_ref,
     tokx, uvbuf, gu_buf, dn_buf, qlat, qrot, newc, newk, pos, a_sem, c_sem) = refs
    rows, width = hidden_ref.shape
    lanes = 128
    tiles = qlat.shape[0]
    lora = tiles * lanes
    heads = qlat.shape[1] // rows
    rope_dim = krt_hbm.shape[0] // rows
    length = krt_hbm.shape[1]
    nope = uk_hbm.shape[0] // heads
    head_dim = nope + rope_dim
    qcols = wq_hbm.shape[1] // 4
    four = 4 * length
    value_dim = uv_hbm.shape[-1]
    scale = head_dim ** -0.5
    lanes = 128
    lat0 = dn_buf.shape[1] - four
    lat1 = dkvt_hbm.shape[0] - lat0
    cache_cols = slice(qcols, qcols + lora)
    kr_cols = slice(width // 2, width // 2 + length)

    def query_copy(i):
        return pltpu.make_async_copy(wq_hbm.at[:, i * qcols:(i + 1) * qcols], gu_buf.at[i // 2, i % 2, :, 0:qcols], a_sem.at[i])

    latent_copies = [
        pltpu.make_async_copy(dkvt_hbm.at[0:lat0], dn_buf.at[1, four:four + lat0], a_sem.at[4]),
        pltpu.make_async_copy(dkvt_hbm.at[lat0:lat0 + lat1], dn_buf.at[2, four:four + lat1], a_sem.at[5]),
    ]
    uk_copy = pltpu.make_async_copy(uk_hbm, gu_buf.at[0, 1, :, cache_cols], a_sem.at[6])
    kr_copies = [pltpu.make_async_copy(krt_hbm.at[w * width:(w + 1) * width], gu_buf.at[2, w, :, kr_cols], a_sem.at[7 + w]) for w in range(2)]
    out_copies = [pltpu.make_async_copy(wo_hbm.at[:, w * (width // 2):(w + 1) * (width // 2)], gu_buf.at[2, w, :, 0:width // 2], a_sem.at[9 + w]) for w in range(2)]
    uv_copies = [pltpu.make_async_copy(uv_hbm.at[i], uvbuf.at[:, :, :, i * value_dim:(i + 1) * value_dim], a_sem.at[11 + i]) for i in range(heads // 2)]
    wide_seqs = 48

    def cache_copy(n):
        if n >= 12:
            w, r = (n - 12) // 2, n % 2
            return pltpu.make_async_copy(ckv_hbm.at[n * four:(n + 1) * four], gu_buf.at[1, w, r * four:(r + 1) * four, cache_cols], c_sem.at[n])
        return pltpu.make_async_copy(ckv_hbm.at[n * four:(n + 1) * four], dn_buf.at[n // 4, 0:four, (n % 4) * lora:(n % 4 + 1) * lora], c_sem.at[n])

    hidden_copy = pltpu.make_async_copy(hidden_hbm, hidden_ref, a_sem.at[19])
    hidden_copy.start()
    query_copy(0).start()
    for copy in latent_copies:
        copy.start()
    uk_copy.start()
    for i in range(1, 4):
        query_copy(i).start()
    for n in range(12, 16):
        cache_copy(n).start()
    for copy in kr_copies:
        copy.start()
    for n in range(8):
        cache_copy(n).start()

    lane = lax.broadcasted_iota(jnp.int32, (rows, lanes), 1)
    hidden_copy.wait()
    hidden = hidden_ref[...].astype(jnp.float32)
    inv = lax.rsqrt(jnp.mean(hidden * hidden, axis=-1, keepdims=True) + NORM_EPS)
    tokx[0:rows] = (hidden * inv * again_ref[...].astype(jnp.float32).reshape(1, -1)).astype(jnp.bfloat16)
    for b in range(rows):
        pos[b:b + 1, :] = jnp.full((1, lanes), lens_ref[b], jnp.int32).astype(jnp.float32)
    quarter = lax.rem(lane, rope_dim // 2).astype(jnp.float32)
    angle = pos[...] * jnp.exp(quarter * (-2.0 / rope_dim * math.log(ROPE_THETA)))
    rope_cos = jnp.cos(angle)
    low_half = lax.rem(lane, rope_dim) < rope_dim // 2
    rope_sin = jnp.where(low_half, -jnp.sin(angle), jnp.sin(angle))

    def rope(value):
        swapped = jnp.where(low_half, pltpu.roll(value, lanes - rope_dim // 2, 1), pltpu.roll(value, rope_dim // 2, 1))
        return value * rope_cos + swapped * rope_sin

    first_half = lane < rope_dim

    def row_of(h):
        return (h % 2) * (heads // 2) + h // 2

    for i in range(4):
        query_copy(i).wait()
        q_cols = jnp.dot(tokx[0:rows], gu_buf[i // 2, i % 2, :, 0:qcols], preferred_element_type=jnp.float32)
        q_cols = q_cols.astype(jnp.bfloat16).astype(jnp.float32)
        if i == 0:
            for copy in uv_copies + out_copies:
                copy.start()
            for n in range(8, 12):
                cache_copy(n).start()
            uk_copy.wait()
        for pair in range(qcols // (2 * head_dim)):
            base = pair * 2 * head_dim
            tile0, tile1, tile2 = (q_cols[:, base + k * lanes:base + (k + 1) * lanes] for k in range(3))
            head = i * (qcols // head_dim) + 2 * pair
            nopes = (tile0, pltpu.roll(jnp.where(first_half, tile2, tile1), lanes // 2, 1))
            turned = rope(jnp.where(first_half, tile1, tile2))
            qrot[:, head // 2, :] = turned
            for odd in range(2):
                h = head + odd
                uk_head = gu_buf[0, 1, h * nope:(h + 1) * nope, cache_cols]
                q_head = jnp.dot(nopes[odd].astype(jnp.bfloat16), uk_head, preferred_element_type=jnp.float32)
                for j in range(tiles):
                    qlat[j, pl.ds(row_of(h), rows, stride=heads), :] = q_head[:, j * lanes:(j + 1) * lanes]
    hooks[0]()

    for copy in latent_copies:
        copy.wait()
    contract = (((1,), (1,)), ((), ()))
    part0 = lax.dot_general(tokx[0:rows], dn_buf[1, four:four + lat0], contract, preferred_element_type=jnp.float32)
    part1 = lax.dot_general(tokx[0:rows], dn_buf[2, four:four + lat1], contract, preferred_element_type=jnp.float32)
    latent = jnp.concatenate([part0, part1[:, :lora - lat0]], axis=-1)
    inv = lax.rsqrt(jnp.mean(latent * latent, axis=-1, keepdims=True) + NORM_EPS)
    c_new = (latent * inv * kgain_ref[...].astype(jnp.float32).reshape(1, -1)).astype(jnp.bfloat16)
    cnew_ref[...] = c_new
    newc[...] = c_new.astype(jnp.float32)
    key_part = jnp.concatenate([part1[:, lora - lat0:], jnp.zeros((rows, lanes - rope_dim), jnp.float32)], axis=-1)
    k_new = rope(key_part)[:, :rope_dim].astype(jnp.bfloat16)
    knew_ref[...] = k_new
    newk[...] = jnp.concatenate([k_new.astype(jnp.float32), jnp.zeros((rows, lanes - rope_dim), jnp.float32)], axis=-1)

    column = lax.broadcasted_iota(jnp.int32, (heads, length), 1)

    def attend(seq0, keys, rope_keys):
        scores, news = [], []
        for s in range(8):
            b = seq0 + s
            q_b = jnp.concatenate([qlat[j, pl.ds(pl.multiple_of(b * heads, heads), heads), :] for j in range(tiles)], axis=-1).astype(jnp.bfloat16)
            pairs = qrot[b]
            r_b = jnp.concatenate([pairs, pltpu.roll(pairs, lanes // 2, 1)], axis=0).astype(jnp.bfloat16)
            score = lax.dot_general(q_b, keys(s), contract, preferred_element_type=jnp.float32)
            score += jnp.dot(r_b[:, :rope_dim], rope_keys(s), preferred_element_type=jnp.float32)
            scores.append(jnp.where(column < lens_ref[b], score * scale, -jnp.inf))
            r_f = jnp.where(lax.broadcasted_iota(jnp.int32, (heads, lanes), 1) < rope_dim, r_b.astype(jnp.float32), 0.0)
            new = jnp.sum(q_b.astype(jnp.float32) * newc[pl.ds(b, 1), :], axis=-1, keepdims=True)
            news.append((new + jnp.sum(r_f * newk[pl.ds(b, 1), :], axis=-1, keepdims=True)) * scale)
        scores = jnp.concatenate(scores, axis=0)
        news = jnp.concatenate(news, axis=0)
        top = jnp.maximum(jnp.max(scores, axis=-1, keepdims=True), news)
        exp_cache = jnp.exp(scores - top)
        exp_new = jnp.exp(news - top)
        total = jnp.sum(exp_cache, axis=-1, keepdims=True) + exp_new
        prob = (exp_cache / total).astype(jnp.bfloat16)
        prob_new = (exp_new / total).astype(jnp.bfloat16).astype(jnp.float32)
        for s in range(8):
            b = seq0 + s
            out = jnp.dot(prob[s * heads:(s + 1) * heads], keys(s), preferred_element_type=jnp.float32)
            out += prob_new[s * heads:(s + 1) * heads] * newc[pl.ds(b, 1), :]
            for j in range(tiles):
                qlat[j, pl.ds(pl.multiple_of(b * heads, heads), heads), :] = out[:, j * lanes:(j + 1) * lanes]

    for copy in kr_copies:
        copy.wait()
    for n in range(12, 16):
        cache_copy(n).wait()
    seqs_half = width // rope_dim

    def wide_step(w, carry):
        seq0 = wide_seqs + 8 * w

        def keys(s):
            return gu_buf[1, w, s * length:(s + 1) * length, cache_cols]

        def rope_keys(s):
            return gu_buf[2, 1, pl.ds((seq0 - seqs_half + s) * rope_dim, rope_dim), kr_cols]

        attend(seq0, keys, rope_keys)
        return carry

    lax.fori_loop(0, 2, wide_step, 0)
    hooks[1]()

    def deep_step(it, carry):
        d, i2 = it // 2, lax.rem(it, 2)
        for k in range(2):
            pltpu.make_async_copy(ckv_hbm.at[0:four], dn_buf.at[d, 0:four, pl.ds(pl.multiple_of((2 * i2 + k) * lora, lora), lora)], c_sem.at[2 * it + k]).wait()

        def keys(s):
            cols = pl.ds(pl.multiple_of((2 * i2 + s // 4) * lora, lora), lora)
            return dn_buf[d, (s % 4) * length:(s % 4 + 1) * length, cols]

        def rope_keys(s):
            return gu_buf[2, it // 4, pl.ds((8 * lax.rem(it, 4) + s) * rope_dim, rope_dim), kr_cols]

        attend(8 * it, keys, rope_keys)
        hooks[2](it)
        return carry

    lax.fori_loop(0, wide_seqs // 8, deep_step, 0)

    for copy in uv_copies:
        copy.wait()
    for h in range(heads):
        o_lat = jnp.concatenate([qlat[j, pl.ds(row_of(h), rows, stride=heads), :] for j in range(tiles)], axis=-1).astype(jnp.bfloat16)
        uv_half = uvbuf.shape[0] // 2
        uv_head = uvbuf[(h % 2) * uv_half:(h % 2 + 1) * uv_half, :, :, (h // 2) * value_dim:(h // 2 + 1) * value_dim].reshape(lora, value_dim)
        tokx[rows:2 * rows, h * value_dim:(h + 1) * value_dim] = jnp.dot(o_lat, uv_head, preferred_element_type=jnp.float32).astype(jnp.bfloat16)
    parts = []
    for w in range(2):
        out_copies[w].wait()
        parts.append(jnp.dot(tokx[rows:2 * rows], gu_buf[2, w, :, 0:width // 2], preferred_element_type=jnp.float32))
    hooks[3]()
    resid = hidden_ref[...].astype(jnp.float32) + jnp.concatenate(parts, axis=-1)
    return resid.astype(jnp.bfloat16)


def silu(value):
    return value * (1.0 / (1.0 + jnp.exp(-value)))


def layer_kernel(dims, hidden_hbm, lens_ref, ids_ref, again_ref, kgain_ref, gain_ref, router_ref, ckv_hbm, krt_hbm, wq_hbm, dkvt_hbm, uk_hbm, uv_hbm, wo_hbm,
                 sgate_hbm, sup_hbm, sdown_hbm, egate_hbm, eup_hbm, edown_hbm, out_ref, cnew_ref, knew_ref,
                 ublk, tokx, midx, send, recv, acc, table, tail, gu_buf, dn_buf, qlat, qrot, newc, newk,
                 gu_sem, dn_sem, us_sem, ur_sem, ys_sem, yr_sem, a_sem, c_sem):
    group, experts_dev, experts, cap, depth, dp_axis = dims
    rows, width = hidden_hbm.shape
    half = rows // 2
    ff = gu_buf.shape[-1]
    n_shared = sgate_hbm.shape[-1] // ff
    steps = experts_dev + n_shared
    slot16 = 16
    slots = group * slot16
    main = send.shape[-1]
    blk = main // 3
    top_k = ids_ref.shape[0]
    lag = 4
    lanes = 128
    me = lax.axis_index(dp_axis)
    chips = group // 2
    core = lax.rem(me, 2)
    chip = me // 2
    partner = chip * 2 + (1 - core)
    left = lax.rem(chip + chips - 1, chips) * 2 + core
    right = lax.rem(chip + 1, chips) * 2 + core
    far = lax.rem(chip + 2, chips) * 2 + core

    def routed(step):
        return (step >= 1) & (step <= experts_dev)

    def either(condition, action_a, action_b):
        if isinstance(condition, bool):
            (action_a if condition else action_b)()
        else:
            pl.when(condition)(action_a)
            pl.when(jnp.logical_not(condition))(action_b)

    def weights_gu(step, which, hbm, shared_hbm, action):
        slot = step % depth if isinstance(step, int) else lax.rem(step, depth)

        def own():
            getattr(pltpu.make_async_copy(hbm.at[step - 1], gu_buf.at[slot, which], gu_sem.at[slot, which]), action)()

        def shared():
            start = step // (steps - 1) * ff
            cols = pl.ds(start if isinstance(step, int) else pl.multiple_of(start, 128), ff)
            getattr(pltpu.make_async_copy(shared_hbm.at[:, cols], gu_buf.at[slot, which], gu_sem.at[slot, which]), action)()

        either(routed(step), own, shared)

    def weights_dn(step, action):
        slot = step % depth if isinstance(step, int) else lax.rem(step, depth)

        def own():
            getattr(pltpu.make_async_copy(edown_hbm.at[step - 1], dn_buf.at[slot], dn_sem.at[slot]), action)()

        def shared():
            start = step // (steps - 1) * ff
            cols = pl.ds(start if isinstance(step, int) else pl.multiple_of(start, 128), ff)
            getattr(pltpu.make_async_copy(sdown_hbm.at[cols], dn_buf.at[slot], dn_sem.at[slot]), action)()

        either(routed(step), own, shared)

    def fetch(step):
        weights_gu(step, 0, egate_hbm, sgate_hbm, "start")
        weights_gu(step, 1, eup_hbm, sup_hbm, "start")

    barrier = pltpu.get_barrier_semaphore()
    for k in range(1, group):
        pl.semaphore_signal(barrier, inc=1, device_id={dp_axis: lax.rem(me + k, group)}, device_id_type=MESH_ID)

    def freed_deep(it):
        for d in range(depth):
            @pl.when(it == 2 * d + 1)
            def _():
                weights_dn(d, "start")

    hooks = (lambda: fetch(0), lambda: fetch(1), freed_deep, lambda: fetch(2))
    resid = attention_phase((hidden_hbm, out_ref, lens_ref, again_ref, kgain_ref, ckv_hbm, krt_hbm, wq_hbm, dkvt_hbm, uk_hbm, uv_hbm, wo_hbm, cnew_ref, knew_ref,
                             tokx, send, gu_buf, dn_buf, qlat, qrot, newc, newk, acc.at[:, 0:128], a_sem, c_sem), hooks)

    resid = resid.astype(jnp.float32)
    inv = lax.rsqrt(jnp.mean(resid * resid, axis=-1, keepdims=True) + NORM_EPS)
    u = (resid * inv * gain_ref[...].astype(jnp.float32).reshape(1, -1)).astype(jnp.bfloat16)
    expert_i = lax.broadcasted_iota(jnp.int32, (lanes, rows), 0)
    picked = ids_ref[0:1, :] == expert_i
    for k in range(1, top_k):
        picked = picked | (ids_ref[k:k + 1, :] == expert_i)
    tok_a = lax.broadcasted_iota(jnp.int32, (rows, rows), 0)
    tok_b = lax.broadcasted_iota(jnp.int32, (rows, rows), 1)
    before = jnp.where(tok_a < tok_b, 1.0, 0.0).astype(jnp.bfloat16)
    rank = jnp.dot(jnp.where(picked, 1.0, 0.0).astype(jnp.bfloat16), before, preferred_element_type=jnp.float32)
    codes_t = jnp.where(picked, rank, -1.0).astype(jnp.bfloat16)
    same = jnp.where(tok_a == tok_b, 1.0, 0.0).astype(jnp.bfloat16)
    codes = lax.dot_general(same, codes_t, (((1,), (1,)), ((), ())), preferred_element_type=jnp.float32).astype(jnp.bfloat16)
    for h in range(2):
        ublk[me, h, :, :width] = u[h * half:(h + 1) * half]
        ublk[me, h, :, width:] = codes[h * half:(h + 1) * half]
    pl.semaphore_wait(barrier, group - 1)

    def block_copy(block, h, dest, sem_no):
        return pltpu.make_async_remote_copy(src_ref=ublk.at[block, h], dst_ref=ublk.at[block, h], send_sem=us_sem.at[sem_no], recv_sem=ur_sem.at[block, h], device_id={dp_axis: dest}, device_id_type=MESH_ID)

    def crossed(block):
        return lax.rem(block + 1 - 2 * core + group, group)

    first_sends = ((me, 0, right), (me, 1, left), (me, 1, right), (me, 0, left), (me, 0, partner), (me, 1, partner))
    relays = ((left, 0, right), (left, 0, partner), (right, 1, left), (right, 1, partner), (left, 1, partner), (right, 0, partner), (far, 0, partner), (far, 1, partner))
    all_sends = first_sends + relays

    def send_block(n):
        block, h, dest = all_sends[n]
        block_copy(block, h, dest, n).start()

    def arrived(block, h):
        block_copy(block, h, partner, 0).wait_recv()

    for n in range(len(first_sends)):
        send_block(n)

    logits = lax.dot_general(u, router_ref[...], (((1,), (1,)), ((), ())), preferred_element_type=jnp.float32)
    logits = logits - jnp.max(logits, axis=-1, keepdims=True)
    expl = jnp.exp(logits)
    prob = expl / jnp.sum(expl, axis=-1, keepdims=True)
    prob = jnp.concatenate([prob, jnp.zeros((rows, lanes - experts), jnp.float32)], axis=-1)
    p0 = prob.astype(jnp.bfloat16)
    rest = prob - p0.astype(jnp.float32)
    p1 = rest.astype(jnp.bfloat16)
    p2 = (rest - p1.astype(jnp.float32)).astype(jnp.bfloat16)
    table[0] = codes
    table[1] = p0
    table[2] = p1
    table[3] = p2
    acc[...] = resid

    def relay():
        seen = set()
        for n in range(len(first_sends), len(all_sends)):
            block, h, _ = all_sends[n]
            if (id(block), h) not in seen:
                seen.add((id(block), h))
                arrived(block, h)
            send_block(n)
        for block in (partner, crossed(left), crossed(right), crossed(far)):
            for h in range(2):
                arrived(block, h)

    row_i = lax.broadcasted_iota(jnp.int32, (lanes, slots), 0)
    col_i = lax.broadcasted_iota(jnp.int32, (lanes, slots), 1)

    def return_copy(step, dest):
        return pltpu.make_async_remote_copy(src_ref=send.at[step, dest], dst_ref=recv.at[step, me], send_sem=ys_sem.at[step, dest], recv_sem=yr_sem.at[step, me], device_id={dp_axis: dest}, device_id_type=MESH_ID)

    def arrival(step, source):
        return pltpu.make_async_remote_copy(src_ref=send.at[step, source], dst_ref=recv.at[step, source], send_sem=ys_sem.at[step, source], recv_sem=yr_sem.at[step, source], device_id={dp_axis: source}, device_id_type=MESH_ID)

    def gather_rows(expert):
        pick = (row_i == me * experts_dev + expert).astype(jnp.float32).astype(jnp.bfloat16)
        code_all = ublk[:, :, :, width:].reshape(group * rows, lanes)
        code_b = jnp.dot(code_all, pick, preferred_element_type=jnp.float32)
        tok = lax.broadcasted_iota(jnp.int32, (group * rows, slots), 0)
        col = lax.broadcasted_iota(jnp.int32, (group * rows, slots), 1)
        hit = (code_b == lax.rem(col, slot16).astype(jnp.float32)) & (tok // rows == col // slot16)
        place = jnp.where(hit, 1.0, 0.0).astype(jnp.bfloat16)
        for c0 in range(0, width, 512):
            rows_u = ublk[:, :, :, c0:c0 + 512].reshape(group * rows, 512)
            picked_rows = lax.dot_general(place, rows_u, (((0,), (0,)), ((), ())), preferred_element_type=jnp.float32)
            tokx[:, c0:c0 + 512] = picked_rows.astype(jnp.bfloat16)

    def pack_block(y_main, q):
        y_main = y_main.reshape(group, 2, 8, blk)
        y_tail = tail[...].reshape(group, 2, 8, blk)
        sub = lax.broadcasted_iota(jnp.int32, (group, 8, blk), 1)
        part = y_tail[:, 1 if q == 2 else 0]
        if q != 1:
            part = pltpu.roll(part.reshape(group * 8, blk).reshape(group, 8, blk), 4, 1)
        low = jnp.where(sub >= 4, part, y_main[:, 1])
        return jnp.concatenate([y_main[:, 0], low], axis=1).astype(jnp.bfloat16)

    def combine(step):
        for k in range(1, group):
            arrival(step, lax.rem(me + k, group)).wait_recv()
        spread = (row_i == (col_i // slot16) * experts_dev + step).astype(jnp.float32).astype(jnp.bfloat16)
        wide = jnp.dot(table[...].reshape(4 * rows, lanes), spread, preferred_element_type=jnp.float32)
        code_b = wide[:rows]
        slot_i = lax.rem(lax.broadcasted_iota(jnp.int32, (rows, slots), 1), slot16)
        slot_f = slot_i.astype(jnp.float32)
        for q in range(3):
            hits = [code_b == slot_f, (slot_i >= cap) & (code_b == slot_f - cap + 4 * q)]
            lhs = jnp.concatenate([jnp.where(hit, wide[p * rows:(p + 1) * rows], 0.0) for hit in hits for p in (1, 2, 3)], axis=0).astype(jnp.bfloat16)
            y_blk = recv[step, :, :, q * blk:(q + 1) * blk].reshape(slots, blk)
            res = jnp.dot(lhs, y_blk, preferred_element_type=jnp.float32)
            acc[:, q * blk:(q + 1) * blk] += res[:rows] + (res[rows:2 * rows] + res[2 * rows:3 * rows])
            acc[:, main:] += res[3 * rows:4 * rows] + (res[4 * rows:5 * rows] + res[5 * rows:])

    def one_step(step, carry):
        slot = lax.rem(step, depth)
        expert = step - 1
        is_routed = routed(step)

        @pl.when(step == 1)
        def _():
            relay()

        @pl.when(is_routed)
        def _():
            gather_rows(expert)

        @pl.when(jnp.logical_not(is_routed))
        def _():
            tokx[:rows] = ublk[me, :, :, :width].reshape(rows, width)
            tokx[rows:] = jnp.zeros((slots - rows, width), jnp.bfloat16)

        weights_gu(step, 0, egate_hbm, sgate_hbm, "wait")
        weights_gu(step, 1, eup_hbm, sup_hbm, "wait")
        for c0 in range(0, ff, 512):
            c1 = min(c0 + 512, ff)
            gate_act = jnp.dot(tokx[...], gu_buf[slot, 0, :, c0:c1], preferred_element_type=jnp.float32)
            up_act = jnp.dot(tokx[...], gu_buf[slot, 1, :, c0:c1], preferred_element_type=jnp.float32)
            midx[:, c0:c1] = (silu(gate_act) * up_act).astype(jnp.bfloat16)

        @pl.when(step + depth < steps)
        def _():
            fetch(step + depth)

        weights_dn(step, "wait")
        tail[...] = jnp.dot(midx[...], dn_buf[slot, :, main:], preferred_element_type=jnp.float32)

        @pl.when(jnp.logical_not(is_routed))
        def _():
            acc[:, main:] += tail[:rows]

        for q in range(3):
            y_main = jnp.dot(midx[...], dn_buf[slot, :, q * blk:(q + 1) * blk], preferred_element_type=jnp.float32)

            @pl.when(is_routed)
            def _():
                send[expert, :, :, q * blk:(q + 1) * blk] = pack_block(y_main, q)

            @pl.when(jnp.logical_not(is_routed))
            def _():
                acc[:, q * blk:(q + 1) * blk] += y_main[:rows]

        @pl.when(step + depth < steps)
        def _():
            weights_dn(step + depth, "start")

        @pl.when(is_routed)
        def _():
            recv[expert, me] = send[expert, me]
            for k in (4, 3, 5, 2, 6, 1, 7):
                return_copy(expert, lax.rem(me + k, group)).start()

        @pl.when(expert >= lag)
        def _():
            combine(expert - lag)

        return carry

    lax.fori_loop(0, steps, one_step, 0)

    def last_combine(step, carry):
        combine(step)
        return carry

    lax.fori_loop(steps - 1 - lag, experts_dev, last_combine, 0)
    out_ref[...] = acc[...].astype(out_ref.dtype)

    for n, (block, h, dest) in enumerate(all_sends):
        block_copy(block, h, dest, n).wait_send()

    def drain(step, carry):
        for k in range(1, group):
            return_copy(step, lax.rem(me + k, group)).wait_send()
        return carry

    lax.fori_loop(0, experts_dev, drain, 0)


def hand_on(*refs):
    for k in range(3):
        refs[3 + k][...] = refs[k][...]


def layer(group, cap, hidden, ckv_cache, kr_cache, seq_lens, expert_ids, attn_gain, kv_gain, moe_gain, w_q, w_dkv, w_uk, w_uv, w_o, w_router, shared_gate, shared_up, shared_down, expert_gate, expert_up, expert_down):
    rows, width = hidden.shape
    heads, nope, lora = w_uk.shape
    length, rope_dim = kr_cache.shape[1:]
    experts_dev, _, ff = expert_gate.shape
    experts = w_router.shape[1]
    depth = 3
    main = 3 * width // 4
    slots = group * 16
    dims = (group, experts_dev, experts, cap, depth, 'dp')
    vmem = pl.BlockSpec(memory_space=pltpu.VMEM)
    hbm = pl.BlockSpec(memory_space=pl.ANY)
    results = pl.pallas_call(
        functools.partial(layer_kernel, dims),
        out_shape=(jax.ShapeDtypeStruct((rows, width), jnp.bfloat16), jax.ShapeDtypeStruct((rows, lora), jnp.bfloat16), jax.ShapeDtypeStruct((rows, rope_dim), jnp.bfloat16)),
        in_specs=[hbm, pl.BlockSpec(memory_space=pltpu.SMEM)] + [vmem] * 5 + [hbm] * 13,
        out_specs=(vmem, vmem, vmem),
        scratch_shapes=[
            pltpu.VMEM((group, 2, rows // 2, width + 128), jnp.bfloat16),
            pltpu.VMEM((slots, width), jnp.bfloat16),
            pltpu.VMEM((slots, ff), jnp.bfloat16),
            pltpu.VMEM((experts_dev, group, 16, main), jnp.bfloat16),
            pltpu.VMEM((experts_dev, group, 16, main), jnp.bfloat16),
            pltpu.VMEM((rows, width), jnp.float32),
            pltpu.VMEM((4, rows, 128), jnp.bfloat16),
            pltpu.VMEM((slots, width - main), jnp.float32),
            pltpu.VMEM((depth, 2, width, ff), jnp.bfloat16),
            pltpu.VMEM((depth, ff, width), jnp.bfloat16),
            pltpu.VMEM((lora // 128, rows * heads, 128), jnp.float32),
            pltpu.VMEM((rows, heads // 2, 128), jnp.float32),
            pltpu.VMEM((rows, lora), jnp.float32),
            pltpu.VMEM((rows, 128), jnp.float32),
            pltpu.SemaphoreType.DMA((depth, 2)),
            pltpu.SemaphoreType.DMA((depth,)),
            pltpu.SemaphoreType.DMA((14,)),
            pltpu.SemaphoreType.DMA((group, 2)),
            pltpu.SemaphoreType.DMA((experts_dev, group)),
            pltpu.SemaphoreType.DMA((experts_dev, group)),
            pltpu.SemaphoreType.DMA((20,)),
            pltpu.SemaphoreType.DMA((16,)),
        ],
        compiler_params=pltpu.CompilerParams(collective_id=0, has_side_effects=True, vmem_limit_bytes=67043328),
        name='decoder_layer',
    )(hidden, seq_lens, expert_ids.T, attn_gain, kv_gain, moe_gain, w_router.T,
      ckv_cache.reshape(rows * length, lora), jnp.swapaxes(kr_cache, 1, 2).reshape(rows * rope_dim, length), w_q, w_dkv.T, w_uk.reshape(heads * nope, lora),
      w_uv.reshape(heads // 2, experts_dev, group, 16, -1), w_o, shared_gate, shared_up, shared_down, expert_gate, expert_up, expert_down)
    return pl.pallas_call(
        hand_on,
        out_shape=tuple(jax.ShapeDtypeStruct(r.shape, r.dtype) for r in results),
        in_specs=[vmem] * 3,
        out_specs=(vmem,) * 3,
        name='hand_on',
    )(*results)


def solution(mesh):
    row_spec = P(('rep', 'dp'))
    full_spec = P()
    expert_spec = P('dp')

    def device_step(hidden, ckv_cache, kr_cache, seq_lens, expert_ids, attn_gain, kv_gain, moe_gain, w_q, w_dkv, w_uk, w_uv, w_o, w_router, shared_gate, shared_up, shared_down, expert_gate, expert_up, expert_down):
        capacity = max(2, 2 * hidden.shape[0] * expert_ids.shape[1] // w_router.shape[1])
        return layer(mesh.shape['dp'], capacity, hidden, ckv_cache, kr_cache, seq_lens, expert_ids, attn_gain, kv_gain, moe_gain, w_q, w_dkv, w_uk, w_uv, w_o, w_router, shared_gate, shared_up, shared_down, expert_gate, expert_up, expert_down)

    in_specs = (row_spec,) * 5 + (full_spec,) * 12 + (expert_spec,) * 3
    return jax.shard_map(device_step, mesh=mesh, in_specs=in_specs, out_specs=(row_spec, row_spec, row_spec), check_vma=False)
```

```python
import functools
import math

import jax
import jax.numpy as jnp
from jax import lax
from jax.experimental import pallas as pl
from jax.experimental.pallas import tpu as pltpu
from jax.sharding import PartitionSpec as P

NORM_EPS = 1e-6
ROPE_THETA = 10000.0


MESH_ID = pl.DeviceIdType.MESH


def attention_phase(refs, hooks):
    (hidden_hbm, hidden_ref, lens_ref, again_ref, kgain_ref, ckv_hbm, krt_hbm, wq_hbm, dkvt_hbm, uk_hbm, uv_hbm, wo_hbm, cnew_ref, knew_ref,
     tokx, uvbuf, gu_buf, dn_buf, qlat, qrot, newc, newk, pos, a_sem, c_sem) = refs
    rows, width = hidden_ref.shape
    lanes = 128
    tiles = qlat.shape[0]
    lora = tiles * lanes
    heads = qlat.shape[1] // rows
    rope_dim = krt_hbm.shape[0] // rows
    length = krt_hbm.shape[1]
    nope = uk_hbm.shape[0] // heads
    head_dim = nope + rope_dim
    qcols = wq_hbm.shape[1] // 4
    four = 4 * length
    value_dim = uv_hbm.shape[-1]
    scale = head_dim ** -0.5
    lanes = 128
    lat0 = dn_buf.shape[1] - four
    lat1 = dkvt_hbm.shape[0] - lat0
    cache_cols = slice(qcols, qcols + lora)
    kr_cols = slice(width // 2, width // 2 + length)

    def query_copy(i):
        return pltpu.make_async_copy(wq_hbm.at[:, i * qcols:(i + 1) * qcols], gu_buf.at[i // 2, i % 2, :, 0:qcols], a_sem.at[i])

    latent_copies = [
        pltpu.make_async_copy(dkvt_hbm.at[0:lat0], dn_buf.at[1, four:four + lat0], a_sem.at[4]),
        pltpu.make_async_copy(dkvt_hbm.at[lat0:lat0 + lat1], dn_buf.at[2, four:four + lat1], a_sem.at[5]),
    ]
    uk_copy = pltpu.make_async_copy(uk_hbm, gu_buf.at[0, 1, :, cache_cols], a_sem.at[6])
    kr_copies = [pltpu.make_async_copy(krt_hbm.at[w * width:(w + 1) * width], gu_buf.at[2, w, :, kr_cols], a_sem.at[7 + w]) for w in range(2)]
    out_copies = [pltpu.make_async_copy(wo_hbm.at[:, w * (width // 2):(w + 1) * (width // 2)], gu_buf.at[2, w, :, 0:width // 2], a_sem.at[9 + w]) for w in range(2)]
    uv_copies = [pltpu.make_async_copy(uv_hbm.at[i], uvbuf.at[:, :, :, i * value_dim:(i + 1) * value_dim], a_sem.at[11 + i]) for i in range(heads // 2)]
    wide_seqs = 48

    def cache_copy(n):
        if n >= 12:
            w, r = (n - 12) // 2, n % 2
            return pltpu.make_async_copy(ckv_hbm.at[n * four:(n + 1) * four], gu_buf.at[1, w, r * four:(r + 1) * four, cache_cols], c_sem.at[n])
        return pltpu.make_async_copy(ckv_hbm.at[n * four:(n + 1) * four], dn_buf.at[n // 4, 0:four, (n % 4) * lora:(n % 4 + 1) * lora], c_sem.at[n])

    hidden_copy = pltpu.make_async_copy(hidden_hbm, hidden_ref, a_sem.at[19])
    hidden_copy.start()
    query_copy(0).start()
    for copy in latent_copies:
        copy.start()
    uk_copy.start()
    for i in range(1, 4):
        query_copy(i).start()
    for n in range(12, 16):
        cache_copy(n).start()
    for copy in kr_copies:
        copy.start()
    for n in range(8):
        cache_copy(n).start()

    lane = lax.broadcasted_iota(jnp.int32, (rows, lanes), 1)
    hidden_copy.wait()
    hidden = hidden_ref[...].astype(jnp.float32)
    inv = lax.rsqrt(jnp.mean(hidden * hidden, axis=-1, keepdims=True) + NORM_EPS)
    tokx[0:rows] = (hidden * inv * again_ref[...].astype(jnp.float32).reshape(1, -1)).astype(jnp.bfloat16)
    for b in range(rows):
        pos[b:b + 1, :] = jnp.full((1, lanes), lens_ref[b], jnp.int32).astype(jnp.float32)
    quarter = lax.rem(lane, rope_dim // 2).astype(jnp.float32)
    angle = pos[...] * jnp.exp(quarter * (-2.0 / rope_dim * math.log(ROPE_THETA)))
    rope_cos = jnp.cos(angle)
    low_half = lax.rem(lane, rope_dim) < rope_dim // 2
    rope_sin = jnp.where(low_half, -jnp.sin(angle), jnp.sin(angle))

    def rope(value):
        swapped = jnp.where(low_half, pltpu.roll(value, lanes - rope_dim // 2, 1), pltpu.roll(value, rope_dim // 2, 1))
        return value * rope_cos + swapped * rope_sin

    first_half = lane < rope_dim

    def row_of(h):
        return (h % 2) * (heads // 2) + h // 2

    for i in range(4):
        query_copy(i).wait()
        q_cols = jnp.dot(tokx[0:rows], gu_buf[i // 2, i % 2, :, 0:qcols], preferred_element_type=jnp.float32)
        q_cols = q_cols.astype(jnp.bfloat16).astype(jnp.float32)
        if i == 0:
            for n in range(8, 12):
                cache_copy(n).start()
            for copy in uv_copies + out_copies:
                copy.start()
            uk_copy.wait()
        for pair in range(qcols // (2 * head_dim)):
            base = pair * 2 * head_dim
            tile0, tile1, tile2 = (q_cols[:, base + k * lanes:base + (k + 1) * lanes] for k in range(3))
            head = i * (qcols // head_dim) + 2 * pair
            nopes = (tile0, pltpu.roll(jnp.where(first_half, tile2, tile1), lanes // 2, 1))
            turned = rope(jnp.where(first_half, tile1, tile2))
            qrot[:, head // 2, :] = turned
            for odd in range(2):
                h = head + odd
                uk_head = gu_buf[0, 1, h * nope:(h + 1) * nope, cache_cols]
                q_head = jnp.dot(nopes[odd].astype(jnp.bfloat16), uk_head, preferred_element_type=jnp.float32)
                for j in range(tiles):
                    qlat[j, pl.ds(row_of(h), rows, stride=heads), :] = q_head[:, j * lanes:(j + 1) * lanes]
    hooks[0]()

    for copy in latent_copies:
        copy.wait()
    contract = (((1,), (1,)), ((), ()))
    part0 = lax.dot_general(tokx[0:rows], dn_buf[1, four:four + lat0], contract, preferred_element_type=jnp.float32)
    part1 = lax.dot_general(tokx[0:rows], dn_buf[2, four:four + lat1], contract, preferred_element_type=jnp.float32)
    latent = jnp.concatenate([part0, part1[:, :lora - lat0]], axis=-1)
    inv = lax.rsqrt(jnp.mean(latent * latent, axis=-1, keepdims=True) + NORM_EPS)
    c_new = (latent * inv * kgain_ref[...].astype(jnp.float32).reshape(1, -1)).astype(jnp.bfloat16)
    cnew_ref[...] = c_new
    newc[...] = c_new.astype(jnp.float32)
    key_part = jnp.concatenate([part1[:, lora - lat0:], jnp.zeros((rows, lanes - rope_dim), jnp.float32)], axis=-1)
    k_new = rope(key_part)[:, :rope_dim].astype(jnp.bfloat16)
    knew_ref[...] = k_new
    newk[...] = jnp.concatenate([k_new.astype(jnp.float32), jnp.zeros((rows, lanes - rope_dim), jnp.float32)], axis=-1)

    column = lax.broadcasted_iota(jnp.int32, (heads, length), 1)

    def attend(seq0, keys, rope_keys):
        scores, news = [], []
        for s in range(8):
            b = seq0 + s
            q_b = jnp.concatenate([qlat[j, pl.ds(pl.multiple_of(b * heads, heads), heads), :] for j in range(tiles)], axis=-1).astype(jnp.bfloat16)
            pairs = qrot[b]
            r_b = jnp.concatenate([pairs, pltpu.roll(pairs, lanes // 2, 1)], axis=0).astype(jnp.bfloat16)
            score = lax.dot_general(q_b, keys(s), contract, preferred_element_type=jnp.float32)
            score += jnp.dot(r_b[:, :rope_dim], rope_keys(s), preferred_element_type=jnp.float32)
            scores.append(jnp.where(column < lens_ref[b], score * scale, -jnp.inf))
            r_f = jnp.where(lax.broadcasted_iota(jnp.int32, (heads, lanes), 1) < rope_dim, r_b.astype(jnp.float32), 0.0)
            new = jnp.sum(q_b.astype(jnp.float32) * newc[pl.ds(b, 1), :], axis=-1, keepdims=True)
            news.append((new + jnp.sum(r_f * newk[pl.ds(b, 1), :], axis=-1, keepdims=True)) * scale)
        scores = jnp.concatenate(scores, axis=0)
        news = jnp.concatenate(news, axis=0)
        top = jnp.maximum(jnp.max(scores, axis=-1, keepdims=True), news)
        exp_cache = jnp.exp(scores - top)
        exp_new = jnp.exp(news - top)
        total = jnp.sum(exp_cache, axis=-1, keepdims=True) + exp_new
        prob = (exp_cache / total).astype(jnp.bfloat16)
        prob_new = (exp_new / total).astype(jnp.bfloat16).astype(jnp.float32)
        for s in range(8):
            b = seq0 + s
            out = jnp.dot(prob[s * heads:(s + 1) * heads], keys(s), preferred_element_type=jnp.float32)
            out += prob_new[s * heads:(s + 1) * heads] * newc[pl.ds(b, 1), :]
            for j in range(tiles):
                qlat[j, pl.ds(pl.multiple_of(b * heads, heads), heads), :] = out[:, j * lanes:(j + 1) * lanes]

    for copy in kr_copies:
        copy.wait()
    for n in range(12, 16):
        cache_copy(n).wait()
    seqs_half = width // rope_dim

    def wide_step(w, carry):
        seq0 = wide_seqs + 8 * w

        def keys(s):
            return gu_buf[1, w, s * length:(s + 1) * length, cache_cols]

        def rope_keys(s):
            return gu_buf[2, 1, pl.ds((seq0 - seqs_half + s) * rope_dim, rope_dim), kr_cols]

        attend(seq0, keys, rope_keys)
        return carry

    lax.fori_loop(0, 2, wide_step, 0)
    hooks[1]()

    def deep_step(it, carry):
        d, i2 = it // 2, lax.rem(it, 2)
        for k in range(2):
            pltpu.make_async_copy(ckv_hbm.at[0:four], dn_buf.at[d, 0:four, pl.ds(pl.multiple_of((2 * i2 + k) * lora, lora), lora)], c_sem.at[2 * it + k]).wait()

        def keys(s):
            cols = pl.ds(pl.multiple_of((2 * i2 + s // 4) * lora, lora), lora)
            return dn_buf[d, (s % 4) * length:(s % 4 + 1) * length, cols]

        def rope_keys(s):
            return gu_buf[2, it // 4, pl.ds((8 * lax.rem(it, 4) + s) * rope_dim, rope_dim), kr_cols]

        attend(8 * it, keys, rope_keys)
        hooks[2](it)
        return carry

    lax.fori_loop(0, wide_seqs // 8, deep_step, 0)

    for copy in uv_copies:
        copy.wait()
    for h in range(heads):
        o_lat = jnp.concatenate([qlat[j, pl.ds(row_of(h), rows, stride=heads), :] for j in range(tiles)], axis=-1).astype(jnp.bfloat16)
        uv_half = uvbuf.shape[0] // 2
        uv_head = uvbuf[(h % 2) * uv_half:(h % 2 + 1) * uv_half, :, :, (h // 2) * value_dim:(h // 2 + 1) * value_dim].reshape(lora, value_dim)
        tokx[rows:2 * rows, h * value_dim:(h + 1) * value_dim] = jnp.dot(o_lat, uv_head, preferred_element_type=jnp.float32).astype(jnp.bfloat16)
    parts = []
    for w in range(2):
        out_copies[w].wait()
        parts.append(jnp.dot(tokx[rows:2 * rows], gu_buf[2, w, :, 0:width // 2], preferred_element_type=jnp.float32))
    hooks[3]()
    resid = hidden_ref[...].astype(jnp.float32) + jnp.concatenate(parts, axis=-1)
    return resid.astype(jnp.bfloat16)


def silu(value):
    return value * (1.0 / (1.0 + jnp.exp(-value)))


def layer_kernel(dims, hidden_hbm, lens_ref, ids_ref, again_ref, kgain_ref, gain_ref, router_ref, ckv_hbm, krt_hbm, wq_hbm, dkvt_hbm, uk_hbm, uv_hbm, wo_hbm,
                 sgate_hbm, sup_hbm, sdown_hbm, egate_hbm, eup_hbm, edown_hbm, out_ref, cnew_ref, knew_ref,
                 ublk, tokx, midx, send, recv, acc, table, tail, gu_buf, dn_buf, qlat, qrot, newc, newk,
                 gu_sem, dn_sem, us_sem, ur_sem, ys_sem, yr_sem, a_sem, c_sem):
    group, experts_dev, experts, cap, depth, dp_axis = dims
    rows, width = hidden_hbm.shape
    half = rows // 2
    ff = gu_buf.shape[-1]
    n_shared = sgate_hbm.shape[-1] // ff
    steps = experts_dev + n_shared
    slot16 = 16
    slots = group * slot16
    main = send.shape[-1]
    blk = main // 3
    top_k = ids_ref.shape[0]
    lag = 4
    lanes = 128
    me = lax.axis_index(dp_axis)
    chips = group // 2
    core = lax.rem(me, 2)
    chip = me // 2
    partner = chip * 2 + (1 - core)
    left = lax.rem(chip + chips - 1, chips) * 2 + core
    right = lax.rem(chip + 1, chips) * 2 + core
    far = lax.rem(chip + 2, chips) * 2 + core

    def routed(step):
        return (step >= 1) & (step <= experts_dev)

    def act(copy, action):
        getattr(copy, action)()

    def either(condition, action_a, action_b):
        if isinstance(condition, bool):
            (action_a if condition else action_b)()
        else:
            pl.when(condition)(action_a)
            pl.when(jnp.logical_not(condition))(action_b)

    def weights_gu(step, which, hbm, shared_hbm, action):
        slot = step % depth if isinstance(step, int) else lax.rem(step, depth)

        def own():
            getattr(pltpu.make_async_copy(hbm.at[step - 1], gu_buf.at[slot, which], gu_sem.at[slot, which]), action)()

        def shared():
            start = step // (steps - 1) * ff
            cols = pl.ds(start if isinstance(step, int) else pl.multiple_of(start, 128), ff)
            getattr(pltpu.make_async_copy(shared_hbm.at[:, cols], gu_buf.at[slot, which], gu_sem.at[slot, which]), action)()

        either(routed(step), own, shared)

    def weights_dn(step, action, part=None):
        slot = step % depth if isinstance(step, int) else lax.rem(step, depth)
        first, count = (0, ff) if part is None else (part * (ff // 2), ff // 2)

        def own():
            act(pltpu.make_async_copy(edown_hbm.at[step - 1, first:first + count], dn_buf.at[slot, first:first + count], dn_sem.at[slot]), action)

        def shared():
            start = step // (steps - 1) * ff + first
            cols = pl.ds(start if isinstance(step, int) else pl.multiple_of(start, 64), count)
            act(pltpu.make_async_copy(sdown_hbm.at[cols], dn_buf.at[slot, first:first + count], dn_sem.at[slot]), action)

        either(routed(step), own, shared)

    def fetch(step):
        weights_gu(step, 0, egate_hbm, sgate_hbm, "start")
        weights_gu(step, 1, eup_hbm, sup_hbm, "start")

    barrier = pltpu.get_barrier_semaphore()
    for k in range(1, group):
        pl.semaphore_signal(barrier, inc=1, device_id={dp_axis: lax.rem(me + k, group)}, device_id_type=MESH_ID)

    def freed_deep(it):
        @pl.when(it == 3)
        def _():
            fetch(0)

        @pl.when(it == 4)
        def _():
            weights_dn(0, "start")

        @pl.when(it == 5)
        def _():
            weights_gu(1, 0, egate_hbm, sgate_hbm, "start")

    def nothing():
        pass

    hooks = (nothing, nothing, freed_deep, nothing)
    resid = attention_phase((hidden_hbm, out_ref, lens_ref, again_ref, kgain_ref, ckv_hbm, krt_hbm, wq_hbm, dkvt_hbm, uk_hbm, uv_hbm, wo_hbm, cnew_ref, knew_ref,
                             tokx, send, gu_buf, dn_buf, qlat, qrot, newc, newk, acc.at[:, 0:128], a_sem, c_sem), hooks)

    resid = resid.astype(jnp.float32)
    inv = lax.rsqrt(jnp.mean(resid * resid, axis=-1, keepdims=True) + NORM_EPS)
    u = (resid * inv * gain_ref[...].astype(jnp.float32).reshape(1, -1)).astype(jnp.bfloat16)
    expert_i = lax.broadcasted_iota(jnp.int32, (lanes, rows), 0)
    picked = ids_ref[0:1, :] == expert_i
    for k in range(1, top_k):
        picked = picked | (ids_ref[k:k + 1, :] == expert_i)
    tok_a = lax.broadcasted_iota(jnp.int32, (rows, rows), 0)
    tok_b = lax.broadcasted_iota(jnp.int32, (rows, rows), 1)
    before = jnp.where(tok_a < tok_b, 1.0, 0.0).astype(jnp.bfloat16)
    rank = jnp.dot(jnp.where(picked, 1.0, 0.0).astype(jnp.bfloat16), before, preferred_element_type=jnp.float32)
    codes_t = jnp.where(picked, rank, -1.0).astype(jnp.bfloat16)
    same = jnp.where(tok_a == tok_b, 1.0, 0.0).astype(jnp.bfloat16)
    codes = lax.dot_general(same, codes_t, (((1,), (1,)), ((), ())), preferred_element_type=jnp.float32).astype(jnp.bfloat16)
    for h in range(2):
        ublk[me, h, :, :width] = u[h * half:(h + 1) * half]
        ublk[me, h, :, width:] = codes[h * half:(h + 1) * half]
    pl.semaphore_wait(barrier, group - 1)

    def block_copy(block, h, dest, sem_no):
        return pltpu.make_async_remote_copy(src_ref=ublk.at[block, h], dst_ref=ublk.at[block, h], send_sem=us_sem.at[sem_no], recv_sem=ur_sem.at[block, h], device_id={dp_axis: dest}, device_id_type=MESH_ID)

    def crossed(block):
        return lax.rem(block + 1 - 2 * core + group, group)

    all_sends = ((me, 0, right), (me, 1, left), (me, 1, right), (me, 0, left), (me, 0, partner), (me, 1, partner),
                 (left, 0, right), (right, 1, left), (left, 0, partner), (right, 1, partner),
                 (left, 1, partner), (right, 0, partner), (far, 0, partner), (far, 1, partner))

    def send_block(n):
        block, h, dest = all_sends[n]
        block_copy(block, h, dest, n).start()

    def arrived(block, h):
        block_copy(block, h, partner, 0).wait_recv()

    for n in (0, 1, 4, 5):
        send_block(n)
    weights_gu(1, 1, eup_hbm, sup_hbm, "start")
    weights_dn(1, "start")
    for n in (2, 3):
        send_block(n)

    def first_relay():
        arrived(left, 0)
        send_block(8)
        arrived(right, 1)
        send_block(9)
        weights_gu(2, 0, egate_hbm, sgate_hbm, "start")
        send_block(6)
        send_block(7)
        weights_gu(2, 1, eup_hbm, sup_hbm, "start")

    def relay():
        arrived(left, 1)
        send_block(10)
        arrived(right, 0)
        send_block(11)
        weights_dn(2, "start")
        weights_gu(3, 0, egate_hbm, sgate_hbm, "start")
        arrived(far, 0)
        send_block(12)
        arrived(far, 1)
        send_block(13)
        weights_gu(3, 1, eup_hbm, sup_hbm, "start")
        weights_dn(3, "start")
        for block in (partner, crossed(left), crossed(right), crossed(far)):
            for h in range(2):
                arrived(block, h)

    logits = lax.dot_general(u, router_ref[...], (((1,), (1,)), ((), ())), preferred_element_type=jnp.float32)
    logits = logits - jnp.max(logits, axis=-1, keepdims=True)
    expl = jnp.exp(logits)
    prob = expl / jnp.sum(expl, axis=-1, keepdims=True)
    prob = jnp.concatenate([prob, jnp.zeros((rows, lanes - experts), jnp.float32)], axis=-1)
    p0 = prob.astype(jnp.bfloat16)
    rest = prob - p0.astype(jnp.float32)
    p1 = rest.astype(jnp.bfloat16)
    p2 = (rest - p1.astype(jnp.float32)).astype(jnp.bfloat16)
    table[0] = codes
    table[1] = p0
    table[2] = p1
    table[3] = p2
    acc[...] = resid

    row_i = lax.broadcasted_iota(jnp.int32, (lanes, slots), 0)
    col_i = lax.broadcasted_iota(jnp.int32, (lanes, slots), 1)

    def return_copy(step, dest):
        return pltpu.make_async_remote_copy(src_ref=send.at[step, dest], dst_ref=recv.at[step, me], send_sem=ys_sem.at[step, dest], recv_sem=yr_sem.at[step, me], device_id={dp_axis: dest}, device_id_type=MESH_ID)

    def arrival(step, source):
        return pltpu.make_async_remote_copy(src_ref=send.at[step, source], dst_ref=recv.at[step, source], send_sem=ys_sem.at[step, source], recv_sem=yr_sem.at[step, source], device_id={dp_axis: source}, device_id_type=MESH_ID)

    groups = ((far, partner), (right, left), (crossed(far),), (crossed(right), crossed(left)))

    def send_group(step, n):
        for dest in groups[n]:
            return_copy(step, dest).start()

    def gather_rows(expert):
        pick = (row_i == me * experts_dev + expert).astype(jnp.float32).astype(jnp.bfloat16)
        code_all = ublk[:, :, :, width:].reshape(group * rows, lanes)
        code_b = jnp.dot(code_all, pick, preferred_element_type=jnp.float32)
        tok = lax.broadcasted_iota(jnp.int32, (group * rows, slots), 0)
        col = lax.broadcasted_iota(jnp.int32, (group * rows, slots), 1)
        hit = (code_b == lax.rem(col, slot16).astype(jnp.float32)) & (tok // rows == col // slot16)
        place = jnp.where(hit, 1.0, 0.0).astype(jnp.bfloat16)
        for c0 in range(0, width, 512):
            rows_u = ublk[:, :, :, c0:c0 + 512].reshape(group * rows, 512)
            picked_rows = lax.dot_general(place, rows_u, (((0,), (0,)), ((), ())), preferred_element_type=jnp.float32)
            tokx[:, c0:c0 + 512] = picked_rows.astype(jnp.bfloat16)

    def pack_block(y_main, q):
        y_main = y_main.reshape(group, 2, 8, blk)
        y_tail = tail[...].reshape(group, 2, 8, blk)
        sub = lax.broadcasted_iota(jnp.int32, (group, 8, blk), 1)
        part = y_tail[:, 1 if q == 2 else 0]
        if q != 1:
            part = pltpu.roll(part.reshape(group * 8, blk).reshape(group, 8, blk), 4, 1)
        low = jnp.where(sub >= 4, part, y_main[:, 1])
        return jnp.concatenate([y_main[:, 0], low], axis=1).astype(jnp.bfloat16)

    def combine(step):
        for k in range(1, group):
            arrival(step, lax.rem(me + k, group)).wait_recv()
        spread = (row_i == (col_i // slot16) * experts_dev + step).astype(jnp.float32).astype(jnp.bfloat16)
        wide = jnp.dot(table[...].reshape(4 * rows, lanes), spread, preferred_element_type=jnp.float32)
        code_b = wide[:rows]
        slot_i = lax.rem(lax.broadcasted_iota(jnp.int32, (rows, slots), 1), slot16)
        slot_f = slot_i.astype(jnp.float32)
        for q in range(3):
            hits = [code_b == slot_f, (slot_i >= cap) & (code_b == slot_f - cap + 4 * q)]
            lhs = jnp.concatenate([jnp.where(hit, wide[p * rows:(p + 1) * rows], 0.0) for hit in hits for p in (1, 2, 3)], axis=0).astype(jnp.bfloat16)
            y_blk = recv[step, :, :, q * blk:(q + 1) * blk].reshape(slots, blk)
            res = jnp.dot(lhs, y_blk, preferred_element_type=jnp.float32)
            acc[:, q * blk:(q + 1) * blk] += res[:rows] + (res[rows:2 * rows] + res[2 * rows:3 * rows])
            acc[:, main:] += res[3 * rows:4 * rows] + (res[4 * rows:5 * rows] + res[5 * rows:])

    def one_step(step, carry):
        slot = lax.rem(step, depth)
        expert = step - 1
        is_routed = routed(step)

        @pl.when(step == 1)
        def _():
            relay()

        @pl.when(is_routed)
        def _():
            gather_rows(expert)

        @pl.when(jnp.logical_not(is_routed))
        def _():
            tokx[:rows] = ublk[me, :, :, :width].reshape(rows, width)
            tokx[rows:] = jnp.zeros((slots - rows, width), jnp.bfloat16)

        weights_gu(step, 0, egate_hbm, sgate_hbm, "wait")
        weights_gu(step, 1, eup_hbm, sup_hbm, "wait")
        for c0 in range(0, ff, 512):
            c1 = min(c0 + 512, ff)
            gate_act = jnp.dot(tokx[...], gu_buf[slot, 0, :, c0:c1], preferred_element_type=jnp.float32)
            up_act = jnp.dot(tokx[...], gu_buf[slot, 1, :, c0:c1], preferred_element_type=jnp.float32)
            midx[:, c0:c1] = (silu(gate_act) * up_act).astype(jnp.bfloat16)

        more = (step >= 1) & (step + depth < steps)
        second = (step >= 2) & (step + depth <= steps)

        @pl.when(more)
        def _():
            weights_gu(step + depth, 0, egate_hbm, sgate_hbm, "start")

        @pl.when(second)
        def _():
            send_group(expert - 1, 2)

        @pl.when(more)
        def _():
            weights_gu(step + depth, 1, eup_hbm, sup_hbm, "start")

        @pl.when(second)
        def _():
            send_group(expert - 1, 3)

        weights_dn(step, "wait")
        tail[...] = jnp.dot(midx[...], dn_buf[slot, :, main:], preferred_element_type=jnp.float32)

        @pl.when(jnp.logical_not(is_routed))
        def _():
            acc[:, main:] += tail[:rows]

        for q in range(3):
            y_main = jnp.dot(midx[...], dn_buf[slot, :, q * blk:(q + 1) * blk], preferred_element_type=jnp.float32)

            @pl.when(is_routed)
            def _():
                send[expert, :, :, q * blk:(q + 1) * blk] = pack_block(y_main, q)

            @pl.when(jnp.logical_not(is_routed))
            def _():
                acc[:, q * blk:(q + 1) * blk] += y_main[:rows]

        @pl.when(is_routed)
        def _():
            recv[expert, me] = send[expert, me]

        @pl.when(more)
        def _():
            weights_dn(step + depth, "start", 0)
            send_group(expert, 0)
            weights_dn(step + depth, "start", 1)
            send_group(expert, 1)

        @pl.when(is_routed & jnp.logical_not(more))
        def _():
            for n in range(4):
                send_group(expert, n)

        @pl.when(step == 0)
        def _():
            first_relay()

        @pl.when(expert >= lag)
        def _():
            combine(expert - lag)

        return carry

    lax.fori_loop(0, steps, one_step, 0)

    def last_combine(step, carry):
        combine(step)
        return carry

    lax.fori_loop(steps - 1 - lag, experts_dev, last_combine, 0)
    out_ref[...] = acc[...].astype(out_ref.dtype)

    for n, (block, h, dest) in enumerate(all_sends):
        block_copy(block, h, dest, n).wait_send()

    def drain(step, carry):
        for k in range(1, group):
            return_copy(step, lax.rem(me + k, group)).wait_send()
        return carry

    lax.fori_loop(0, experts_dev, drain, 0)


def hand_on(*refs):
    for k in range(3):
        refs[3 + k][...] = refs[k][...]


def layer(group, cap, hidden, ckv_cache, kr_cache, seq_lens, expert_ids, attn_gain, kv_gain, moe_gain, w_q, w_dkv, w_uk, w_uv, w_o, w_router, shared_gate, shared_up, shared_down, expert_gate, expert_up, expert_down):
    rows, width = hidden.shape
    heads, nope, lora = w_uk.shape
    length, rope_dim = kr_cache.shape[1:]
    experts_dev, _, ff = expert_gate.shape
    experts = w_router.shape[1]
    depth = 3
    main = 3 * width // 4
    slots = group * 16
    dims = (group, experts_dev, experts, cap, depth, 'dp')
    vmem = pl.BlockSpec(memory_space=pltpu.VMEM)
    hbm = pl.BlockSpec(memory_space=pl.ANY)
    results = pl.pallas_call(
        functools.partial(layer_kernel, dims),
        out_shape=(jax.ShapeDtypeStruct((rows, width), jnp.bfloat16), jax.ShapeDtypeStruct((rows, lora), jnp.bfloat16), jax.ShapeDtypeStruct((rows, rope_dim), jnp.bfloat16)),
        in_specs=[hbm, pl.BlockSpec(memory_space=pltpu.SMEM)] + [vmem] * 5 + [hbm] * 13,
        out_specs=(vmem, vmem, vmem),
        scratch_shapes=[
            pltpu.VMEM((group, 2, rows // 2, width + 128), jnp.bfloat16),
            pltpu.VMEM((slots, width), jnp.bfloat16),
            pltpu.VMEM((slots, ff), jnp.bfloat16),
            pltpu.VMEM((experts_dev, group, 16, main), jnp.bfloat16),
            pltpu.VMEM((experts_dev, group, 16, main), jnp.bfloat16),
            pltpu.VMEM((rows, width), jnp.float32),
            pltpu.VMEM((4, rows, 128), jnp.bfloat16),
            pltpu.VMEM((slots, width - main), jnp.float32),
            pltpu.VMEM((depth, 2, width, ff), jnp.bfloat16),
            pltpu.VMEM((depth, ff, width), jnp.bfloat16),
            pltpu.VMEM((lora // 128, rows * heads, 128), jnp.float32),
            pltpu.VMEM((rows, heads // 2, 128), jnp.float32),
            pltpu.VMEM((rows, lora), jnp.float32),
            pltpu.VMEM((rows, 128), jnp.float32),
            pltpu.SemaphoreType.DMA((depth, 2)),
            pltpu.SemaphoreType.DMA((depth,)),
            pltpu.SemaphoreType.DMA((14,)),
            pltpu.SemaphoreType.DMA((group, 2)),
            pltpu.SemaphoreType.DMA((experts_dev, group)),
            pltpu.SemaphoreType.DMA((experts_dev, group)),
            pltpu.SemaphoreType.DMA((20,)),
            pltpu.SemaphoreType.DMA((16,)),
        ],
        compiler_params=pltpu.CompilerParams(collective_id=0, has_side_effects=True, vmem_limit_bytes=67043328),
        name='decoder_layer',
    )(hidden, seq_lens, expert_ids.T, attn_gain, kv_gain, moe_gain, w_router.T,
      ckv_cache.reshape(rows * length, lora), jnp.swapaxes(kr_cache, 1, 2).reshape(rows * rope_dim, length), w_q, w_dkv.T, w_uk.reshape(heads * nope, lora),
      w_uv.reshape(heads // 2, experts_dev, group, 16, -1), w_o, shared_gate, shared_up, shared_down, expert_gate, expert_up, expert_down)
    return pl.pallas_call(
        hand_on,
        out_shape=tuple(jax.ShapeDtypeStruct(r.shape, r.dtype) for r in results),
        in_specs=[vmem] * 3,
        out_specs=(vmem,) * 3,
        name='hand_on',
    )(*results)


def solution(mesh):
    row_spec = P(('rep', 'dp'))
    full_spec = P()
    expert_spec = P('dp')

    def device_step(hidden, ckv_cache, kr_cache, seq_lens, expert_ids, attn_gain, kv_gain, moe_gain, w_q, w_dkv, w_uk, w_uv, w_o, w_router, shared_gate, shared_up, shared_down, expert_gate, expert_up, expert_down):
        capacity = max(2, 2 * hidden.shape[0] * expert_ids.shape[1] // w_router.shape[1])
        return layer(mesh.shape['dp'], capacity, hidden, ckv_cache, kr_cache, seq_lens, expert_ids, attn_gain, kv_gain, moe_gain, w_q, w_dkv, w_uk, w_uv, w_o, w_router, shared_gate, shared_up, shared_down, expert_gate, expert_up, expert_down)

    in_specs = (row_spec,) * 5 + (full_spec,) * 12 + (expert_spec,) * 3
    return jax.shard_map(device_step, mesh=mesh, in_specs=in_specs, out_specs=(row_spec, row_spec, row_spec), check_vma=False)
```

```python
import functools
import math

import jax
import jax.numpy as jnp
from jax import lax
from jax.experimental import pallas as pl
from jax.experimental.pallas import tpu as pltpu
from jax.sharding import PartitionSpec as P

NORM_EPS = 1e-6
ROPE_THETA = 10000.0


MESH_ID = pl.DeviceIdType.MESH


def attention_phase(refs, hooks):
    (hidden_hbm, hidden_ref, lens_ref, again_ref, kgain_ref, ckv_hbm, krt_hbm, wq_hbm, dkvt_hbm, uk_hbm, uv_hbm, wo_hbm, cnew_ref, knew_ref,
     tokx, uvbuf, gu_buf, dn_buf, qlat, qrot, newc, newk, pos, a_sem, c_sem) = refs
    rows, width = hidden_ref.shape
    lanes = 128
    tiles = qlat.shape[0]
    lora = tiles * lanes
    heads = qlat.shape[1] // rows
    rope_dim = krt_hbm.shape[0] // rows
    length = krt_hbm.shape[1]
    nope = uk_hbm.shape[0] // heads
    head_dim = nope + rope_dim
    qcols = wq_hbm.shape[1] // 4
    four = 4 * length
    value_dim = uv_hbm.shape[-1]
    scale = head_dim ** -0.5
    lanes = 128
    lat0 = dn_buf.shape[1] - four
    lat1 = dkvt_hbm.shape[0] - lat0
    cache_cols = slice(qcols, qcols + lora)
    kr_cols = slice(width // 2, width // 2 + length)

    def query_copy(i):
        return pltpu.make_async_copy(wq_hbm.at[:, i * qcols:(i + 1) * qcols], gu_buf.at[i // 2, i % 2, :, 0:qcols], a_sem.at[i])

    latent_copies = [
        pltpu.make_async_copy(dkvt_hbm.at[0:lat0], dn_buf.at[1, four:four + lat0], a_sem.at[4]),
        pltpu.make_async_copy(dkvt_hbm.at[lat0:lat0 + lat1], dn_buf.at[2, four:four + lat1], a_sem.at[5]),
    ]
    uk_copy = pltpu.make_async_copy(uk_hbm, gu_buf.at[0, 1, :, cache_cols], a_sem.at[6])
    kr_copies = [pltpu.make_async_copy(krt_hbm.at[w * width:(w + 1) * width], gu_buf.at[2, w, :, kr_cols], a_sem.at[7 + w]) for w in range(2)]
    out_copies = [pltpu.make_async_copy(wo_hbm.at[:, w * (width // 2):(w + 1) * (width // 2)], gu_buf.at[2, w, :, 0:width // 2], a_sem.at[9 + w]) for w in range(2)]
    uv_copies = [pltpu.make_async_copy(uv_hbm.at[i], uvbuf.at[:, :, :, i * value_dim:(i + 1) * value_dim], a_sem.at[11 + i]) for i in range(heads // 2)]
    wide_seqs = 48

    def cache_copy(n):
        if n >= 12:
            w, r = (n - 12) // 2, n % 2
            return pltpu.make_async_copy(ckv_hbm.at[n * four:(n + 1) * four], gu_buf.at[1, w, r * four:(r + 1) * four, cache_cols], c_sem.at[n])
        return pltpu.make_async_copy(ckv_hbm.at[n * four:(n + 1) * four], dn_buf.at[n // 4, 0:four, (n % 4) * lora:(n % 4 + 1) * lora], c_sem.at[n])

    hidden_copy = pltpu.make_async_copy(hidden_hbm, hidden_ref, a_sem.at[19])
    hidden_copy.start()
    hooks[5]()
    query_copy(0).start()
    for copy in latent_copies:
        copy.start()
    uk_copy.start()
    for i in range(1, 4):
        query_copy(i).start()
    for n in range(12, 16):
        cache_copy(n).start()
    for copy in kr_copies:
        copy.start()
    for n in range(8):
        cache_copy(n).start()

    hooks[4]()

    lane = lax.broadcasted_iota(jnp.int32, (rows, lanes), 1)
    hidden_copy.wait()
    hidden = hidden_ref[...].astype(jnp.float32)
    inv = lax.rsqrt(jnp.mean(hidden * hidden, axis=-1, keepdims=True) + NORM_EPS)
    tokx[0:rows] = (hidden * inv * again_ref[...].astype(jnp.float32).reshape(1, -1)).astype(jnp.bfloat16)
    for b in range(rows):
        pos[b:b + 1, :] = jnp.full((1, lanes), lens_ref[b], jnp.int32).astype(jnp.float32)
    quarter = lax.rem(lane, rope_dim // 2).astype(jnp.float32)
    angle = pos[...] * jnp.exp(quarter * (-2.0 / rope_dim * math.log(ROPE_THETA)))
    rope_cos = jnp.cos(angle)
    low_half = lax.rem(lane, rope_dim) < rope_dim // 2
    rope_sin = jnp.where(low_half, -jnp.sin(angle), jnp.sin(angle))

    def rope(value):
        swapped = jnp.where(low_half, pltpu.roll(value, lanes - rope_dim // 2, 1), pltpu.roll(value, rope_dim // 2, 1))
        return value * rope_cos + swapped * rope_sin

    first_half = lane < rope_dim

    def row_of(h):
        return (h % 2) * (heads // 2) + h // 2

    for i in range(4):
        query_copy(i).wait()
        q_cols = jnp.dot(tokx[0:rows], gu_buf[i // 2, i % 2, :, 0:qcols], preferred_element_type=jnp.float32)
        q_cols = q_cols.astype(jnp.bfloat16).astype(jnp.float32)
        if i == 0:
            for copy in uv_copies + out_copies:
                copy.start()
            for n in range(8, 12):
                cache_copy(n).start()
            uk_copy.wait()
        for pair in range(qcols // (2 * head_dim)):
            base = pair * 2 * head_dim
            tile0, tile1, tile2 = (q_cols[:, base + k * lanes:base + (k + 1) * lanes] for k in range(3))
            head = i * (qcols // head_dim) + 2 * pair
            nopes = (tile0, pltpu.roll(jnp.where(first_half, tile2, tile1), lanes // 2, 1))
            turned = rope(jnp.where(first_half, tile1, tile2))
            qrot[:, head // 2, :] = turned
            for odd in range(2):
                h = head + odd
                uk_head = gu_buf[0, 1, h * nope:(h + 1) * nope, cache_cols]
                q_head = jnp.dot(nopes[odd].astype(jnp.bfloat16), uk_head, preferred_element_type=jnp.float32)
                for j in range(tiles):
                    qlat[j, pl.ds(row_of(h), rows, stride=heads), :] = q_head[:, j * lanes:(j + 1) * lanes]
    hooks[0]()

    for copy in latent_copies:
        copy.wait()
    contract = (((1,), (1,)), ((), ()))
    part0 = lax.dot_general(tokx[0:rows], dn_buf[1, four:four + lat0], contract, preferred_element_type=jnp.float32)
    part1 = lax.dot_general(tokx[0:rows], dn_buf[2, four:four + lat1], contract, preferred_element_type=jnp.float32)
    latent = jnp.concatenate([part0, part1[:, :lora - lat0]], axis=-1)
    inv = lax.rsqrt(jnp.mean(latent * latent, axis=-1, keepdims=True) + NORM_EPS)
    c_new = (latent * inv * kgain_ref[...].astype(jnp.float32).reshape(1, -1)).astype(jnp.bfloat16)
    cnew_ref[...] = c_new
    newc[...] = c_new.astype(jnp.float32)
    key_part = jnp.concatenate([part1[:, lora - lat0:], jnp.zeros((rows, lanes - rope_dim), jnp.float32)], axis=-1)
    k_new = rope(key_part)[:, :rope_dim].astype(jnp.bfloat16)
    knew_ref[...] = k_new
    newk[...] = jnp.concatenate([k_new.astype(jnp.float32), jnp.zeros((rows, lanes - rope_dim), jnp.float32)], axis=-1)

    column = lax.broadcasted_iota(jnp.int32, (heads, length), 1)

    def attend(seq0, keys, rope_keys):
        scores, news = [], []
        for s in range(8):
            b = seq0 + s
            q_b = jnp.concatenate([qlat[j, pl.ds(pl.multiple_of(b * heads, heads), heads), :] for j in range(tiles)], axis=-1).astype(jnp.bfloat16)
            pairs = qrot[b]
            r_b = jnp.concatenate([pairs, pltpu.roll(pairs, lanes // 2, 1)], axis=0).astype(jnp.bfloat16)
            score = lax.dot_general(q_b, keys(s), contract, preferred_element_type=jnp.float32)
            score += jnp.dot(r_b[:, :rope_dim], rope_keys(s), preferred_element_type=jnp.float32)
            scores.append(jnp.where(column < lens_ref[b], score * scale, -jnp.inf))
            r_f = jnp.where(lax.broadcasted_iota(jnp.int32, (heads, lanes), 1) < rope_dim, r_b.astype(jnp.float32), 0.0)
            new = jnp.sum(q_b.astype(jnp.float32) * newc[pl.ds(b, 1), :], axis=-1, keepdims=True)
            news.append((new + jnp.sum(r_f * newk[pl.ds(b, 1), :], axis=-1, keepdims=True)) * scale)
        scores = jnp.concatenate(scores, axis=0)
        news = jnp.concatenate(news, axis=0)
        top = jnp.maximum(jnp.max(scores, axis=-1, keepdims=True), news)
        exp_cache = jnp.exp(scores - top)
        exp_new = jnp.exp(news - top)
        total = jnp.sum(exp_cache, axis=-1, keepdims=True) + exp_new
        prob = (exp_cache / total).astype(jnp.bfloat16)
        prob_new = (exp_new / total).astype(jnp.bfloat16).astype(jnp.float32)
        for s in range(8):
            b = seq0 + s
            out = jnp.dot(prob[s * heads:(s + 1) * heads], keys(s), preferred_element_type=jnp.float32)
            out += prob_new[s * heads:(s + 1) * heads] * newc[pl.ds(b, 1), :]
            for j in range(tiles):
                qlat[j, pl.ds(pl.multiple_of(b * heads, heads), heads), :] = out[:, j * lanes:(j + 1) * lanes]

    for copy in kr_copies:
        copy.wait()
    for n in range(12, 16):
        cache_copy(n).wait()
    seqs_half = width // rope_dim

    def wide_step(w, carry):
        seq0 = wide_seqs + 8 * w

        def keys(s):
            return gu_buf[1, w, s * length:(s + 1) * length, cache_cols]

        def rope_keys(s):
            return gu_buf[2, 1, pl.ds((seq0 - seqs_half + s) * rope_dim, rope_dim), kr_cols]

        attend(seq0, keys, rope_keys)
        return carry

    lax.fori_loop(0, 2, wide_step, 0)
    hooks[1]()

    def deep_step(it, carry):
        d, i2 = it // 2, lax.rem(it, 2)
        for k in range(2):
            pltpu.make_async_copy(ckv_hbm.at[0:four], dn_buf.at[d, 0:four, pl.ds(pl.multiple_of((2 * i2 + k) * lora, lora), lora)], c_sem.at[2 * it + k]).wait()

        def keys(s):
            cols = pl.ds(pl.multiple_of((2 * i2 + s // 4) * lora, lora), lora)
            return dn_buf[d, (s % 4) * length:(s % 4 + 1) * length, cols]

        def rope_keys(s):
            return gu_buf[2, it // 4, pl.ds((8 * lax.rem(it, 4) + s) * rope_dim, rope_dim), kr_cols]

        attend(8 * it, keys, rope_keys)
        hooks[2](it)
        return carry

    lax.fori_loop(0, wide_seqs // 8, deep_step, 0)

    for copy in uv_copies:
        copy.wait()
    for h in range(heads):
        o_lat = jnp.concatenate([qlat[j, pl.ds(row_of(h), rows, stride=heads), :] for j in range(tiles)], axis=-1).astype(jnp.bfloat16)
        uv_half = uvbuf.shape[0] // 2
        uv_head = uvbuf[(h % 2) * uv_half:(h % 2 + 1) * uv_half, :, :, (h // 2) * value_dim:(h // 2 + 1) * value_dim].reshape(lora, value_dim)
        tokx[rows:2 * rows, h * value_dim:(h + 1) * value_dim] = jnp.dot(o_lat, uv_head, preferred_element_type=jnp.float32).astype(jnp.bfloat16)
    parts = []
    for w in range(2):
        out_copies[w].wait()
        parts.append(jnp.dot(tokx[rows:2 * rows], gu_buf[2, w, :, 0:width // 2], preferred_element_type=jnp.float32))
    hooks[3]()
    resid = hidden_ref[...].astype(jnp.float32) + jnp.concatenate(parts, axis=-1)
    return resid.astype(jnp.bfloat16)


def silu(value):
    return value * (1.0 / (1.0 + jnp.exp(-value)))


def layer_kernel(dims, hidden_hbm, lens_hbm, ids_hbm, again_hbm, kgain_hbm, gain_hbm, router_hbm, ckv_hbm, krt_hbm, wq_hbm, dkvt_hbm, uk_hbm, uv_hbm, wo_hbm,
                 sgate_hbm, sup_hbm, sdown_hbm, egate_hbm, eup_hbm, edown_hbm, out_ref, cnew_ref, knew_ref,
                 ublk, tokx, midx, send, recv, acc, table, tail, gu_buf, dn_buf, qlat, qrot, newc, newk,
                 lens_ref, ids_ref, again_ref, kgain_ref, gain_ref, router_ref, small_sem,
                 gu_sem, dn_sem, us_sem, ur_sem, ys_sem, yr_sem, a_sem, c_sem):
    group, experts_dev, experts, cap, depth, dp_axis = dims
    rows, width = hidden_hbm.shape
    half = rows // 2
    ff = gu_buf.shape[-1]
    n_shared = sgate_hbm.shape[-1] // ff
    steps = experts_dev + n_shared
    slot16 = 16
    slots = group * slot16
    main = send.shape[-1]
    blk = main // 3
    top_k = ids_hbm.shape[0]
    lag = 4
    lanes = 128
    me = lax.axis_index(dp_axis)
    chips = group // 2
    core = lax.rem(me, 2)
    chip = me // 2
    partner = chip * 2 + (1 - core)
    left = lax.rem(chip + chips - 1, chips) * 2 + core
    right = lax.rem(chip + 1, chips) * 2 + core
    far = lax.rem(chip + 2, chips) * 2 + core

    def routed(step):
        return (step >= 1) & (step <= experts_dev)

    def either(condition, action_a, action_b):
        if isinstance(condition, bool):
            (action_a if condition else action_b)()
        else:
            pl.when(condition)(action_a)
            pl.when(jnp.logical_not(condition))(action_b)

    def weights_gu(step, which, hbm, shared_hbm, action):
        slot = step % depth if isinstance(step, int) else lax.rem(step, depth)

        def own():
            getattr(pltpu.make_async_copy(hbm.at[step - 1], gu_buf.at[slot, which], gu_sem.at[slot, which]), action)()

        def shared():
            start = step // (steps - 1) * ff
            cols = pl.ds(start if isinstance(step, int) else pl.multiple_of(start, 128), ff)
            getattr(pltpu.make_async_copy(shared_hbm.at[:, cols], gu_buf.at[slot, which], gu_sem.at[slot, which]), action)()

        either(routed(step), own, shared)

    def weights_dn(step, action):
        slot = step % depth if isinstance(step, int) else lax.rem(step, depth)

        def own():
            getattr(pltpu.make_async_copy(edown_hbm.at[step - 1], dn_buf.at[slot], dn_sem.at[slot]), action)()

        def shared():
            start = step // (steps - 1) * ff
            cols = pl.ds(start if isinstance(step, int) else pl.multiple_of(start, 128), ff)
            getattr(pltpu.make_async_copy(sdown_hbm.at[cols], dn_buf.at[slot], dn_sem.at[slot]), action)()

        either(routed(step), own, shared)

    def fetch(step):
        weights_gu(step, 0, egate_hbm, sgate_hbm, "start")
        weights_gu(step, 1, eup_hbm, sup_hbm, "start")

    barrier = pltpu.get_barrier_semaphore()
    small = [pltpu.make_async_copy(src, dst, small_sem.at[k]) for k, (src, dst) in enumerate(
        ((again_hbm, again_ref), (lens_hbm, lens_ref), (ids_hbm, ids_ref), (kgain_hbm, kgain_ref), (gain_hbm, gain_ref), (router_hbm, router_ref)))]

    def request():
        for copy in small:
            copy.start()

    def opening():
        for k in range(1, group):
            pl.semaphore_signal(barrier, inc=1, device_id={dp_axis: lax.rem(me + k, group)}, device_id_type=MESH_ID)
        small[2].wait()
        expert_i = lax.broadcasted_iota(jnp.int32, (lanes, rows), 0)
        picked = ids_ref[0:1, :] == expert_i
        for k in range(1, top_k):
            picked = picked | (ids_ref[k:k + 1, :] == expert_i)
        tok_a = lax.broadcasted_iota(jnp.int32, (rows, rows), 0)
        tok_b = lax.broadcasted_iota(jnp.int32, (rows, rows), 1)
        before = jnp.where(tok_a < tok_b, 1.0, 0.0).astype(jnp.bfloat16)
        rank = jnp.dot(jnp.where(picked, 1.0, 0.0).astype(jnp.bfloat16), before, preferred_element_type=jnp.float32)
        codes_t = jnp.where(picked, rank, -1.0).astype(jnp.bfloat16)
        same = jnp.where(tok_a == tok_b, 1.0, 0.0).astype(jnp.bfloat16)
        codes = lax.dot_general(same, codes_t, (((1,), (1,)), ((), ())), preferred_element_type=jnp.float32).astype(jnp.bfloat16)
        table[0] = codes
        for h in range(2):
            ublk[me, h, :, width:] = codes[h * half:(h + 1) * half]
        for k in (0, 1, 3, 4, 5):
            small[k].wait()

    def freed_deep(it):
        for d in range(depth):
            @pl.when(it == 2 * d + 1)
            def _():
                weights_dn(d, "start")

    hooks = (lambda: fetch(0), lambda: fetch(1), freed_deep, lambda: fetch(2), opening, request)
    resid = attention_phase((hidden_hbm, out_ref, lens_ref, again_ref, kgain_ref, ckv_hbm, krt_hbm, wq_hbm, dkvt_hbm, uk_hbm, uv_hbm, wo_hbm, cnew_ref, knew_ref,
                             tokx, send, gu_buf, dn_buf, qlat, qrot, newc, newk, acc.at[:, 0:128], a_sem, c_sem), hooks)

    resid = resid.astype(jnp.float32)
    inv = lax.rsqrt(jnp.mean(resid * resid, axis=-1, keepdims=True) + NORM_EPS)
    u = (resid * inv * gain_ref[...].astype(jnp.float32).reshape(1, -1)).astype(jnp.bfloat16)
    for h in range(2):
        ublk[me, h, :, :width] = u[h * half:(h + 1) * half]
    pl.semaphore_wait(barrier, group - 1)

    def block_copy(block, h, dest, sem_no):
        return pltpu.make_async_remote_copy(src_ref=ublk.at[block, h], dst_ref=ublk.at[block, h], send_sem=us_sem.at[sem_no], recv_sem=ur_sem.at[block, h], device_id={dp_axis: dest}, device_id_type=MESH_ID)

    def crossed(block):
        return lax.rem(block + 1 - 2 * core + group, group)

    first_sends = ((me, 0, right), (me, 1, left), (me, 1, right), (me, 0, left), (me, 0, partner), (me, 1, partner))
    relays = ((left, 0, right), (left, 0, partner), (right, 1, left), (right, 1, partner), (left, 1, partner), (right, 0, partner), (far, 0, partner), (far, 1, partner))
    all_sends = first_sends + relays

    def send_block(n):
        block, h, dest = all_sends[n]
        block_copy(block, h, dest, n).start()

    def arrived(block, h):
        block_copy(block, h, partner, 0).wait_recv()

    for n in range(len(first_sends)):
        send_block(n)

    logits = lax.dot_general(u, router_ref[...], (((1,), (1,)), ((), ())), preferred_element_type=jnp.float32)
    logits = logits - jnp.max(logits, axis=-1, keepdims=True)
    expl = jnp.exp(logits)
    prob = expl / jnp.sum(expl, axis=-1, keepdims=True)
    prob = jnp.concatenate([prob, jnp.zeros((rows, lanes - experts), jnp.float32)], axis=-1)
    p0 = prob.astype(jnp.bfloat16)
    rest = prob - p0.astype(jnp.float32)
    p1 = rest.astype(jnp.bfloat16)
    p2 = (rest - p1.astype(jnp.float32)).astype(jnp.bfloat16)
    table[1] = p0
    table[2] = p1
    table[3] = p2
    acc[...] = resid

    def relay():
        seen = set()
        for n in range(len(first_sends), len(all_sends)):
            block, h, _ = all_sends[n]
            if (id(block), h) not in seen:
                seen.add((id(block), h))
                arrived(block, h)
            send_block(n)
        for block in (partner, crossed(left), crossed(right), crossed(far)):
            for h in range(2):
                arrived(block, h)

    row_i = lax.broadcasted_iota(jnp.int32, (lanes, slots), 0)
    col_i = lax.broadcasted_iota(jnp.int32, (lanes, slots), 1)

    def return_copy(step, dest):
        return pltpu.make_async_remote_copy(src_ref=send.at[step, dest], dst_ref=recv.at[step, me], send_sem=ys_sem.at[step, dest], recv_sem=yr_sem.at[step, me], device_id={dp_axis: dest}, device_id_type=MESH_ID)

    def arrival(step, source):
        return pltpu.make_async_remote_copy(src_ref=send.at[step, source], dst_ref=recv.at[step, source], send_sem=ys_sem.at[step, source], recv_sem=yr_sem.at[step, source], device_id={dp_axis: source}, device_id_type=MESH_ID)

    def gather_rows(expert):
        pick = (row_i == me * experts_dev + expert).astype(jnp.float32).astype(jnp.bfloat16)
        code_all = ublk[:, :, :, width:].reshape(group * rows, lanes)
        code_b = jnp.dot(code_all, pick, preferred_element_type=jnp.float32)
        tok = lax.broadcasted_iota(jnp.int32, (group * rows, slots), 0)
        col = lax.broadcasted_iota(jnp.int32, (group * rows, slots), 1)
        hit = (code_b == lax.rem(col, slot16).astype(jnp.float32)) & (tok // rows == col // slot16)
        place = jnp.where(hit, 1.0, 0.0).astype(jnp.bfloat16)
        for c0 in range(0, width, 512):
            rows_u = ublk[:, :, :, c0:c0 + 512].reshape(group * rows, 512)
            picked_rows = lax.dot_general(place, rows_u, (((0,), (0,)), ((), ())), preferred_element_type=jnp.float32)
            tokx[:, c0:c0 + 512] = picked_rows.astype(jnp.bfloat16)

    def pack_block(y_main, q):
        y_main = y_main.reshape(group, 2, 8, blk)
        y_tail = tail[...].reshape(group, 2, 8, blk)
        sub = lax.broadcasted_iota(jnp.int32, (group, 8, blk), 1)
        part = y_tail[:, 1 if q == 2 else 0]
        if q != 1:
            part = pltpu.roll(part.reshape(group * 8, blk).reshape(group, 8, blk), 4, 1)
        low = jnp.where(sub >= 4, part, y_main[:, 1])
        return jnp.concatenate([y_main[:, 0], low], axis=1).astype(jnp.bfloat16)

    def combine(step):
        for k in range(1, group):
            arrival(step, lax.rem(me + k, group)).wait_recv()
        spread = (row_i == (col_i // slot16) * experts_dev + step).astype(jnp.float32).astype(jnp.bfloat16)
        wide = jnp.dot(table[...].reshape(4 * rows, lanes), spread, preferred_element_type=jnp.float32)
        code_b = wide[:rows]
        slot_i = lax.rem(lax.broadcasted_iota(jnp.int32, (rows, slots), 1), slot16)
        slot_f = slot_i.astype(jnp.float32)
        for q in range(3):
            hits = [code_b == slot_f, (slot_i >= cap) & (code_b == slot_f - cap + 4 * q)]
            lhs = jnp.concatenate([jnp.where(hit, wide[p * rows:(p + 1) * rows], 0.0) for hit in hits for p in (1, 2, 3)], axis=0).astype(jnp.bfloat16)
            y_blk = recv[step, :, :, q * blk:(q + 1) * blk].reshape(slots, blk)
            res = jnp.dot(lhs, y_blk, preferred_element_type=jnp.float32)
            acc[:, q * blk:(q + 1) * blk] += res[:rows] + (res[rows:2 * rows] + res[2 * rows:3 * rows])
            acc[:, main:] += res[3 * rows:4 * rows] + (res[4 * rows:5 * rows] + res[5 * rows:])

    def one_step(step, carry):
        slot = lax.rem(step, depth)
        expert = step - 1
        is_routed = routed(step)

        @pl.when(step == 1)
        def _():
            relay()

        @pl.when(is_routed)
        def _():
            gather_rows(expert)

        @pl.when(jnp.logical_not(is_routed))
        def _():
            tokx[:rows] = ublk[me, :, :, :width].reshape(rows, width)
            tokx[rows:] = jnp.zeros((slots - rows, width), jnp.bfloat16)

        weights_gu(step, 0, egate_hbm, sgate_hbm, "wait")
        weights_gu(step, 1, eup_hbm, sup_hbm, "wait")
        for c0 in range(0, ff, 512):
            c1 = min(c0 + 512, ff)
            gate_act = jnp.dot(tokx[...], gu_buf[slot, 0, :, c0:c1], preferred_element_type=jnp.float32)
            up_act = jnp.dot(tokx[...], gu_buf[slot, 1, :, c0:c1], preferred_element_type=jnp.float32)
            midx[:, c0:c1] = (silu(gate_act) * up_act).astype(jnp.bfloat16)

        @pl.when(step + depth < steps)
        def _():
            fetch(step + depth)

        weights_dn(step, "wait")
        tail[...] = jnp.dot(midx[...], dn_buf[slot, :, main:], preferred_element_type=jnp.float32)

        @pl.when(jnp.logical_not(is_routed))
        def _():
            acc[:, main:] += tail[:rows]

        for q in range(3):
            y_main = jnp.dot(midx[...], dn_buf[slot, :, q * blk:(q + 1) * blk], preferred_element_type=jnp.float32)

            @pl.when(is_routed)
            def _():
                send[expert, :, :, q * blk:(q + 1) * blk] = pack_block(y_main, q)

            @pl.when(jnp.logical_not(is_routed))
            def _():
                acc[:, q * blk:(q + 1) * blk] += y_main[:rows]

        @pl.when(step + depth < steps)
        def _():
            weights_dn(step + depth, "start")

        @pl.when(is_routed)
        def _():
            recv[expert, me] = send[expert, me]
            for k in (4, 3, 5, 2, 6, 1, 7):
                return_copy(expert, lax.rem(me + k, group)).start()

        @pl.when(expert >= lag)
        def _():
            combine(expert - lag)

        return carry

    lax.fori_loop(0, steps, one_step, 0)

    def last_combine(step, carry):
        combine(step)
        return carry

    lax.fori_loop(steps - 1 - lag, experts_dev, last_combine, 0)
    out_ref[...] = acc[...].astype(out_ref.dtype)

    for n, (block, h, dest) in enumerate(all_sends):
        block_copy(block, h, dest, n).wait_send()

    def drain(step, carry):
        for k in range(1, group):
            return_copy(step, lax.rem(me + k, group)).wait_send()
        return carry

    lax.fori_loop(0, experts_dev, drain, 0)


def hand_on(*refs):
    for k in range(3):
        refs[3 + k][...] = refs[k][...]


def layer(group, cap, hidden, ckv_cache, kr_cache, seq_lens, expert_ids, attn_gain, kv_gain, moe_gain, w_q, w_dkv, w_uk, w_uv, w_o, w_router, shared_gate, shared_up, shared_down, expert_gate, expert_up, expert_down):
    rows, width = hidden.shape
    heads, nope, lora = w_uk.shape
    length, rope_dim = kr_cache.shape[1:]
    experts_dev, _, ff = expert_gate.shape
    experts = w_router.shape[1]
    depth = 3
    main = 3 * width // 4
    slots = group * 16
    dims = (group, experts_dev, experts, cap, depth, 'dp')
    vmem = pl.BlockSpec(memory_space=pltpu.VMEM)
    hbm = pl.BlockSpec(memory_space=pl.ANY)
    results = pl.pallas_call(
        functools.partial(layer_kernel, dims),
        out_shape=(jax.ShapeDtypeStruct((rows, width), jnp.bfloat16), jax.ShapeDtypeStruct((rows, lora), jnp.bfloat16), jax.ShapeDtypeStruct((rows, rope_dim), jnp.bfloat16)),
        in_specs=[hbm] * 20,
        out_specs=(vmem, vmem, vmem),
        scratch_shapes=[
            pltpu.VMEM((group, 2, rows // 2, width + 128), jnp.bfloat16),
            pltpu.VMEM((slots, width), jnp.bfloat16),
            pltpu.VMEM((slots, ff), jnp.bfloat16),
            pltpu.VMEM((experts_dev, group, 16, main), jnp.bfloat16),
            pltpu.VMEM((experts_dev, group, 16, main), jnp.bfloat16),
            pltpu.VMEM((rows, width), jnp.float32),
            pltpu.VMEM((4, rows, 128), jnp.bfloat16),
            pltpu.VMEM((slots, width - main), jnp.float32),
            pltpu.VMEM((depth, 2, width, ff), jnp.bfloat16),
            pltpu.VMEM((depth, ff, width), jnp.bfloat16),
            pltpu.VMEM((lora // 128, rows * heads, 128), jnp.float32),
            pltpu.VMEM((rows, heads // 2, 128), jnp.float32),
            pltpu.VMEM((rows, lora), jnp.float32),
            pltpu.VMEM((rows, 128), jnp.float32),
            pltpu.SMEM(seq_lens.shape, jnp.int32),
            pltpu.VMEM(expert_ids.shape[::-1], jnp.int32),
            pltpu.VMEM(attn_gain.shape, jnp.bfloat16),
            pltpu.VMEM(kv_gain.shape, jnp.bfloat16),
            pltpu.VMEM(moe_gain.shape, jnp.bfloat16),
            pltpu.VMEM(w_router.shape[::-1], jnp.bfloat16),
            pltpu.SemaphoreType.DMA((6,)),
            pltpu.SemaphoreType.DMA((depth, 2)),
            pltpu.SemaphoreType.DMA((depth,)),
            pltpu.SemaphoreType.DMA((14,)),
            pltpu.SemaphoreType.DMA((group, 2)),
            pltpu.SemaphoreType.DMA((experts_dev, group)),
            pltpu.SemaphoreType.DMA((experts_dev, group)),
            pltpu.SemaphoreType.DMA((20,)),
            pltpu.SemaphoreType.DMA((16,)),
        ],
        compiler_params=pltpu.CompilerParams(collective_id=0, has_side_effects=True, vmem_limit_bytes=67043328),
        name='decoder_layer',
    )(hidden, seq_lens, expert_ids.T, attn_gain, kv_gain, moe_gain, w_router.T,
      ckv_cache.reshape(rows * length, lora), jnp.swapaxes(kr_cache, 1, 2).reshape(rows * rope_dim, length), w_q, w_dkv.T, w_uk.reshape(heads * nope, lora),
      w_uv.reshape(heads // 2, experts_dev, group, 16, -1), w_o, shared_gate, shared_up, shared_down, expert_gate, expert_up, expert_down)
    return pl.pallas_call(
        hand_on,
        out_shape=tuple(jax.ShapeDtypeStruct(r.shape, r.dtype) for r in results),
        in_specs=[vmem] * 3,
        out_specs=(vmem,) * 3,
        name='hand_on',
    )(*results)


def solution(mesh):
    row_spec = P(('rep', 'dp'))
    full_spec = P()
    expert_spec = P('dp')

    def device_step(hidden, ckv_cache, kr_cache, seq_lens, expert_ids, attn_gain, kv_gain, moe_gain, w_q, w_dkv, w_uk, w_uv, w_o, w_router, shared_gate, shared_up, shared_down, expert_gate, expert_up, expert_down):
        capacity = max(2, 2 * hidden.shape[0] * expert_ids.shape[1] // w_router.shape[1])
        return layer(mesh.shape['dp'], capacity, hidden, ckv_cache, kr_cache, seq_lens, expert_ids, attn_gain, kv_gain, moe_gain, w_q, w_dkv, w_uk, w_uv, w_o, w_router, shared_gate, shared_up, shared_down, expert_gate, expert_up, expert_down)

    in_specs = (row_spec,) * 5 + (full_spec,) * 12 + (expert_spec,) * 3
    return jax.shard_map(device_step, mesh=mesh, in_specs=in_specs, out_specs=(row_spec, row_spec, row_spec), check_vma=False)
```
